32 devices in a mesh: dp: 4 (over y, core), sp: 2 (over x), tp: 4 (over z).
Axes of the slice: x: 2, y: 2, z: 4, core: 2. Of those that a mesh axis runs over, the one named last changes fastest.
Arguments:
- query: bfloat16 [4, 768, 3072], P('dp', 'sp', 'tp'), may hold values from -110 to 110
- key: bfloat16 [4, 768, 3072], P('dp', 'sp', 'tp'), may hold values from -8 to 8
- value: bfloat16 [4, 768, 3072], P('dp', 'sp', 'tp'), may hold values from -6 to 6
- text_key: bfloat16 [4, 256, 3072], P('dp', None, 'tp'), may hold values from -6 to 6
- text_value: bfloat16 [4, 256, 3072], P('dp', None, 'tp'), may hold values from -6 to 6
- grad_out: bfloat16 [4, 768, 3072], P('dp', 'sp', 'tp'), may hold values from -6 to 6
- gate: bfloat16 [4, 3072], P('dp'), may hold values from 0.5 to 1.5
- out_weight: bfloat16 [3072, 3072], P('tp', 'dp'), may hold values from -0.109375 to 0.109375
- windows: int32 [2, 2], P('sp'), may hold values from 0 to 2, as said below
- tile_map: int32 [2, 1], replicated, may hold values from 0 to 2, as said below
- text_count: int32 [4], P('dp'), may hold values from 1 to 256
Outputs:
- grad_query: bfloat16 [4, 768, 3072], P('dp', 'sp', 'tp')
- grad_key: bfloat16 [4, 768, 3072], P('dp', 'sp', 'tp')
- grad_value: bfloat16 [4, 768, 3072], P('dp', 'sp', 'tp')
- grad_text_key: bfloat16 [4, 256, 3072], P('dp', None, 'tp')
- grad_text_value: bfloat16 [4, 256, 3072], P('dp', None, 'tp')
- grad_weight: float32 [3072, 3072], P('tp', 'dp')
The draws below stay inside these ranges and needn't reach their ends.
Inputs may be any that keep to these rules, and one draw needn't show every extreme that they name: `tile_map`: the positions within each row are distinct. `windows`: the time reach is 0 or 1; the first tile of every time slab has time reach 1 and spatial reach 2.
All inputs are finite; a program needn't handle non-finite values.
Results may differ from the reference program's by a relative error of at most 0.024.
Values may be sent and summed in bfloat16 or wider, within the bound.
A program may use at most 128 MiB of HBM per device.

```python
import jax
import jax.numpy as jnp
from jax import lax

D = 3072
HD = 128
TILE = 384
TILES_DEV = 1
TXT = 256
VTOK = 768
SAMPLES = 4
NTILES = 2
N_SP = 2


def base_keys(key):
    raw = jax.random.normal(jax.random.fold_in(key, 11), (SAMPLES, VTOK, D), jnp.float32)
    return jnp.clip(raw, -6.0, 6.0)


def draw_key(key, part):
    keys = base_keys(key)
    return keys.astype(jnp.bfloat16)


def draw_query(key, part):
    fresh = jnp.clip(jax.random.normal(jax.random.fold_in(key, 13), (SAMPLES, VTOK, D), jnp.float32), -6.0, 6.0)
    return fresh.astype(jnp.bfloat16)


def draw_tile_map(key, part):
    streams = jax.random.split(jax.random.fold_in(key, 21), N_SP)
    orders = jax.vmap(lambda stream: jax.random.permutation(stream, 3 * TILES_DEV)[:TILES_DEV])(streams)
    orders = orders.astype(jnp.int32)
    highest = 3 * TILES_DEV - 1
    first_row = orders[0]
    has_lowest = jnp.any(first_row == 0)
    first_row = first_row.at[0].set(jnp.where(has_lowest, first_row[0], 0))
    orders = orders.at[0].set(first_row)
    last_row = orders[N_SP - 1]
    has_highest = jnp.any(last_row == highest)
    last_row = last_row.at[0].set(jnp.where(has_highest, last_row[0], highest))
    orders = orders.at[N_SP - 1].set(last_row)
    return orders.astype(jnp.int32)


def draw_windows(key, part):
    time_reach = jax.random.randint(jax.random.fold_in(key, 31), (NTILES,), 0, 2)
    space_reach = jax.random.randint(jax.random.fold_in(key, 32), (NTILES,), 0, 3 * TILES_DEV)
    first = jnp.arange(NTILES) % TILES_DEV == 0
    time_reach = jnp.where(first, 1, time_reach)
    space_reach = jnp.where(first, 3 * TILES_DEV - 1, space_reach)
    return jnp.stack([time_reach, space_reach], axis=1).astype(jnp.int32)


def place_ends(result, stream_key, least, top_value):
    longest = result.shape.index(max(result.shape))
    spots = []
    for shift in (0, 1):
        where = [jax.random.randint(jax.random.fold_in(stream_key, axis), (), 0, length) for axis, length in enumerate(result.shape)]
        where[longest] = (where[longest] + shift) % result.shape[longest]
        spots.append(tuple(where))
    return result.at[spots[0]].set(least).at[spots[1]].set(top_value)


def steps_of(own_key, shape, cuts, low, largest):
    level = 1.0
    for position, blocks in cuts:
        steps = jax.random.uniform(jax.random.fold_in(jax.random.fold_in(own_key, 6), position), (blocks,), jnp.float32, low / len(cuts), largest / len(cuts))
        level = level * jnp.repeat(jnp.exp(steps), shape[position] // blocks).reshape((-1,) + (1,) * (len(shape) - 1 - position))
    return level


def normal_values(own_key, dims, width, most, cuts=(), held_as=jnp.bfloat16):
    values = width * jax.random.normal(own_key, dims, jnp.float32)
    if cuts:
        values = values * steps_of(own_key, dims, cuts, -0.22, 0.18)
    return jnp.clip(values, -most, most).astype(held_as)


def setup_inputs(seed: int = 0) -> dict:
    streams_of = jax.random.split(jax.random.key(seed), 12)
    return {
        "query": draw_query(jax.random.fold_in(streams_of[11], 71), 0),
        "key": draw_key(jax.random.fold_in(streams_of[11], 71), 0),
        "value": normal_values(streams_of[2], (SAMPLES, VTOK, D), 1.0, 6.0, ((0, 4), (1, 2), (2, 4))),
        "text_key": normal_values(streams_of[3], (SAMPLES, TXT, D), 1.0, 6.0, ((0, 4), (2, 4))),
        "text_value": normal_values(streams_of[4], (SAMPLES, TXT, D), 1.0, 6.0, ((0, 4), (2, 4))),
        "grad_out": normal_values(streams_of[5], (SAMPLES, VTOK, D), 1.0, 6.0, ((0, 4), (1, 2), (2, 4))),
        "gate": jnp.clip(0.5 + 1.0 * jax.random.uniform(streams_of[6], (SAMPLES, D), jnp.float32) ** steps_of(streams_of[6], (SAMPLES, D), ((0, 4),), -0.2, 0.2), 0.5, 1.5).astype(jnp.bfloat16),
        "out_weight": normal_values(streams_of[7], (D, D), D ** -0.5, 0.109375, ((0, 4), (1, 4))),
        "windows": draw_windows(jax.random.fold_in(streams_of[11], 71), 0),
        "tile_map": draw_tile_map(jax.random.fold_in(streams_of[11], 71), 0),
        "text_count": place_ends(jax.random.randint(streams_of[10], (SAMPLES,), 1, TXT + 1), jax.random.fold_in(streams_of[10], 1), 1, TXT).astype(jnp.int32),
    }


def window_mask(own_map, side_maps, valid, spans, text_live):
    reach = jnp.abs(jnp.arange(3, dtype=jnp.int32) - 1)
    near_time = reach[None, :, None] <= spans[:, 0][:, None, None]
    near_space = jnp.abs(own_map[:, None, None] - side_maps[None, :, :]) <= spans[:, 1][:, None, None]
    allowed = near_time & near_space & valid[None, :, None]
    count = own_map.shape[0]
    tiles = allowed.reshape(count, 3 * count)
    video = jnp.broadcast_to(tiles[:, None, :, None], (count, TILE, 3 * count, TILE))
    video = video.reshape(count * TILE, 3 * count * TILE)
    text = jnp.broadcast_to(text_live[None, :], (count * TILE, text_live.shape[0]))
    return jnp.concatenate([video, text], axis=1)


def tile_attention(query, keys, values, grad_attn, allowed):
    factor = HD ** -0.5
    scores = factor * jnp.dot(query, keys.T, preferred_element_type=jnp.float32)
    scores = jnp.where(allowed, scores, -1e30)
    top = jnp.max(scores, axis=1, keepdims=True)
    weights = jnp.exp(scores - top)
    weights = weights / jnp.sum(weights, axis=1, keepdims=True)
    probs = weights.astype(jnp.bfloat16)
    attended = jnp.dot(probs, values, preferred_element_type=jnp.float32).astype(jnp.bfloat16)
    delta = jnp.sum(grad_attn.astype(jnp.float32) * attended.astype(jnp.float32), axis=1, keepdims=True)
    grad_probs = jnp.dot(grad_attn, values.T, preferred_element_type=jnp.float32)
    grad_scores = (weights * (grad_probs - delta)).astype(jnp.bfloat16)
    grad_query = factor * jnp.dot(grad_scores, keys, preferred_element_type=jnp.float32)
    grad_keys = factor * jnp.dot(grad_scores.T, query, preferred_element_type=jnp.float32)
    grad_values = jnp.dot(probs.T, grad_attn, preferred_element_type=jnp.float32)
    return attended, grad_query, grad_keys, grad_values


def gather_back(parts, slabs, tok):
    video = parts[:, :3 * tok].reshape(slabs, 3, tok, HD)
    empty = jnp.zeros((1, tok, HD), jnp.float32)
    total = video[:, 1] + jnp.concatenate([video[1:, 0], empty], axis=0)
    total = total + jnp.concatenate([empty, video[:-1, 2]], axis=0)
    return total.reshape(slabs * tok, HD), jnp.sum(parts[:, 3 * tok:], axis=0)


def reference(query, key, value, text_key, text_value, grad_out, gate, out_weight, windows, tile_map, text_count):
    slabs = N_SP
    tok = TILE * TILES_DEV
    heads = D // HD
    blank = jnp.zeros((1, TILES_DEV), jnp.int32)
    padded_map = jnp.concatenate([blank, tile_map.astype(jnp.int32), blank], axis=0)
    weight_grad = jnp.zeros((D, D), jnp.float32)
    outs = [[], [], [], [], []]
    for sample in range(SAMPLES):
        scaled = (grad_out[sample].astype(jnp.float32) * gate[sample].astype(jnp.float32)[None, :]).astype(jnp.bfloat16)
        grad_attn = jnp.dot(scaled, out_weight.T, preferred_element_type=jnp.float32).astype(jnp.bfloat16)
        text_live = jnp.arange(TXT, dtype=jnp.int32) < text_count[sample]

        def one_head(head):
            start = (head * HD).astype(jnp.int32)

            def cut(array):
                return lax.dynamic_slice_in_dim(array, start, HD, 1)

            queries = cut(query[sample]).reshape(slabs, tok, HD)
            grads = cut(grad_attn).reshape(slabs, tok, HD)
            zero_slab = jnp.zeros((1, tok, HD), jnp.bfloat16)
            keys = jnp.concatenate([zero_slab, cut(key[sample]).reshape(slabs, tok, HD), zero_slab], axis=0)
            vals = jnp.concatenate([zero_slab, cut(value[sample]).reshape(slabs, tok, HD), zero_slab], axis=0)
            text_k = cut(text_key[sample])
            text_v = cut(text_value[sample])

            def one_slab(slab):
                slab = slab.astype(jnp.int32)
                near_k = lax.dynamic_slice_in_dim(keys, slab, 3, 0).reshape(3 * tok, HD)
                near_v = lax.dynamic_slice_in_dim(vals, slab, 3, 0).reshape(3 * tok, HD)
                all_k = jnp.concatenate([near_k, text_k], axis=0)
                all_v = jnp.concatenate([near_v, text_v], axis=0)
                own_map = lax.dynamic_index_in_dim(tile_map.astype(jnp.int32), slab, 0, keepdims=False)
                side_maps = lax.dynamic_slice_in_dim(padded_map, slab, 3, 0)
                others = slab + jnp.arange(3, dtype=jnp.int32) - 1
                valid = (others >= 0) & (others < slabs)
                spans = lax.dynamic_slice_in_dim(windows.astype(jnp.int32), slab * TILES_DEV, TILES_DEV, 0)
                allowed = window_mask(own_map, side_maps, valid, spans, text_live)
                qs = lax.dynamic_index_in_dim(queries, slab, 0, keepdims=False)
                gs = lax.dynamic_index_in_dim(grads, slab, 0, keepdims=False)
                return tile_attention(qs, all_k, all_v, gs, allowed)

            attended, grad_q, grad_k, grad_v = lax.map(one_slab, jnp.arange(slabs, dtype=jnp.int32))
            video_k, text_gk = gather_back(grad_k, slabs, tok)
            video_v, text_gv = gather_back(grad_v, slabs, tok)
            return attended.reshape(slabs * tok, HD), grad_q.reshape(slabs * tok, HD), video_k, video_v, text_gk, text_gv

        results = lax.map(one_head, jnp.arange(heads, dtype=jnp.int32))

        def joined(stacked):
            return jnp.transpose(stacked, (1, 0, 2)).reshape(stacked.shape[1], D)

        attended = joined(results[0])
        weight_grad = weight_grad + jnp.dot(attended.T, scaled, preferred_element_type=jnp.float32)
        for place in range(5):
            outs[place].append(joined(results[place + 1]).astype(jnp.bfloat16))
    stacked = [jnp.stack(items, axis=0) for items in outs]
    return stacked[0], stacked[1], stacked[2], stacked[3], stacked[4], weight_grad
```

```python
import functools

import jax
import jax.numpy as jnp
from jax import lax
from jax.experimental import pallas as pl
from jax.experimental.pallas import tpu as pltpu
from jax.sharding import PartitionSpec as P

HD = 128
GROUPS = 2


NT = (((1,), (1,)), ((), ()))
NN = (((1,), (0,)), ((), ()))
TN = (((0,), (0,)), ((), ()))


def mm(a, b, dims):
    return lax.dot_general(a, b, dims, preferred_element_type=jnp.float32)


def ring_gather(block, axis):
    n = lax.axis_size(axis)
    rel = [block] + [None] * (n - 1)
    up = [(i, (i + 1) % n) for i in range(n)]
    down = [((i + 1) % n, i) for i in range(n)]
    ahead = behind = block
    for step in range(1, (n - 1) // 2 + 1):
        ahead = lax.ppermute(ahead, axis, down)
        behind = lax.ppermute(behind, axis, up)
        rel[step] = ahead
        rel[n - step] = behind
    if n % 2 == 0:
        half = block.shape[0] // 2
        first = lax.ppermute(ahead[:half], axis, down)
        second = lax.ppermute(behind[half:], axis, up)
        rel[n // 2] = jnp.concatenate([first, second], axis=0)
    return rel


def xor_route(axis, bit):
    n = lax.axis_size(axis)
    return [(i, i ^ bit) for i in range(n)]


def bits_of(n):
    return [1 << b for b in range(n.bit_length() - 1)]


def xor_gather(block, axis):
    n = lax.axis_size(axis)
    rel = {0: block}
    for bit in reversed(bits_of(n)):
        got = {d | bit: lax.ppermute(b, axis, xor_route(axis, bit)) for d, b in rel.items()}
        rel.update(got)
    return [rel[d] for d in range(n)]


def grad_attn_kernel(n_tp, n_dp, idx_ref, *refs):
    s_refs = refs[:n_tp]
    w_refs = refs[n_tp : n_tp + n_dp]
    nat_ref, ga_ref, acc_ref = refs[n_tp + n_dp :]
    me_tp = idx_ref[0]
    me_dp = idx_ref[1]
    w = s_refs[0].shape[1]
    for j in range(n_tp):
        nat_ref[lax.rem(me_tp + j, n_tp)] = s_refs[j][...]
    r = w_refs[0].shape[1] // w
    acc = None
    for d in range(n_dp):
        for piece in range(r):
            s = nat_ref[(me_dp ^ d) * r + piece]
            term = mm(s, w_refs[d][:, piece * w : (piece + 1) * w], NT)
            if d == 0 and piece == 0:
                acc_ref[...] = term
            else:
                acc_ref[...] += term
    ga_ref[...] = acc_ref[...].astype(jnp.bfloat16)


def grad_attn_call(index, s_rel, w_rel):
    tok, w = s_rel[0].shape
    rows = w_rel[0].shape[0]
    n_tp, n_dp = len(s_rel), len(w_rel)
    vm = pl.BlockSpec(memory_space=pltpu.VMEM)
    return pl.pallas_call(
        functools.partial(grad_attn_kernel, n_tp, n_dp),
        out_shape=(
            jax.ShapeDtypeStruct((n_tp, tok, w), jnp.bfloat16),
            jax.ShapeDtypeStruct((tok, rows), jnp.bfloat16),
        ),
        in_specs=[pl.BlockSpec(memory_space=pltpu.SMEM)] + [vm] * (n_tp + n_dp),
        out_specs=(vm, vm),
        scratch_shapes=[pltpu.VMEM((tok, rows), jnp.float32)],
        cost_estimate=pl.CostEstimate(
            flops=2 * tok * rows * n_tp * w, bytes_accessed=12 << 20, transcendentals=0
        ),
        name="grad_attn",
    )(index, *s_rel, *w_rel)


def attention_kernel(count, nk, q_ref, ga_ref, bias_ref, *refs):
    k_refs = refs[:nk]
    v_refs = refs[nk : 2 * nk]
    at_ref, gq_ref = refs[2 * nk : 2 * nk + 2]
    gk_refs = refs[2 * nk + 2 : 3 * nk + 2]
    gv_refs = refs[3 * nk + 2 : 4 * nk + 2]
    factor = HD ** (-0.5)
    tok = q_ref.shape[0]
    tile = tok // count
    keys = jnp.concatenate([r[...] for r in k_refs], axis=0)
    vals = jnp.concatenate([r[...] for r in v_refs], axis=0)
    gk_sum = gv_sum = None
    for t in range(count):
        rows = slice(t * tile, (t + 1) * tile)
        q = q_ref[rows, :]
        ga = ga_ref[rows, :]
        scores = factor * mm(keys, q, NT) + bias_ref[t]
        top = jnp.max(scores, axis=0, keepdims=True)
        weights = jnp.exp(scores - top)
        total = jnp.sum(weights, axis=0, keepdims=True)
        weights = weights * (1.0 / total)
        probs = weights.astype(jnp.bfloat16)
        att = mm(vals, probs, TN).astype(jnp.bfloat16)
        at_ref[:, rows] = att
        ga_t = ga.astype(jnp.float32).T
        delta = jnp.sum(ga_t * att.astype(jnp.float32), axis=0, keepdims=True)
        gp = mm(vals, ga, NT)
        gs = (weights * (gp - delta)).astype(jnp.bfloat16)
        gq = factor * mm(keys, gs, TN)
        gq_ref[rows, :] = gq.T.astype(jnp.bfloat16)
        gk = factor * mm(gs, q, NN)
        gv = mm(probs, ga, NN)
        gk_sum = gk if t == 0 else gk_sum + gk
        gv_sum = gv if t == 0 else gv_sum + gv
    at = 0
    for i in range(nk):
        n = gk_refs[i].shape[0]
        gk_refs[i][...] = gk_sum[at : at + n].astype(gk_refs[i].dtype)
        gv_refs[i][...] = gv_sum[at : at + n].astype(gv_refs[i].dtype)
        at += n


def attention_call(first, heads, count, q, ga, bias, ks, vs):
    tok = q.shape[0]
    nk = len(ks)

    def head(n):
        return pl.BlockSpec((n, HD), lambda h: (0, first + h))

    def out(n):
        return pl.BlockSpec((n, HD), lambda h: (0, h))

    sizes = [k.shape[0] for k in ks]
    kinds = [jnp.float32 if i == 0 else jnp.bfloat16 for i in range(nk)]
    kinds[-1] = jnp.float32
    total = sum(sizes)
    width = heads * HD
    grads = [jax.ShapeDtypeStruct((n, width), kind) for n, kind in zip(sizes, kinds)]
    return pl.pallas_call(
        functools.partial(attention_kernel, count, nk),
        grid=(heads,),
        out_shape=[
            jax.ShapeDtypeStruct((width, tok), jnp.bfloat16),
            jax.ShapeDtypeStruct((tok, width), jnp.bfloat16),
        ]
        + grads
        + grads,
        in_specs=[head(tok), head(tok), pl.BlockSpec(memory_space=pltpu.VMEM)]
        + [head(n) for n in sizes]
        + [head(n) for n in sizes],
        out_specs=[pl.BlockSpec((HD, tok), lambda h: (h, 0)), out(tok)]
        + [out(n) for n in sizes]
        + [out(n) for n in sizes],
        cost_estimate=pl.CostEstimate(
            flops=heads * 20 * tok * total * HD,
            bytes_accessed=heads * 4 << 20,
            transcendentals=heads * tok * total,
        ),
        name="attention",
    )(q, ga, bias, *ks, *vs)


def weight_kernel(n_dp, groups, idx_ref, nat_ref, *refs):
    at_refs = refs[:groups]
    outs = refs[groups:]
    me_dp = idx_ref[1]
    w = nat_ref.shape[2]
    r = outs[0].shape[1] // w
    for d in range(n_dp):
        for piece in range(r):
            s = nat_ref[(me_dp ^ d) * r + piece]
            row = 0
            for at in at_refs:
                n = at.shape[0]
                outs[d][row : row + n, piece * w : (piece + 1) * w] = mm(at[...], s, NN).astype(
                    outs[d].dtype
                )
                row += n


def weight_call(index, nat, ats, n_dp):
    n_tp, tok, w = nat.shape
    rows = sum(a.shape[0] for a in ats)
    cols = n_tp * w // n_dp
    vm = pl.BlockSpec(memory_space=pltpu.VMEM)
    return pl.pallas_call(
        functools.partial(weight_kernel, n_dp, len(ats)),
        out_shape=[
            jax.ShapeDtypeStruct((rows, cols), jnp.bfloat16 if d & 1 else jnp.float32)
            for d in range(n_dp)
        ],
        in_specs=[pl.BlockSpec(memory_space=pltpu.SMEM)] + [vm] * (1 + len(ats)),
        out_specs=[vm] * n_dp,
        cost_estimate=pl.CostEstimate(
            flops=2 * tok * rows * n_tp * w, bytes_accessed=16 << 20, transcendentals=0
        ),
        name="weight",
    )(index, nat, *ats)


def total_over(block, axis):
    for bit in bits_of(lax.axis_size(axis)):
        got = lax.ppermute(block.astype(jnp.bfloat16), axis, xor_route(axis, bit))
        block = block + got.astype(jnp.float32)
    return block


VMEM = 67043328


def copy_kernel(n, *refs):
    srcs, dsts, sem = refs[:n], refs[n : 2 * n], refs[2 * n]
    copies = []
    for src, dst in zip(srcs, dsts):
        pieces = 4 if src.dtype == jnp.float32 else 1
        rows = src.shape[0] // pieces
        for i in range(pieces):
            at = pl.ds(i * rows, rows)
            copies.append(pltpu.make_async_copy(src.at[at], dst.at[at], sem.at[len(copies)]))
    for c in copies:
        c.start()
    for c in copies:
        c.wait()


def copy_call(arrays):
    n = len(arrays)
    return pl.pallas_call(
        functools.partial(copy_kernel, n),
        out_shape=[jax.ShapeDtypeStruct(a.shape, a.dtype) for a in arrays],
        in_specs=[pl.BlockSpec(memory_space=pltpu.VMEM)] * n,
        out_specs=[pl.BlockSpec(memory_space=pltpu.HBM)] * n,
        scratch_shapes=[pltpu.SemaphoreType.DMA((4 * n,))],
        compiler_params=pltpu.CompilerParams(vmem_limit_bytes=4 << 20),
        name="results",
    )(*arrays)


MESH = pl.DeviceIdType.MESH


def mega_kernel(
    count,
    n_tp,
    n_dp,
    q_hbm,
    k_hbm,
    v_hbm,
    tk_hbm,
    tv_hbm,
    s_hbm,
    w_hbm,
    gate_hbm,
    windows_hbm,
    map_hbm,
    live_hbm,
    gq_ref,
    gk_ref,
    gv_ref,
    gtk_ref,
    gtv_ref,
    gw_ref,
    q_ref,
    gate_ref,
    windows_ref,
    map_ref,
    live_ref,
    keys,
    vals,
    q_far,
    ga_own,
    ga_far,
    win_own,
    win_far,
    raw,
    nat,
    w_all,
    acc,
    att_t,
    weights_s,
    gk_sum,
    gv_sum,
    parts,
    outgoing,
    incoming,
    last_out,
    last_in,
    x_out,
    x_in,
    ls,
    xs,
    xr,
    ws,
    wr,
    us,
    ur,
    ds,
    dr,
    ps,
    pr,
    ys,
    yr,
    gs_sem,
    gr_sem,
):
    factor = HD ** (-0.5)
    bf16, f32 = jnp.bfloat16, jnp.float32
    tok, width = q_ref.shape
    text = tk_hbm.shape[0]
    heads = width // HD
    chunks = 2 * heads
    step_rows = width // chunks
    tile = tok // count
    near = tok + text
    w = raw.shape[2]
    half = tok // 2
    me_sp = lax.axis_index("sp")
    me_dp = lax.axis_index("dp")
    me_tp = lax.axis_index("tp")
    far_sp = 1 - me_sp
    core_bit, top_bit = bits_of(n_dp)
    core_peer, top_peer = {"dp": me_dp ^ core_bit}, {"dp": me_dp ^ top_bit}
    sp_far = {"sp": far_sp}
    has_up = me_tp + 1 < n_tp
    has_down = me_tp >= 1
    last = n_tp - 2

    barrier = pltpu.get_barrier_semaphore()
    for peer in (sp_far, core_peer, top_peer):
        pl.semaphore_signal(barrier, inc=1, device_id=peer, device_id_type=MESH)

    @pl.when(has_up)
    def _():
        pl.semaphore_signal(barrier, inc=1, device_id={"tp": me_tp + 1}, device_id_type=MESH)

    @pl.when(has_down)
    def _():
        pl.semaphore_signal(barrier, inc=1, device_id={"tp": me_tp - 1}, device_id_type=MESH)

    loads = [
        pltpu.make_async_copy(a, b, ls.at[i])
        for i, (a, b) in enumerate(
            [
                (s_hbm, raw.at[me_tp]),
                (k_hbm, keys.at[pl.ds(0, tok)]),
                (w_hbm, w_all.at[me_dp]),
                (v_hbm, vals.at[pl.ds(0, tok)]),
                (q_hbm, q_ref),
                (gate_hbm, gate_ref),
                (windows_hbm, windows_ref),
                (tk_hbm, keys.at[pl.ds(tok, text)]),
                (tv_hbm, vals.at[pl.ds(tok, text)]),
                (map_hbm, map_ref),
                (live_hbm, live_ref),
            ]
        )
    ]
    for c in loads:
        c.start()
    pl.semaphore_wait(barrier, 3 + jnp.where(has_up, 1, 0) + jnp.where(has_down, 1, 0))

    def remote(src, dst, send, recv, where):
        return pltpu.make_async_remote_copy(
            src_ref=src,
            dst_ref=dst,
            send_sem=send,
            recv_sem=recv,
            device_id=where,
            device_id_type=MESH,
        )

    def halves(n):
        return [pl.ds(0, n // 2), pl.ds(n // 2, n // 2)]

    x_copies = [
        remote(win_own, win_far, xs.at[0], xr.at[0], sp_far),
        remote(keys.at[pl.ds(0, tok)], keys.at[pl.ds(near, tok)], xs.at[1], xr.at[1], sp_far),
        remote(vals.at[pl.ds(0, tok)], vals.at[pl.ds(near, tok)], xs.at[2], xr.at[2], sp_far),
        remote(q_ref, q_far, xs.at[3], xr.at[3], sp_far),
    ] + [
        remote(ga_own.at[rows], ga_far.at[rows], xs.at[4 + i], xr.at[4 + i], sp_far)
        for i, rows in enumerate(halves(tok))
    ]

    w_core = remote(w_all.at[me_dp], w_all.at[me_dp], ws.at[0], wr.at[0], core_peer)
    w_top = [
        remote(w_all.at[me_dp, rows], w_all.at[me_dp, rows], ws.at[1 + i], wr.at[1 + i], top_peer)
        for i, rows in enumerate(halves(width))
    ]
    w_relay = [
        remote(
            w_all.at[me_dp ^ top_bit, rows],
            w_all.at[me_dp ^ top_bit, rows],
            ws.at[3 + i],
            wr.at[3 + i],
            core_peer,
        )
        for i, rows in enumerate(halves(width))
    ]

    def up_copy(step, i):
        ref = raw.at[me_tp - step, halves(tok)[i]]
        return remote(ref, ref, us.at[step, i], ur.at[step, i], {"tp": me_tp + 1})

    def down_copy(step, i):
        ref = raw.at[me_tp + step, halves(tok)[i]]
        return remote(ref, ref, ds.at[step, i], dr.at[step, i], {"tp": me_tp - 1})

    def up_sends(step):
        return has_up & (me_tp >= step)

    def down_sends(step):
        return has_down & (me_tp + step < n_tp)

    def start_z(step, i):
        @pl.when(up_sends(step))
        def _():
            up_copy(step, i).start()

        @pl.when(down_sends(step))
        def _():
            down_copy(step, i).start()

    def arrived(step, i):
        @pl.when(me_tp >= step + 1)
        def _():
            ref = raw.at[me_tp - 1 - step, halves(tok)[i]]
            remote(ref, ref, us.at[step, i], ur.at[step, i], {"tp": me_tp - 1}).wait_recv()

        @pl.when(me_tp + 1 + step < n_tp)
        def _():
            ref = raw.at[me_tp + 1 + step, halves(tok)[i]]
            remote(ref, ref, ds.at[step, i], dr.at[step, i], {"tp": me_tp + 1}).wait_recv()

    def relay(step, i):
        arrived(step, i)
        if step + 1 < n_tp - 1:
            start_z(step + 1, i)

    def each_block(step, act):
        def side(i, carry):
            block = me_tp + (2 * i - 1) * (step + 1)

            @pl.when((block >= 0) & (block < n_tp))
            def _():
                act(block)

            return carry

        lax.fori_loop(0, 2, side, 0)

    loads[0].wait()
    for i in range(2):
        start_z(0, i)
    loads[1].wait()
    x_copies[1].start()
    loads[2].wait()
    for c in w_top:
        c.start()
    w_core.start()
    loads[3].wait()
    x_copies[2].start()
    loads[4].wait()
    x_copies[3].start()
    loads[6].wait()
    win_own[:count, :2] = windows_ref[...]
    x_copies[0].start()
    for i in (5, 7, 8, 9, 10):
        loads[i].wait()

    def scale(block, rows=slice(None)):
        gate = gate_ref[:, pl.ds(pl.multiple_of(block * w, HD), w)].astype(f32)
        nat[block, rows] = (raw[block, rows].astype(f32) * gate).astype(bf16)

    def add_block(block):
        acc[...] += mm(nat[block], w_all[block], NT)

    def p_copy(block):
        slot = lax.div(block, 2)
        return remote(outgoing.at[slot], incoming.at[slot], ps.at[slot], pr.at[slot], core_peer)

    def part(block):
        parts[block] = mm(att_t[...], nat[block], NN)

        @pl.when(lax.rem(block + me_dp, 2) == 1)
        def _():
            outgoing[lax.div(block, 2)] = parts[block].astype(bf16)
            p_copy(block).start()

    def bias_of(vis, t, far):
        owner = far_sp if far else me_sp
        place = map_ref[t, owner]

        def span(slab):
            apart = jnp.abs(owner - slab)
            spans = []
            for j in range(count):
                distance = jnp.abs(place - map_ref[j, slab])
                seen = (vis[t : t + 1, 0:1] >= apart) & (vis[t : t + 1, 1:2] >= distance)
                value = jnp.where(seen, 0.0, -1e30).astype(f32)
                spans.append(jnp.broadcast_to(value, (tile, 1)))
            return spans

        place_of = lax.broadcasted_iota(jnp.int32, (text, 1), 0)
        words = jnp.where(place_of < live_ref[0], 0.0, -1e30).astype(f32)
        return jnp.concatenate(span(me_sp) + [words] + span(far_sp), axis=0)

    def soft(q, h_cols, bias):
        scores = factor * mm(keys[:, h_cols], q, NT) + bias
        top = jnp.max(scores, axis=0, keepdims=True)
        weights = jnp.exp(scores - top)
        total = jnp.sum(weights, axis=0, keepdims=True)
        return weights * (1.0 / total)

    def cols_of(h):
        return pl.ds(pl.multiple_of(h * HD, HD), HD)

    def delta_of(ga, att):
        return jnp.sum(ga.astype(f32).T * att.astype(f32), axis=0, keepdims=True)

    def rows_of(t):
        return slice(t * tile, (t + 1) * tile)

    def chunk_rows(h):
        return pl.ds(pl.multiple_of(h * step_rows, step_rows), step_rows)

    def y_copy(h):
        rows = chunk_rows(h)
        return remote(last_out.at[rows], last_in.at[rows], ys.at[h], yr.at[h], top_peer)

    def g_copy(h):
        rows = chunk_rows(h)
        return remote(x_out.at[rows], x_in.at[rows], gs_sem.at[h], gr_sem.at[h], sp_far)

    scale(me_tp)
    relay(0, 0)
    relay(0, 1)
    each_block(0, scale)
    x_copies[1].wait_recv()

    def forward(h, carry):
        c = cols_of(h)
        for t in range(count):
            rows = rows_of(t)
            weights_s[h, :, rows] = soft(q_ref[rows, c], c, bias_of(win_own, t, False))
        return carry

    lax.fori_loop(0, heads, forward, 0)
    w_top[0].wait_recv()
    w_relay[0].start()
    relay(1, 0)
    relay(1, 1)
    for step in range(2, last):
        for i in range(2):
            relay(step, i)
    w_top[1].wait_recv()
    w_relay[1].start()
    x_copies[2].wait_recv()

    def attend(h, carry):
        c = cols_of(h)
        att_t[c, :] = mm(vals[:, c], weights_s[h].astype(bf16), TN).astype(bf16)
        return carry

    lax.fori_loop(0, heads, attend, 0)
    part(me_tp)
    each_block(0, part)
    for step in range(1, last):
        each_block(step, scale)
        each_block(step, part)
    w_core.wait_recv()
    for c in w_relay:
        c.wait_recv()
    acc[...] = mm(nat[me_tp], w_all[me_tp], NT)
    for step in range(last):
        each_block(step, add_block)

    away = me_dp ^ top_bit

    def send_top():
        p_copy(away).wait_recv()

        def chunk(h, carry):
            rows = chunk_rows(h)
            both = parts[away, rows, :] + incoming[lax.div(away, 2), rows, :].astype(f32)
            last_out[rows, :] = both.astype(bf16)
            y_copy(h).start()
            return carry

        lax.fori_loop(0, chunks, chunk, 0)

    late = jnp.abs(away - me_tp) == n_tp - 1

    @pl.when(jnp.logical_not(late))
    def _():
        send_top()

    for i in range(2):
        rows = slice(i * half, (i + 1) * half)
        arrived(last, i)

        def add_half(block):
            scale(block, rows)
            acc[rows] += mm(nat[block, rows], w_all[block], NT)

        each_block(last, add_half)
        ga_own[rows] = acc[rows].astype(bf16)
        x_copies[4 + i].start()
    each_block(last, part)

    def backward(h, carry):
        c = cols_of(h)
        for t in range(count):
            rows = rows_of(t)
            q = q_ref[rows, c]
            ga = ga_own[rows, c]
            weights = weights_s[h, :, rows]
            delta = delta_of(ga, att_t[c, rows])
            gp = mm(vals[:, c], ga, NT)
            gs = (weights * (gp - delta)).astype(bf16)
            gq_ref[rows, c] = (factor * mm(keys[:, c], gs, TN)).T.astype(bf16)
            gk = mm(gs[:near], q, NN)
            gv = mm(weights[:near].astype(bf16), ga, NN)
            if t == 0:
                gk_sum[:, c] = gk
                gv_sum[:, c] = gv
            else:
                gk_sum[:, c] += gk
                gv_sum[:, c] += gv

        @pl.when((h == heads // 2) & late)
        def _():
            send_top()

        return carry

    lax.fori_loop(0, heads, backward, 0)
    p_copy(me_dp).wait_recv()

    def pass_on(h):
        y_copy(h).wait_recv()
        rows = chunk_rows(h)
        mine = parts[me_dp, rows, :] + incoming[lax.div(me_dp, 2), rows, :].astype(f32)
        total = mine + last_in[rows, :].astype(f32)
        gw_ref[rows, :] = total
        x_out[rows, :] = total.astype(bf16)
        g_copy(h).start()

    x_copies[0].wait_recv()
    x_copies[3].wait_recv()

    def far_soft(h, carry):
        c = cols_of(h)
        for t in range(count):
            rows = rows_of(t)
            weights = soft(q_far[rows, c], c, bias_of(win_far, t, True))
            weights_s[h, :, rows] = weights
            att_t[c, rows] = mm(vals[:, c], weights.astype(bf16), TN).astype(bf16)
        pass_on(h)
        return carry

    lax.fori_loop(0, heads, far_soft, 0)
    x_copies[4].wait_recv()
    x_copies[5].wait_recv()

    def far(h, carry):
        c = cols_of(h)
        gk_all = gk_sum[:, c]
        gv_all = gv_sum[:, c]
        for t in range(count):
            rows = rows_of(t)
            q = q_far[rows, c]
            ga = ga_far[rows, c]
            weights = weights_s[h, :near, rows]
            delta = delta_of(ga, att_t[c, rows])
            gp = mm(vals[:near, c], ga, NT)
            gs = (weights * (gp - delta)).astype(bf16)
            gk_all += mm(gs, q, NN)
            gv_all += mm(weights.astype(bf16), ga, NN)
        gk_ref[:, c] = (factor * gk_all[:tok]).astype(bf16)
        gtk_ref[:, c] = (factor * gk_all[tok:]).astype(bf16)
        gv_ref[:, c] = gv_all[:tok].astype(bf16)
        gtv_ref[:, c] = gv_all[tok:].astype(bf16)
        pass_on(heads + h)
        return carry

    lax.fori_loop(0, heads, far, 0)
    for c in x_copies:
        c.wait_send()
    for c in [w_core] + w_top + w_relay:
        c.wait_send()
    for slot in range(n_dp // 2):
        p_copy(2 * slot).wait_send()
    for step in range(n_tp - 1):
        for i in range(2):

            @pl.when(up_sends(step))
            def _():
                up_copy(step, i).wait_send()

            @pl.when(down_sends(step))
            def _():
                down_copy(step, i).wait_send()

    def finish(h, carry):
        rows = chunk_rows(h)
        g_copy(h).wait_recv()
        gw_ref[rows, :] += x_in[rows, :].astype(f32)
        g_copy(h).wait_send()
        y_copy(h).wait_send()
        return carry

    lax.fori_loop(0, chunks, finish, 0)


def mega_call(n_tp, n_dp, q, k, v, tk, tv, s, w, gate, windows, tile_map, text_count):
    tok, width = q.shape
    text = tk.shape[0]
    heads = width // HD
    cols = w.shape[1]
    total = 2 * tok + text
    near = tok + text
    count = tile_map.shape[0]
    pairs = n_dp // 2
    bf16, f32 = jnp.bfloat16, jnp.float32
    dma = pltpu.SemaphoreType.DMA
    shapes = [
        ((tok, width), bf16),
        ((tok, width), bf16),
        ((tok, width), bf16),
        ((text, width), bf16),
        ((text, width), bf16),
        ((width, cols), f32),
    ]
    small = [
        pltpu.VMEM((tok, width), bf16),
        pltpu.VMEM(gate.shape, bf16),
        pltpu.VMEM(windows.shape, jnp.int32),
        pltpu.SMEM(tile_map.shape, jnp.int32),
        pltpu.SMEM(text_count.shape, jnp.int32),
    ]
    scratch = [
        ((total, width), bf16),
        ((total, width), bf16),
        ((tok, width), bf16),
        ((tok, width), bf16),
        ((tok, width), bf16),
        ((count + -count % 8, HD), jnp.int32),
        ((count + -count % 8, HD), jnp.int32),
        ((n_tp, tok, s.shape[1]), bf16),
        ((n_tp, tok, s.shape[1]), bf16),
        ((n_dp, width, cols), bf16),
        ((tok, width), f32),
        ((width, tok), bf16),
        ((heads, total, tok), f32),
        ((near, width), f32),
        ((near, width), f32),
        ((n_dp, width, cols), f32),
        ((pairs, width, cols), bf16),
        ((pairs, width, cols), bf16),
        ((width, cols), bf16),
        ((width, cols), bf16),
        ((width, cols), bf16),
        ((width, cols), bf16),
    ]
    sems = [(11,), (6,), (6,), (5,), (5,)] + [(n_tp, 2)] * 4 + [(pairs,)] * 2 + [(2 * heads,)] * 4
    held = sum(jnp.dtype(b).itemsize * a[0] * a[1] for a, b in shapes)
    return pl.pallas_call(
        functools.partial(mega_kernel, count, n_tp, n_dp),
        out_shape=[pltpu.VMEM(a, b) for a, b in shapes],
        in_specs=[pl.BlockSpec(memory_space=pltpu.HBM)] * 11,
        out_specs=[pl.BlockSpec(memory_space=pltpu.VMEM)] * 6,
        scratch_shapes=small + [pltpu.VMEM(a, b) for a, b in scratch] + [dma(n) for n in sems],
        compiler_params=pltpu.CompilerParams(
            collective_id=0, has_side_effects=True, vmem_limit_bytes=VMEM - held - (1 << 20)
        ),
        name="attention_backward",
    )(q, k, v, tk, tv, s, w, gate, windows, tile_map, text_count)


def per_device(
    query,
    key,
    value,
    text_key,
    text_value,
    grad_out,
    gate,
    out_weight,
    windows,
    tile_map,
    text_count,
):
    q, k, v = query[0], key[0], value[0]
    tk, tv = text_key[0], text_value[0]
    tok, width = q.shape
    n_sp = lax.axis_size("sp")
    n_dp = lax.axis_size("dp")
    n_tp = lax.axis_size("tp")
    me_sp = lax.axis_index("sp")
    me_tp = lax.axis_index("tp")
    me_dp = lax.axis_index("dp")
    index = jnp.stack([me_tp, me_dp]).astype(jnp.int32)

    offsets = sorted({1 % n_sp, (n_sp - 1) % n_sp} - {0})

    def from_offset(block, offset):
        route = [((i + offset) % n_sp, i) for i in range(n_sp)]
        route = [(a, b) for a, b in route if abs(a - b) <= 1]
        return lax.ppermute(block, "sp", route)

    def to_offset(block, offset):
        route = [(i, (i + offset) % n_sp) for i in range(n_sp)]
        route = [(a, b) for a, b in route if abs(a - b) <= 1]
        return lax.ppermute(block, "sp", route)

    own_gate = lax.dynamic_slice_in_dim(gate[0], me_tp * width, width, 0)
    scaled = (grad_out[0].astype(jnp.float32) * own_gate.astype(jnp.float32)[None, :]).astype(
        jnp.bfloat16
    )
    own_map = lax.dynamic_index_in_dim(tile_map, me_sp, 0, keepdims=False)
    count = own_map.shape[0]
    tile = tok // count
    live = jnp.arange(tk.shape[0], dtype=jnp.int32) < text_count[0]

    def tiles_seen(o):
        other = lax.rem(me_sp + o, n_sp)
        apart = jnp.abs(other - me_sp)
        other_map = lax.dynamic_index_in_dim(tile_map, other, 0, keepdims=False)
        near_time = (apart <= windows[:, 0]) & (apart <= 1)
        near_space = jnp.abs(own_map[:, None] - other_map[None, :]) <= windows[:, 1][:, None]
        return near_time[:, None] & near_space

    if offsets == [n_sp - 1] and n_tp == n_dp and len(bits_of(n_dp)) == 2:
        outs = mega_call(
            n_tp,
            n_dp,
            q,
            k,
            v,
            tk,
            tv,
            grad_out[0],
            out_weight,
            gate,
            windows,
            tile_map.T,
            text_count,
        )
        outs = copy_call(outs)
        return tuple(o[None] for o in outs[:5]) + (outs[5],)

    near_k = [from_offset(k, o) for o in offsets]
    near_v = [from_offset(v, o) for o in offsets]

    s_rel = ring_gather(scaled, "tp")
    w_rel = xor_gather(out_weight, "dp")

    seen = [jnp.repeat(tiles_seen(o), tile, axis=1) for o in [0] + offsets]
    seen.append(jnp.broadcast_to(live[None, :], (count, tk.shape[0])))
    bias = jnp.where(jnp.concatenate(seen, axis=1), 0.0, -1e30).astype(jnp.float32)[:, :, None]

    nat, ga = grad_attn_call(index, s_rel, w_rel)

    heads = width // HD
    groups = GROUPS if heads % GROUPS == 0 else 1
    each = heads // groups
    ks = [k] + near_k + [tk]
    vs = [v] + near_v + [tv]
    nk = len(ks)
    ats, gqs, gks, gvs, gtk, gtv = [], [], [], [], [], []
    for g in range(groups):
        res = attention_call(g * each, each, count, q, ga, bias, ks, vs)
        at, gq = res[:2]
        gk, gv = list(res[2 : 2 + nk]), list(res[2 + nk :])
        ats.append(at)
        gqs.append(gq)
        own_k, own_v = gk[0], gv[0]
        for i, o in enumerate(offsets):
            own_k = own_k + to_offset(gk[1 + i], o).astype(jnp.float32)
            own_v = own_v + to_offset(gv[1 + i], o).astype(jnp.float32)
        gks.append(own_k)
        gvs.append(own_v)
        gtk.append(total_over(gk[-1], "sp"))
        gtv.append(total_over(gv[-1], "sp"))

    parts = dict(enumerate(weight_call(index, nat, ats, n_dp)))
    for bit in bits_of(n_dp):
        got = {
            d: lax.ppermute(parts[d | bit].astype(jnp.bfloat16), "dp", xor_route("dp", bit))
            for d in parts
            if not d & bit
        }
        parts = {d: parts[d].astype(jnp.float32) + got[d].astype(jnp.float32) for d in got}
    weight_grad = total_over(parts[0], "sp")

    def joined(pieces):
        return jnp.concatenate(pieces, axis=1).astype(jnp.bfloat16)[None]

    return (joined(gqs), joined(gks), joined(gvs), joined(gtk), joined(gtv), weight_grad)


def solution(mesh):
    placed = (
        P("dp", "sp", "tp"),
        P("dp", "sp", "tp"),
        P("dp", "sp", "tp"),
        P("dp", None, "tp"),
        P("dp", None, "tp"),
        P("dp", "sp", "tp"),
        P("dp", None),
        P("tp", "dp"),
        P("sp", None),
        P(),
        P("dp"),
    )
    return jax.shard_map(
        per_device,
        mesh=mesh,
        in_specs=placed,
        out_specs=(
            P("dp", "sp", "tp"),
            P("dp", "sp", "tp"),
            P("dp", "sp", "tp"),
            P("dp", None, "tp"),
            P("dp", None, "tp"),
            P("tp", "dp"),
        ),
        check_vma=False,
    )
```

```python
import functools

import jax
import jax.numpy as jnp
from jax import lax
from jax.experimental import pallas as pl
from jax.experimental.pallas import tpu as pltpu
from jax.sharding import PartitionSpec as P

HD = 128
GROUPS = 2
SHARE = 0.5


NT = (((1,), (1,)), ((), ()))
NN = (((1,), (0,)), ((), ()))
TN = (((0,), (0,)), ((), ()))


def mm(a, b, dims):
    return lax.dot_general(a, b, dims, preferred_element_type=jnp.float32)


def ring_gather(block, axis):
    n = lax.axis_size(axis)
    rel = [block] + [None] * (n - 1)
    up = [(i, (i + 1) % n) for i in range(n)]
    down = [((i + 1) % n, i) for i in range(n)]
    ahead = behind = block
    for step in range(1, (n - 1) // 2 + 1):
        ahead = lax.ppermute(ahead, axis, down)
        behind = lax.ppermute(behind, axis, up)
        rel[step] = ahead
        rel[n - step] = behind
    if n % 2 == 0:
        half = block.shape[0] // 2
        first = lax.ppermute(ahead[:half], axis, down)
        second = lax.ppermute(behind[half:], axis, up)
        rel[n // 2] = jnp.concatenate([first, second], axis=0)
    return rel


def xor_route(axis, bit):
    n = lax.axis_size(axis)
    return [(i, i ^ bit) for i in range(n)]


def bits_of(n):
    return [1 << b for b in range(n.bit_length() - 1)]


def xor_gather(block, axis):
    n = lax.axis_size(axis)
    rel = {0: block}
    for bit in reversed(bits_of(n)):
        got = {d | bit: lax.ppermute(b, axis, xor_route(axis, bit)) for d, b in rel.items()}
        rel.update(got)
    return [rel[d] for d in range(n)]


def grad_attn_kernel(n_tp, n_dp, idx_ref, *refs):
    s_refs = refs[:n_tp]
    w_refs = refs[n_tp : n_tp + n_dp]
    nat_ref, ga_ref, acc_ref = refs[n_tp + n_dp :]
    me_tp = idx_ref[0]
    me_dp = idx_ref[1]
    w = s_refs[0].shape[1]
    for j in range(n_tp):
        nat_ref[lax.rem(me_tp + j, n_tp)] = s_refs[j][...]
    r = w_refs[0].shape[1] // w
    acc = None
    for d in range(n_dp):
        for piece in range(r):
            s = nat_ref[(me_dp ^ d) * r + piece]
            term = mm(s, w_refs[d][:, piece * w : (piece + 1) * w], NT)
            if d == 0 and piece == 0:
                acc_ref[...] = term
            else:
                acc_ref[...] += term
    ga_ref[...] = acc_ref[...].astype(jnp.bfloat16)


def grad_attn_call(index, s_rel, w_rel):
    tok, w = s_rel[0].shape
    rows = w_rel[0].shape[0]
    n_tp, n_dp = len(s_rel), len(w_rel)
    vm = pl.BlockSpec(memory_space=pltpu.VMEM)
    return pl.pallas_call(
        functools.partial(grad_attn_kernel, n_tp, n_dp),
        out_shape=(
            jax.ShapeDtypeStruct((n_tp, tok, w), jnp.bfloat16),
            jax.ShapeDtypeStruct((tok, rows), jnp.bfloat16),
        ),
        in_specs=[pl.BlockSpec(memory_space=pltpu.SMEM)] + [vm] * (n_tp + n_dp),
        out_specs=(vm, vm),
        scratch_shapes=[pltpu.VMEM((tok, rows), jnp.float32)],
        cost_estimate=pl.CostEstimate(
            flops=2 * tok * rows * n_tp * w, bytes_accessed=12 << 20, transcendentals=0
        ),
        name="grad_attn",
    )(index, *s_rel, *w_rel)


def attention_kernel(count, nk, q_ref, ga_ref, bias_ref, *refs):
    k_refs = refs[:nk]
    v_refs = refs[nk : 2 * nk]
    at_ref, gq_ref = refs[2 * nk : 2 * nk + 2]
    gk_refs = refs[2 * nk + 2 : 3 * nk + 2]
    gv_refs = refs[3 * nk + 2 : 4 * nk + 2]
    factor = HD ** (-0.5)
    tok = q_ref.shape[0]
    tile = tok // count
    keys = jnp.concatenate([r[...] for r in k_refs], axis=0)
    vals = jnp.concatenate([r[...] for r in v_refs], axis=0)
    gk_sum = gv_sum = None
    for t in range(count):
        rows = slice(t * tile, (t + 1) * tile)
        q = q_ref[rows, :]
        ga = ga_ref[rows, :]
        scores = factor * mm(keys, q, NT) + bias_ref[t]
        top = jnp.max(scores, axis=0, keepdims=True)
        weights = jnp.exp(scores - top)
        total = jnp.sum(weights, axis=0, keepdims=True)
        weights = weights * (1.0 / total)
        probs = weights.astype(jnp.bfloat16)
        att = mm(vals, probs, TN).astype(jnp.bfloat16)
        at_ref[:, rows] = att
        ga_t = ga.astype(jnp.float32).T
        delta = jnp.sum(ga_t * att.astype(jnp.float32), axis=0, keepdims=True)
        gp = mm(vals, ga, NT)
        gs = (weights * (gp - delta)).astype(jnp.bfloat16)
        gq = factor * mm(keys, gs, TN)
        gq_ref[rows, :] = gq.T.astype(jnp.bfloat16)
        gk = factor * mm(gs, q, NN)
        gv = mm(probs, ga, NN)
        gk_sum = gk if t == 0 else gk_sum + gk
        gv_sum = gv if t == 0 else gv_sum + gv
    at = 0
    for i in range(nk):
        n = gk_refs[i].shape[0]
        gk_refs[i][...] = gk_sum[at : at + n].astype(gk_refs[i].dtype)
        gv_refs[i][...] = gv_sum[at : at + n].astype(gv_refs[i].dtype)
        at += n


def attention_call(first, heads, count, q, ga, bias, ks, vs):
    tok = q.shape[0]
    nk = len(ks)

    def head(n):
        return pl.BlockSpec((n, HD), lambda h: (0, first + h))

    def out(n):
        return pl.BlockSpec((n, HD), lambda h: (0, h))

    sizes = [k.shape[0] for k in ks]
    kinds = [jnp.float32 if i == 0 else jnp.bfloat16 for i in range(nk)]
    kinds[-1] = jnp.float32
    total = sum(sizes)
    width = heads * HD
    grads = [jax.ShapeDtypeStruct((n, width), kind) for n, kind in zip(sizes, kinds)]
    return pl.pallas_call(
        functools.partial(attention_kernel, count, nk),
        grid=(heads,),
        out_shape=[
            jax.ShapeDtypeStruct((width, tok), jnp.bfloat16),
            jax.ShapeDtypeStruct((tok, width), jnp.bfloat16),
        ]
        + grads
        + grads,
        in_specs=[head(tok), head(tok), pl.BlockSpec(memory_space=pltpu.VMEM)]
        + [head(n) for n in sizes]
        + [head(n) for n in sizes],
        out_specs=[pl.BlockSpec((HD, tok), lambda h: (h, 0)), out(tok)]
        + [out(n) for n in sizes]
        + [out(n) for n in sizes],
        cost_estimate=pl.CostEstimate(
            flops=heads * 20 * tok * total * HD,
            bytes_accessed=heads * 4 << 20,
            transcendentals=heads * tok * total,
        ),
        name="attention",
    )(q, ga, bias, *ks, *vs)


def weight_kernel(n_dp, groups, idx_ref, nat_ref, *refs):
    at_refs = refs[:groups]
    outs = refs[groups:]
    me_dp = idx_ref[1]
    w = nat_ref.shape[2]
    r = outs[0].shape[1] // w
    for d in range(n_dp):
        for piece in range(r):
            s = nat_ref[(me_dp ^ d) * r + piece]
            row = 0
            for at in at_refs:
                n = at.shape[0]
                outs[d][row : row + n, piece * w : (piece + 1) * w] = mm(at[...], s, NN).astype(
                    outs[d].dtype
                )
                row += n


def weight_call(index, nat, ats, n_dp):
    n_tp, tok, w = nat.shape
    rows = sum(a.shape[0] for a in ats)
    cols = n_tp * w // n_dp
    vm = pl.BlockSpec(memory_space=pltpu.VMEM)
    return pl.pallas_call(
        functools.partial(weight_kernel, n_dp, len(ats)),
        out_shape=[
            jax.ShapeDtypeStruct((rows, cols), jnp.bfloat16 if d & 1 else jnp.float32)
            for d in range(n_dp)
        ],
        in_specs=[pl.BlockSpec(memory_space=pltpu.SMEM)] + [vm] * (1 + len(ats)),
        out_specs=[vm] * n_dp,
        cost_estimate=pl.CostEstimate(
            flops=2 * tok * rows * n_tp * w, bytes_accessed=16 << 20, transcendentals=0
        ),
        name="weight",
    )(index, nat, *ats)


def total_over(block, axis):
    for bit in bits_of(lax.axis_size(axis)):
        got = lax.ppermute(block.astype(jnp.bfloat16), axis, xor_route(axis, bit))
        block = block + got.astype(jnp.float32)
    return block


VMEM = 67043328


def copy_kernel(n, *refs):
    srcs, dsts, sem = refs[:n], refs[n : 2 * n], refs[2 * n]
    copies = []
    for src, dst in zip(srcs, dsts):
        pieces = 4 if src.dtype == jnp.float32 else 1
        rows = src.shape[0] // pieces
        for i in range(pieces):
            at = pl.ds(i * rows, rows)
            copies.append(pltpu.make_async_copy(src.at[at], dst.at[at], sem.at[len(copies)]))
    for c in copies:
        c.start()
    for c in copies:
        c.wait()


def copy_call(arrays):
    n = len(arrays)
    return pl.pallas_call(
        functools.partial(copy_kernel, n),
        out_shape=[jax.ShapeDtypeStruct(a.shape, a.dtype) for a in arrays],
        in_specs=[pl.BlockSpec(memory_space=pltpu.VMEM)] * n,
        out_specs=[pl.BlockSpec(memory_space=pltpu.HBM)] * n,
        scratch_shapes=[pltpu.SemaphoreType.DMA((4 * n,))],
        compiler_params=pltpu.CompilerParams(vmem_limit_bytes=4 << 20),
        name="results",
    )(*arrays)


MESH = pl.DeviceIdType.MESH


def mega_kernel(
    count,
    n_tp,
    n_dp,
    q_hbm,
    k_hbm,
    v_hbm,
    tk_hbm,
    tv_hbm,
    s_hbm,
    w_hbm,
    gate_hbm,
    windows_hbm,
    map_hbm,
    live_hbm,
    gq_ref,
    gk_ref,
    gv_ref,
    gtk_ref,
    gtv_ref,
    gw_ref,
    q_ref,
    gate_ref,
    windows_ref,
    map_ref,
    live_ref,
    keys,
    vals,
    q_far,
    ga_own,
    ga_far,
    win_own,
    win_far,
    raw,
    nat,
    raw_far,
    w_all,
    acc,
    att_t,
    att_far,
    weights_s,
    weights_far,
    gk_sum,
    gv_sum,
    parts,
    outgoing,
    incoming,
    last_out,
    last_in,
    x_out,
    x_in,
    both_outgoing,
    both_incoming,
    both_out,
    both_in,
    ls,
    xs,
    xr,
    ws,
    wr,
    us,
    ur,
    ds,
    dr,
    fus,
    fur,
    fds,
    fdr,
    ps,
    pr,
    bps,
    bpr,
    ys,
    yr,
    bys,
    byr,
    gs_sem,
    gr_sem,
):
    factor = HD ** (-0.5)
    bf16, f32 = jnp.bfloat16, jnp.float32
    tok, width = q_ref.shape
    text = tk_hbm.shape[0]
    heads = width // HD
    chunks = heads
    step_rows = width // chunks
    early = heads // 2
    tile = tok // count
    near = tok + text
    w = raw.shape[2]
    half = tok // 2
    wide = raw_far.shape[2]
    me_sp = lax.axis_index("sp")
    me_dp = lax.axis_index("dp")
    me_tp = lax.axis_index("tp")
    far_sp = 1 - me_sp
    core_bit, top_bit = bits_of(n_dp)
    core_peer, top_peer = {"dp": me_dp ^ core_bit}, {"dp": me_dp ^ top_bit}
    sp_far = {"sp": far_sp}
    has_up = me_tp + 1 < n_tp
    has_down = me_tp >= 1
    last = n_tp - 2

    barrier = pltpu.get_barrier_semaphore()
    for peer in (sp_far, core_peer, top_peer):
        pl.semaphore_signal(barrier, inc=1, device_id=peer, device_id_type=MESH)

    @pl.when(has_up)
    def _():
        pl.semaphore_signal(barrier, inc=1, device_id={"tp": me_tp + 1}, device_id_type=MESH)

    @pl.when(has_down)
    def _():
        pl.semaphore_signal(barrier, inc=1, device_id={"tp": me_tp - 1}, device_id_type=MESH)

    loads = [
        pltpu.make_async_copy(a, b, ls.at[i])
        for i, (a, b) in enumerate(
            [
                (s_hbm, raw.at[me_tp]),
                (k_hbm, keys.at[pl.ds(0, tok)]),
                (w_hbm, w_all.at[me_dp]),
                (v_hbm, vals.at[pl.ds(0, tok)]),
                (q_hbm, q_ref),
                (gate_hbm, gate_ref),
                (windows_hbm, windows_ref),
                (tk_hbm, keys.at[pl.ds(tok, text)]),
                (tv_hbm, vals.at[pl.ds(tok, text)]),
                (map_hbm, map_ref),
                (live_hbm, live_ref),
            ]
        )
    ]
    for c in loads:
        c.start()
    pl.semaphore_wait(barrier, 3 + jnp.where(has_up, 1, 0) + jnp.where(has_down, 1, 0))

    def remote(src, dst, send, recv, where):
        return pltpu.make_async_remote_copy(
            src_ref=src,
            dst_ref=dst,
            send_sem=send,
            recv_sem=recv,
            device_id=where,
            device_id_type=MESH,
        )

    def halves(n):
        return [pl.ds(0, n // 2), pl.ds(n // 2, n // 2)]

    x_copies = [
        remote(win_own, win_far, xs.at[0], xr.at[0], sp_far),
        remote(keys.at[pl.ds(0, tok)], keys.at[pl.ds(near, tok)], xs.at[1], xr.at[1], sp_far),
        remote(vals.at[pl.ds(0, tok)], vals.at[pl.ds(near, tok)], xs.at[2], xr.at[2], sp_far),
        remote(
            q_ref.at[:, pl.ds(0, early * HD)],
            q_far.at[:, pl.ds(0, early * HD)],
            xs.at[3],
            xr.at[3],
            sp_far,
        ),
    ] + [
        remote(ga_own.at[rows], ga_far.at[rows], xs.at[4 + i], xr.at[4 + i], sp_far)
        for i, rows in enumerate(halves(tok))
    ]
    q_rest = pl.ds(early * HD, width - early * HD)
    x_copies.append(remote(q_ref.at[:, q_rest], q_far.at[:, q_rest], xs.at[6], xr.at[6], sp_far))
    grad_far = [
        remote(
            raw.at[me_tp, rows, pl.ds(0, wide)],
            raw_far.at[me_tp, rows],
            xs.at[7 + i],
            xr.at[7 + i],
            sp_far,
        )
        for i, rows in enumerate(halves(tok))
    ]

    w_core = remote(w_all.at[me_dp], w_all.at[me_dp], ws.at[0], wr.at[0], core_peer)
    w_top = [
        remote(w_all.at[me_dp, rows], w_all.at[me_dp, rows], ws.at[1 + i], wr.at[1 + i], top_peer)
        for i, rows in enumerate(halves(width))
    ]
    w_relay = [
        remote(
            w_all.at[me_dp ^ top_bit, rows],
            w_all.at[me_dp ^ top_bit, rows],
            ws.at[3 + i],
            wr.at[3 + i],
            core_peer,
        )
        for i, rows in enumerate(halves(width))
    ]

    near_line = (raw, us, ur, ds, dr)
    far_line = (raw_far, fus, fur, fds, fdr)

    def up_copy(line, step, i, block, where):
        ref = line[0].at[block, halves(tok)[i]]
        return remote(ref, ref, line[1].at[step, i], line[2].at[step, i], {"tp": where})

    def down_copy(line, step, i, block, where):
        ref = line[0].at[block, halves(tok)[i]]
        return remote(ref, ref, line[3].at[step, i], line[4].at[step, i], {"tp": where})

    def send_z(line, step, i, act):
        @pl.when(has_up & (me_tp >= step))
        def _():
            act(up_copy(line, step, i, me_tp - step, me_tp + 1))

        @pl.when(has_down & (me_tp + step < n_tp))
        def _():
            act(down_copy(line, step, i, me_tp + step, me_tp - 1))

    def start_z(line, step, i):
        send_z(line, step, i, lambda c: c.start())

    def relay(line, step, i):
        @pl.when(has_up & (me_tp >= step + 1))
        def _():
            up_copy(line, step, i, me_tp - 1 - step, me_tp - 1).wait_recv()
            up_copy(line, step + 1, i, me_tp - 1 - step, me_tp + 1).start()

        @pl.when(has_down & (me_tp + 1 + step < n_tp))
        def _():
            down_copy(line, step, i, me_tp + 1 + step, me_tp + 1).wait_recv()
            down_copy(line, step + 1, i, me_tp + 1 + step, me_tp - 1).start()

    def settle(line, step, i):
        @pl.when(jnp.logical_not(has_up) & (me_tp >= step + 1))
        def _():
            up_copy(line, step, i, me_tp - 1 - step, me_tp - 1).wait_recv()

        @pl.when(jnp.logical_not(has_down) & (me_tp + 1 + step < n_tp))
        def _():
            down_copy(line, step, i, me_tp + 1 + step, me_tp + 1).wait_recv()

    def each_block(step, act):
        def side(i, carry):
            block = me_tp + (2 * i - 1) * (step + 1)

            @pl.when((block >= 0) & (block < n_tp))
            def _():
                act(block)

            return carry

        lax.fori_loop(0, 2, side, 0)

    loads[0].wait()
    for i in range(2):
        start_z(near_line, 0, i)
    loads[1].wait()
    x_copies[1].start()
    loads[2].wait()
    for c in w_top:
        c.start()
    w_core.start()
    loads[3].wait()
    x_copies[2].start()
    loads[4].wait()
    x_copies[3].start()
    for c in grad_far:
        c.start()
    loads[6].wait()
    win_own[:count, :2] = windows_ref[...]
    x_copies[0].start()
    x_copies[6].start()
    for i in (5, 7, 8, 9, 10):
        loads[i].wait()

    def scale(block, rows=slice(None)):
        gate = gate_ref[:, pl.ds(pl.multiple_of(block * w, HD), w)].astype(f32)
        nat[block, rows] = (raw[block, rows].astype(f32) * gate).astype(bf16)

    def add_block(block):
        acc[...] += mm(nat[block], w_all[block], NT)

    def p_copy(block):
        slot = lax.div(block, 2)
        return remote(outgoing.at[slot], incoming.at[slot], ps.at[slot], pr.at[slot], core_peer)

    def part(block):
        parts[block] = mm(att_t[...], nat[block], NN)

        @pl.when(lax.rem(block + me_dp, 2) == 1)
        def _():
            outgoing[lax.div(block, 2)] = parts[block, :, wide:].astype(bf16)
            p_copy(block).start()

    def both_copy(block):
        slot = lax.div(block, 2)
        return remote(
            both_outgoing.at[slot], both_incoming.at[slot], bps.at[slot], bpr.at[slot], core_peer
        )

    def part_far(block):
        gate = gate_ref[:, pl.ds(pl.multiple_of(block * w, HD), wide)].astype(f32)
        cols = (raw_far[block].astype(f32) * gate).astype(bf16)
        both = parts[block, :, :wide] + mm(att_far[...], cols, NN)

        @pl.when(lax.rem(block + me_dp, 2) == 1)
        def _():
            both_outgoing[lax.div(block, 2)] = both.astype(bf16)
            both_copy(block).start()

        @pl.when(lax.rem(block + me_dp, 2) == 0)
        def _():
            parts[block, :, :wide] = both

    def bias_of(vis, t, far):
        owner = far_sp if far else me_sp
        place = map_ref[t, owner]

        def span(slab):
            apart = jnp.abs(owner - slab)
            spans = []
            for j in range(count):
                distance = jnp.abs(place - map_ref[j, slab])
                seen = (vis[t : t + 1, 0:1] >= apart) & (vis[t : t + 1, 1:2] >= distance)
                value = jnp.where(seen, 0.0, -1e30).astype(f32)
                spans.append(jnp.broadcast_to(value, (tile, 1)))
            return spans

        place_of = lax.broadcasted_iota(jnp.int32, (text, 1), 0)
        words = jnp.where(place_of < live_ref[0], 0.0, -1e30).astype(f32)
        return jnp.concatenate(span(me_sp) + [words] + span(far_sp), axis=0)

    def soft(q, h_cols, bias):
        scores = factor * mm(keys[:, h_cols], q, NT) + bias
        top = jnp.max(scores, axis=0, keepdims=True)
        weights = jnp.exp(scores - top)
        total = jnp.sum(weights, axis=0, keepdims=True)
        return weights * (1.0 / total)

    def cols_of(h):
        return pl.ds(pl.multiple_of(h * HD, HD), HD)

    def delta_of(ga, att):
        return jnp.sum(ga.astype(f32).T * att.astype(f32), axis=0, keepdims=True)

    def rows_of(t):
        return slice(t * tile, (t + 1) * tile)

    def chunk_rows(h):
        return pl.ds(pl.multiple_of(h * step_rows, step_rows), step_rows)

    def y_copy(h):
        rows = chunk_rows(h)
        return remote(last_out.at[rows], last_in.at[rows], ys.at[0], yr.at[h], top_peer)

    def g_copy(h):
        rows = chunk_rows(h)
        return remote(x_out.at[rows], x_in.at[rows], gs_sem.at[0], gr_sem.at[h], sp_far)

    def both_top(h):
        rows = chunk_rows(h)
        return remote(both_out.at[rows], both_in.at[rows], bys.at[0], byr.at[h], top_peer)

    scale(me_tp)
    for i in range(2):
        relay(near_line, 0, i)
    for i in range(2):
        settle(near_line, 0, i)
    each_block(0, scale)
    x_copies[1].wait_recv()

    def forward(h, carry):
        c = cols_of(h)
        for t in range(count):
            rows = rows_of(t)
            weights_s[h, :, rows] = soft(q_ref[rows, c], c, bias_of(win_own, t, False))
        return carry

    lax.fori_loop(0, heads, forward, 0)
    w_top[0].wait_recv()
    w_relay[0].start()
    for step in range(1, last):
        for i in range(2):
            relay(near_line, step, i)
    w_top[1].wait_recv()
    w_relay[1].start()
    for step in range(1, last):
        for i in range(2):
            settle(near_line, step, i)
    x_copies[2].wait_recv()

    def attend(h, carry):
        c = cols_of(h)
        att_t[c, :] = mm(vals[:, c], weights_s[h].astype(bf16), TN).astype(bf16)
        return carry

    lax.fori_loop(0, heads, attend, 0)
    part(me_tp)
    each_block(0, part)
    for step in range(1, last):
        each_block(step, scale)
        each_block(step, part)
    w_core.wait_recv()
    for c in w_relay:
        c.wait_recv()
    acc[...] = mm(nat[me_tp], w_all[me_tp], NT)
    for step in range(last):
        each_block(step, add_block)

    away = me_dp ^ top_bit

    def send_top():
        p_copy(away).wait_recv()

        def chunk(h, carry):
            rows = chunk_rows(h)
            mine = parts[away, rows, wide:]
            pair = mine + incoming[lax.div(away, 2), rows, :].astype(f32)
            last_out[rows, :] = pair.astype(bf16)
            y_copy(h).start()
            return carry

        lax.fori_loop(0, chunks, chunk, 0)

    def send_both_top():
        both_copy(away).wait_recv()

        def chunk(h, carry):
            rows = chunk_rows(h)
            mine = parts[away, rows, :wide]
            pair = mine + both_incoming[lax.div(away, 2), rows, :].astype(f32)
            both_out[rows, :] = pair.astype(bf16)
            both_top(h).start()
            return carry

        lax.fori_loop(0, chunks, chunk, 0)

    late = jnp.abs(away - me_tp) == n_tp - 1

    @pl.when(jnp.logical_not(late))
    def _():
        send_top()

    for i in range(2):
        rows = slice(i * half, (i + 1) * half)
        grad_far[i].wait_recv()
        start_z(far_line, 0, i)
        settle(near_line, last, i)

        def add_half(block):
            scale(block, rows)
            acc[rows] += mm(nat[block, rows], w_all[block], NT)

        each_block(last, add_half)
        ga_own[rows] = acc[rows].astype(bf16)
        x_copies[4 + i].start()
    each_block(last, part)

    def backward(h, carry):
        c = cols_of(h)
        for t in range(count):
            rows = rows_of(t)
            q = q_ref[rows, c]
            ga = ga_own[rows, c]
            weights = weights_s[h, :, rows]
            delta = delta_of(ga, att_t[c, rows])
            gp = mm(vals[:, c], ga, NT)
            gs = (weights * (gp - delta)).astype(bf16)
            gq_ref[rows, c] = (factor * mm(keys[:, c], gs, TN)).T.astype(bf16)
            gk = mm(gs[:near], q, NN)
            gv = mm(weights[:near].astype(bf16), ga, NN)
            if t == 0:
                gk_sum[:, c] = gk
                gv_sum[:, c] = gv
            else:
                gk_sum[:, c] += gk
                gv_sum[:, c] += gv

        return carry

    def pass_on(h):
        y_copy(h).wait_recv()
        rows = chunk_rows(h)
        mine = parts[me_dp, rows, wide:] + incoming[lax.div(me_dp, 2), rows, :].astype(f32)
        total = mine + last_in[rows, :].astype(f32)
        gw_ref[rows, wide:] = total
        x_out[rows, :] = total.astype(bf16)
        g_copy(h).start()

    x_copies[0].wait_recv()
    x_copies[3].wait_recv()

    def far_soft(h, carry):
        c = cols_of(h)
        for t in range(count):
            rows = rows_of(t)
            weights = soft(q_far[rows, c], c, bias_of(win_far, t, True))
            weights_far[h, :, rows] = weights[:near]
            att_far[c, rows] = mm(vals[:, c], weights.astype(bf16), TN).astype(bf16)
        return carry

    lax.fori_loop(0, early, far_soft, 0)

    @pl.when(late)
    def _():
        send_top()

    for i in range(2):
        relay(far_line, 0, i)
    x_copies[6].wait_recv()
    lax.fori_loop(early, heads, far_soft, 0)
    part_far(me_tp)
    for step in range(last):
        for i in range(2):
            if step:
                relay(far_line, step, i)
            settle(far_line, step, i)
        each_block(step, part_far)
    p_copy(me_dp).wait_recv()

    def pass_next(h, carry):
        pass_on(h)
        return carry

    lax.fori_loop(0, early, pass_next, 0)

    @pl.when(jnp.logical_not(late))
    def _():
        send_both_top()

    lax.fori_loop(0, heads - 2, backward, 0)
    for i in range(2):
        settle(far_line, last, i)
    each_block(last, part_far)
    lax.fori_loop(early, chunks, pass_next, 0)
    lax.fori_loop(heads - 2, heads, backward, 0)

    @pl.when(late)
    def _():
        send_both_top()

    x_copies[4].wait_recv()
    x_copies[5].wait_recv()

    def far(h, carry):
        c = cols_of(h)
        gk_all = gk_sum[:, c]
        gv_all = gv_sum[:, c]
        for t in range(count):
            rows = rows_of(t)
            q = q_far[rows, c]
            ga = ga_far[rows, c]
            weights = weights_far[h, :, rows]
            delta = delta_of(ga, att_far[c, rows])
            gp = mm(vals[:near, c], ga, NT)
            gs = (weights * (gp - delta)).astype(bf16)
            gk_all += mm(gs, q, NN)
            gv_all += mm(weights.astype(bf16), ga, NN)
        gk_ref[:, c] = (factor * gk_all[:tok]).astype(bf16)
        gtk_ref[:, c] = (factor * gk_all[tok:]).astype(bf16)
        gv_ref[:, c] = gv_all[:tok].astype(bf16)
        gtv_ref[:, c] = gv_all[tok:].astype(bf16)
        return carry

    lax.fori_loop(0, heads, far, 0)
    both_copy(me_dp).wait_recv()

    def finish_both(h, carry):
        rows = chunk_rows(h)
        both_top(h).wait_recv()
        mine = parts[me_dp, rows, :wide] + both_incoming[lax.div(me_dp, 2), rows, :].astype(f32)
        gw_ref[rows, :wide] = mine + both_in[rows, :].astype(f32)
        return carry

    lax.fori_loop(0, chunks, finish_both, 0)
    for c in x_copies + grad_far:
        c.wait_send()
    remote(last_out, last_in, ys.at[0], yr.at[0], top_peer).wait_send()
    remote(both_out, both_in, bys.at[0], byr.at[0], top_peer).wait_send()
    for c in [w_core] + w_top + w_relay:
        c.wait_send()
    for slot in range(n_dp // 2):
        p_copy(2 * slot).wait_send()
        both_copy(2 * slot).wait_send()
    for line in (near_line, far_line):
        for step in range(n_tp - 1):
            for i in range(2):
                send_z(line, step, i, lambda c: c.wait_send())

    def finish(h, carry):
        rows = chunk_rows(h)
        g_copy(h).wait_recv()
        gw_ref[rows, wide:] += x_in[rows, :].astype(f32)
        return carry

    lax.fori_loop(0, chunks, finish, 0)
    remote(x_out, x_in, gs_sem.at[0], gr_sem.at[0], sp_far).wait_send()


def mega_call(n_tp, n_dp, q, k, v, tk, tv, s, w, gate, windows, tile_map, text_count):
    tok, width = q.shape
    text = tk.shape[0]
    heads = width // HD
    cols = w.shape[1]
    total = 2 * tok + text
    near = tok + text
    count = tile_map.shape[0]
    pairs = n_dp // 2
    wide = int(cols * SHARE) // HD * HD
    bf16, f32 = jnp.bfloat16, jnp.float32
    dma = pltpu.SemaphoreType.DMA
    shapes = [
        ((tok, width), bf16),
        ((tok, width), bf16),
        ((tok, width), bf16),
        ((text, width), bf16),
        ((text, width), bf16),
        ((width, cols), f32),
    ]
    small = [
        pltpu.VMEM((tok, width), bf16),
        pltpu.VMEM(gate.shape, bf16),
        pltpu.VMEM(windows.shape, jnp.int32),
        pltpu.SMEM(tile_map.shape, jnp.int32),
        pltpu.SMEM(text_count.shape, jnp.int32),
    ]
    scratch = [
        ((total, width), bf16),
        ((total, width), bf16),
        ((tok, width), bf16),
        ((tok, width), bf16),
        ((tok, width), bf16),
        ((count + -count % 8, HD), jnp.int32),
        ((count + -count % 8, HD), jnp.int32),
        ((n_tp, tok, s.shape[1]), bf16),
        ((n_tp, tok, s.shape[1]), bf16),
        ((n_tp, tok, wide), bf16),
        ((n_dp, width, cols), bf16),
        ((tok, width), f32),
        ((width, tok), bf16),
        ((width, tok), bf16),
        ((heads, total, tok), f32),
        ((heads, near, tok), f32),
        ((near, width), f32),
        ((near, width), f32),
        ((n_dp, width, cols), f32),
        ((pairs, width, cols - wide), bf16),
        ((pairs, width, cols - wide), bf16),
        ((width, cols - wide), bf16),
        ((width, cols - wide), bf16),
        ((width, cols - wide), bf16),
        ((width, cols - wide), bf16),
        ((pairs, width, wide), bf16),
        ((pairs, width, wide), bf16),
        ((width, wide), bf16),
        ((width, wide), bf16),
    ]
    sems = [(11,), (9,), (9,), (5,), (5,)] + [(n_tp - 1, 2)] * 8 + [(pairs,)] * 4
    sems += [(1,), (heads,)] * 3
    held = sum(jnp.dtype(b).itemsize * a[0] * a[1] for a, b in shapes)
    return pl.pallas_call(
        functools.partial(mega_kernel, count, n_tp, n_dp),
        out_shape=[pltpu.VMEM(a, b) for a, b in shapes],
        in_specs=[pl.BlockSpec(memory_space=pltpu.HBM)] * 11,
        out_specs=[pl.BlockSpec(memory_space=pltpu.VMEM)] * 6,
        scratch_shapes=small + [pltpu.VMEM(a, b) for a, b in scratch] + [dma(n) for n in sems],
        compiler_params=pltpu.CompilerParams(
            collective_id=0, has_side_effects=True, vmem_limit_bytes=VMEM - held - (1 << 18)
        ),
        name="attention_backward",
    )(q, k, v, tk, tv, s, w, gate, windows, tile_map, text_count)


def per_device(
    query,
    key,
    value,
    text_key,
    text_value,
    grad_out,
    gate,
    out_weight,
    windows,
    tile_map,
    text_count,
):
    q, k, v = query[0], key[0], value[0]
    tk, tv = text_key[0], text_value[0]
    tok, width = q.shape
    n_sp = lax.axis_size("sp")
    n_dp = lax.axis_size("dp")
    n_tp = lax.axis_size("tp")
    me_sp = lax.axis_index("sp")
    me_tp = lax.axis_index("tp")
    me_dp = lax.axis_index("dp")
    index = jnp.stack([me_tp, me_dp]).astype(jnp.int32)

    offsets = sorted({1 % n_sp, (n_sp - 1) % n_sp} - {0})

    def from_offset(block, offset):
        route = [((i + offset) % n_sp, i) for i in range(n_sp)]
        route = [(a, b) for a, b in route if abs(a - b) <= 1]
        return lax.ppermute(block, "sp", route)

    def to_offset(block, offset):
        route = [(i, (i + offset) % n_sp) for i in range(n_sp)]
        route = [(a, b) for a, b in route if abs(a - b) <= 1]
        return lax.ppermute(block, "sp", route)

    own_gate = lax.dynamic_slice_in_dim(gate[0], me_tp * width, width, 0)
    scaled = (grad_out[0].astype(jnp.float32) * own_gate.astype(jnp.float32)[None, :]).astype(
        jnp.bfloat16
    )
    own_map = lax.dynamic_index_in_dim(tile_map, me_sp, 0, keepdims=False)
    count = own_map.shape[0]
    tile = tok // count
    live = jnp.arange(tk.shape[0], dtype=jnp.int32) < text_count[0]

    def tiles_seen(o):
        other = lax.rem(me_sp + o, n_sp)
        apart = jnp.abs(other - me_sp)
        other_map = lax.dynamic_index_in_dim(tile_map, other, 0, keepdims=False)
        near_time = (apart <= windows[:, 0]) & (apart <= 1)
        near_space = jnp.abs(own_map[:, None] - other_map[None, :]) <= windows[:, 1][:, None]
        return near_time[:, None] & near_space

    if offsets == [n_sp - 1] and n_tp == n_dp and len(bits_of(n_dp)) == 2:
        outs = mega_call(
            n_tp,
            n_dp,
            q,
            k,
            v,
            tk,
            tv,
            grad_out[0],
            out_weight,
            gate,
            windows,
            tile_map.T,
            text_count,
        )
        outs = copy_call(outs)
        return tuple(o[None] for o in outs[:5]) + (outs[5],)

    near_k = [from_offset(k, o) for o in offsets]
    near_v = [from_offset(v, o) for o in offsets]

    s_rel = ring_gather(scaled, "tp")
    w_rel = xor_gather(out_weight, "dp")

    seen = [jnp.repeat(tiles_seen(o), tile, axis=1) for o in [0] + offsets]
    seen.append(jnp.broadcast_to(live[None, :], (count, tk.shape[0])))
    bias = jnp.where(jnp.concatenate(seen, axis=1), 0.0, -1e30).astype(jnp.float32)[:, :, None]

    nat, ga = grad_attn_call(index, s_rel, w_rel)

    heads = width // HD
    groups = GROUPS if heads % GROUPS == 0 else 1
    each = heads // groups
    ks = [k] + near_k + [tk]
    vs = [v] + near_v + [tv]
    nk = len(ks)
    ats, gqs, gks, gvs, gtk, gtv = [], [], [], [], [], []
    for g in range(groups):
        res = attention_call(g * each, each, count, q, ga, bias, ks, vs)
        at, gq = res[:2]
        gk, gv = list(res[2 : 2 + nk]), list(res[2 + nk :])
        ats.append(at)
        gqs.append(gq)
        own_k, own_v = gk[0], gv[0]
        for i, o in enumerate(offsets):
            own_k = own_k + to_offset(gk[1 + i], o).astype(jnp.float32)
            own_v = own_v + to_offset(gv[1 + i], o).astype(jnp.float32)
        gks.append(own_k)
        gvs.append(own_v)
        gtk.append(total_over(gk[-1], "sp"))
        gtv.append(total_over(gv[-1], "sp"))

    parts = dict(enumerate(weight_call(index, nat, ats, n_dp)))
    for bit in bits_of(n_dp):
        got = {
            d: lax.ppermute(parts[d | bit].astype(jnp.bfloat16), "dp", xor_route("dp", bit))
            for d in parts
            if not d & bit
        }
        parts = {d: parts[d].astype(jnp.float32) + got[d].astype(jnp.float32) for d in got}
    weight_grad = total_over(parts[0], "sp")

    def joined(pieces):
        return jnp.concatenate(pieces, axis=1).astype(jnp.bfloat16)[None]

    return (joined(gqs), joined(gks), joined(gvs), joined(gtk), joined(gtv), weight_grad)


def solution(mesh):
    placed = (
        P("dp", "sp", "tp"),
        P("dp", "sp", "tp"),
        P("dp", "sp", "tp"),
        P("dp", None, "tp"),
        P("dp", None, "tp"),
        P("dp", "sp", "tp"),
        P("dp", None),
        P("tp", "dp"),
        P("sp", None),
        P(),
        P("dp"),
    )
    return jax.shard_map(
        per_device,
        mesh=mesh,
        in_specs=placed,
        out_specs=(
            P("dp", "sp", "tp"),
            P("dp", "sp", "tp"),
            P("dp", "sp", "tp"),
            P("dp", None, "tp"),
            P("dp", None, "tp"),
            P("tp", "dp"),
        ),
        check_vma=False,
    )
```

```python
import functools

import jax
import jax.numpy as jnp
from jax import lax
from jax.experimental import pallas as pl
from jax.experimental.pallas import tpu as pltpu
from jax.sharding import PartitionSpec as P

HD = 128
GROUPS = 2
SHARE = 0.5


NT = (((1,), (1,)), ((), ()))
NN = (((1,), (0,)), ((), ()))
TN = (((0,), (0,)), ((), ()))


def mm(a, b, dims):
    return lax.dot_general(a, b, dims, preferred_element_type=jnp.float32)


def ring_gather(block, axis):
    n = lax.axis_size(axis)
    rel = [block] + [None] * (n - 1)
    up = [(i, (i + 1) % n) for i in range(n)]
    down = [((i + 1) % n, i) for i in range(n)]
    ahead = behind = block
    for step in range(1, (n - 1) // 2 + 1):
        ahead = lax.ppermute(ahead, axis, down)
        behind = lax.ppermute(behind, axis, up)
        rel[step] = ahead
        rel[n - step] = behind
    if n % 2 == 0:
        half = block.shape[0] // 2
        first = lax.ppermute(ahead[:half], axis, down)
        second = lax.ppermute(behind[half:], axis, up)
        rel[n // 2] = jnp.concatenate([first, second], axis=0)
    return rel


def xor_route(axis, bit):
    n = lax.axis_size(axis)
    return [(i, i ^ bit) for i in range(n)]


def bits_of(n):
    return [1 << b for b in range(n.bit_length() - 1)]


def xor_gather(block, axis):
    n = lax.axis_size(axis)
    rel = {0: block}
    for bit in reversed(bits_of(n)):
        got = {d | bit: lax.ppermute(b, axis, xor_route(axis, bit)) for d, b in rel.items()}
        rel.update(got)
    return [rel[d] for d in range(n)]


def grad_attn_kernel(n_tp, n_dp, idx_ref, *refs):
    s_refs = refs[:n_tp]
    w_refs = refs[n_tp : n_tp + n_dp]
    nat_ref, ga_ref, acc_ref = refs[n_tp + n_dp :]
    me_tp = idx_ref[0]
    me_dp = idx_ref[1]
    w = s_refs[0].shape[1]
    for j in range(n_tp):
        nat_ref[lax.rem(me_tp + j, n_tp)] = s_refs[j][...]
    r = w_refs[0].shape[1] // w
    acc = None
    for d in range(n_dp):
        for piece in range(r):
            s = nat_ref[(me_dp ^ d) * r + piece]
            term = mm(s, w_refs[d][:, piece * w : (piece + 1) * w], NT)
            if d == 0 and piece == 0:
                acc_ref[...] = term
            else:
                acc_ref[...] += term
    ga_ref[...] = acc_ref[...].astype(jnp.bfloat16)


def grad_attn_call(index, s_rel, w_rel):
    tok, w = s_rel[0].shape
    rows = w_rel[0].shape[0]
    n_tp, n_dp = len(s_rel), len(w_rel)
    vm = pl.BlockSpec(memory_space=pltpu.VMEM)
    return pl.pallas_call(
        functools.partial(grad_attn_kernel, n_tp, n_dp),
        out_shape=(
            jax.ShapeDtypeStruct((n_tp, tok, w), jnp.bfloat16),
            jax.ShapeDtypeStruct((tok, rows), jnp.bfloat16),
        ),
        in_specs=[pl.BlockSpec(memory_space=pltpu.SMEM)] + [vm] * (n_tp + n_dp),
        out_specs=(vm, vm),
        scratch_shapes=[pltpu.VMEM((tok, rows), jnp.float32)],
        cost_estimate=pl.CostEstimate(
            flops=2 * tok * rows * n_tp * w, bytes_accessed=12 << 20, transcendentals=0
        ),
        name="grad_attn",
    )(index, *s_rel, *w_rel)


def attention_kernel(count, nk, q_ref, ga_ref, bias_ref, *refs):
    k_refs = refs[:nk]
    v_refs = refs[nk : 2 * nk]
    at_ref, gq_ref = refs[2 * nk : 2 * nk + 2]
    gk_refs = refs[2 * nk + 2 : 3 * nk + 2]
    gv_refs = refs[3 * nk + 2 : 4 * nk + 2]
    factor = HD ** (-0.5)
    tok = q_ref.shape[0]
    tile = tok // count
    keys = jnp.concatenate([r[...] for r in k_refs], axis=0)
    vals = jnp.concatenate([r[...] for r in v_refs], axis=0)
    gk_sum = gv_sum = None
    for t in range(count):
        rows = slice(t * tile, (t + 1) * tile)
        q = q_ref[rows, :]
        ga = ga_ref[rows, :]
        scores = factor * mm(keys, q, NT) + bias_ref[t]
        top = jnp.max(scores, axis=0, keepdims=True)
        weights = jnp.exp(scores - top)
        total = jnp.sum(weights, axis=0, keepdims=True)
        weights = weights * (1.0 / total)
        probs = weights.astype(jnp.bfloat16)
        att = mm(vals, probs, TN).astype(jnp.bfloat16)
        at_ref[:, rows] = att
        ga_t = ga.astype(jnp.float32).T
        delta = jnp.sum(ga_t * att.astype(jnp.float32), axis=0, keepdims=True)
        gp = mm(vals, ga, NT)
        gs = (weights * (gp - delta)).astype(jnp.bfloat16)
        gq = factor * mm(keys, gs, TN)
        gq_ref[rows, :] = gq.T.astype(jnp.bfloat16)
        gk = factor * mm(gs, q, NN)
        gv = mm(probs, ga, NN)
        gk_sum = gk if t == 0 else gk_sum + gk
        gv_sum = gv if t == 0 else gv_sum + gv
    at = 0
    for i in range(nk):
        n = gk_refs[i].shape[0]
        gk_refs[i][...] = gk_sum[at : at + n].astype(gk_refs[i].dtype)
        gv_refs[i][...] = gv_sum[at : at + n].astype(gv_refs[i].dtype)
        at += n


def attention_call(first, heads, count, q, ga, bias, ks, vs):
    tok = q.shape[0]
    nk = len(ks)

    def head(n):
        return pl.BlockSpec((n, HD), lambda h: (0, first + h))

    def out(n):
        return pl.BlockSpec((n, HD), lambda h: (0, h))

    sizes = [k.shape[0] for k in ks]
    kinds = [jnp.float32 if i == 0 else jnp.bfloat16 for i in range(nk)]
    kinds[-1] = jnp.float32
    total = sum(sizes)
    width = heads * HD
    grads = [jax.ShapeDtypeStruct((n, width), kind) for n, kind in zip(sizes, kinds)]
    return pl.pallas_call(
        functools.partial(attention_kernel, count, nk),
        grid=(heads,),
        out_shape=[
            jax.ShapeDtypeStruct((width, tok), jnp.bfloat16),
            jax.ShapeDtypeStruct((tok, width), jnp.bfloat16),
        ]
        + grads
        + grads,
        in_specs=[head(tok), head(tok), pl.BlockSpec(memory_space=pltpu.VMEM)]
        + [head(n) for n in sizes]
        + [head(n) for n in sizes],
        out_specs=[pl.BlockSpec((HD, tok), lambda h: (h, 0)), out(tok)]
        + [out(n) for n in sizes]
        + [out(n) for n in sizes],
        cost_estimate=pl.CostEstimate(
            flops=heads * 20 * tok * total * HD,
            bytes_accessed=heads * 4 << 20,
            transcendentals=heads * tok * total,
        ),
        name="attention",
    )(q, ga, bias, *ks, *vs)


def weight_kernel(n_dp, groups, idx_ref, nat_ref, *refs):
    at_refs = refs[:groups]
    outs = refs[groups:]
    me_dp = idx_ref[1]
    w = nat_ref.shape[2]
    r = outs[0].shape[1] // w
    for d in range(n_dp):
        for piece in range(r):
            s = nat_ref[(me_dp ^ d) * r + piece]
            row = 0
            for at in at_refs:
                n = at.shape[0]
                outs[d][row : row + n, piece * w : (piece + 1) * w] = mm(at[...], s, NN).astype(
                    outs[d].dtype
                )
                row += n


def weight_call(index, nat, ats, n_dp):
    n_tp, tok, w = nat.shape
    rows = sum(a.shape[0] for a in ats)
    cols = n_tp * w // n_dp
    vm = pl.BlockSpec(memory_space=pltpu.VMEM)
    return pl.pallas_call(
        functools.partial(weight_kernel, n_dp, len(ats)),
        out_shape=[
            jax.ShapeDtypeStruct((rows, cols), jnp.bfloat16 if d & 1 else jnp.float32)
            for d in range(n_dp)
        ],
        in_specs=[pl.BlockSpec(memory_space=pltpu.SMEM)] + [vm] * (1 + len(ats)),
        out_specs=[vm] * n_dp,
        cost_estimate=pl.CostEstimate(
            flops=2 * tok * rows * n_tp * w, bytes_accessed=16 << 20, transcendentals=0
        ),
        name="weight",
    )(index, nat, *ats)


def total_over(block, axis):
    for bit in bits_of(lax.axis_size(axis)):
        got = lax.ppermute(block.astype(jnp.bfloat16), axis, xor_route(axis, bit))
        block = block + got.astype(jnp.float32)
    return block


VMEM = 67043328


def copy_kernel(n, *refs):
    srcs, dsts, sem = refs[:n], refs[n : 2 * n], refs[2 * n]
    copies = []
    for src, dst in zip(srcs, dsts):
        pieces = 4 if src.dtype == jnp.float32 else 1
        rows = src.shape[0] // pieces
        for i in range(pieces):
            at = pl.ds(i * rows, rows)
            copies.append(pltpu.make_async_copy(src.at[at], dst.at[at], sem.at[len(copies)]))
    for c in copies:
        c.start()
    for c in copies:
        c.wait()


def copy_call(arrays):
    n = len(arrays)
    return pl.pallas_call(
        functools.partial(copy_kernel, n),
        out_shape=[jax.ShapeDtypeStruct(a.shape, a.dtype) for a in arrays],
        in_specs=[pl.BlockSpec(memory_space=pltpu.VMEM)] * n,
        out_specs=[pl.BlockSpec(memory_space=pltpu.HBM)] * n,
        scratch_shapes=[pltpu.SemaphoreType.DMA((4 * n,))],
        compiler_params=pltpu.CompilerParams(vmem_limit_bytes=4 << 20),
        name="results",
    )(*arrays)


MESH = pl.DeviceIdType.MESH


def mega_kernel(
    count,
    n_tp,
    n_dp,
    q_hbm,
    k_hbm,
    v_hbm,
    tk_hbm,
    tv_hbm,
    s_hbm,
    w_hbm,
    gate_hbm,
    windows_hbm,
    map_hbm,
    live_hbm,
    gq_ref,
    gk_ref,
    gv_ref,
    gtk_ref,
    gtv_ref,
    gw_ref,
    q_ref,
    gate_ref,
    windows_ref,
    map_ref,
    live_ref,
    keys,
    vals,
    q_far,
    ga_own,
    ga_far,
    win_own,
    win_far,
    raw,
    nat,
    raw_far,
    w_all,
    acc,
    att_t,
    att_far,
    weights_s,
    weights_far,
    gk_sum,
    gv_sum,
    parts,
    outgoing,
    incoming,
    last_out,
    last_in,
    x_out,
    x_in,
    both_outgoing,
    both_incoming,
    both_out,
    both_in,
    ls,
    xs,
    xr,
    ws,
    wr,
    us,
    ur,
    ds,
    dr,
    fus,
    fur,
    fds,
    fdr,
    ps,
    pr,
    bps,
    bpr,
    ys,
    yr,
    bys,
    byr,
    gs_sem,
    gr_sem,
):
    factor = HD ** (-0.5)
    bf16, f32 = jnp.bfloat16, jnp.float32
    tok, width = q_ref.shape
    text = tk_hbm.shape[0]
    heads = width // HD
    chunks = heads
    step_rows = width // chunks
    early = heads // 2
    tile = tok // count
    near = tok + text
    w = raw.shape[2]
    half = tok // 2
    wide = raw_far.shape[2]
    me_sp = lax.axis_index("sp")
    me_dp = lax.axis_index("dp")
    me_tp = lax.axis_index("tp")
    far_sp = 1 - me_sp
    core_bit, top_bit = bits_of(n_dp)
    core_peer, top_peer = {"dp": me_dp ^ core_bit}, {"dp": me_dp ^ top_bit}
    sp_far = {"sp": far_sp}
    has_up = me_tp + 1 < n_tp
    has_down = me_tp >= 1
    last = n_tp - 2

    barrier = pltpu.get_barrier_semaphore()
    for peer in (sp_far, core_peer, top_peer):
        pl.semaphore_signal(barrier, inc=1, device_id=peer, device_id_type=MESH)

    @pl.when(has_up)
    def _():
        pl.semaphore_signal(barrier, inc=1, device_id={"tp": me_tp + 1}, device_id_type=MESH)

    @pl.when(has_down)
    def _():
        pl.semaphore_signal(barrier, inc=1, device_id={"tp": me_tp - 1}, device_id_type=MESH)

    loads = [
        pltpu.make_async_copy(a, b, ls.at[i])
        for i, (a, b) in enumerate(
            [
                (s_hbm, raw.at[me_tp]),
                (k_hbm, keys.at[pl.ds(0, tok)]),
                (w_hbm, w_all.at[me_dp]),
                (v_hbm, vals.at[pl.ds(0, tok)]),
                (q_hbm, q_ref),
                (gate_hbm, gate_ref),
                (windows_hbm, windows_ref),
                (tk_hbm, keys.at[pl.ds(tok, text)]),
                (tv_hbm, vals.at[pl.ds(tok, text)]),
                (map_hbm, map_ref),
                (live_hbm, live_ref),
            ]
        )
    ]
    for c in loads:
        c.start()
    pl.semaphore_wait(barrier, 3 + jnp.where(has_up, 1, 0) + jnp.where(has_down, 1, 0))

    def remote(src, dst, send, recv, where):
        return pltpu.make_async_remote_copy(
            src_ref=src,
            dst_ref=dst,
            send_sem=send,
            recv_sem=recv,
            device_id=where,
            device_id_type=MESH,
        )

    def halves(n):
        return [pl.ds(0, n // 2), pl.ds(n // 2, n // 2)]

    x_copies = [
        remote(win_own, win_far, xs.at[0], xr.at[0], sp_far),
        remote(keys.at[pl.ds(0, tok)], keys.at[pl.ds(near, tok)], xs.at[1], xr.at[1], sp_far),
        remote(vals.at[pl.ds(0, tok)], vals.at[pl.ds(near, tok)], xs.at[1], xr.at[2], sp_far),
        remote(
            q_ref.at[:, pl.ds(0, early * HD)],
            q_far.at[:, pl.ds(0, early * HD)],
            xs.at[3],
            xr.at[3],
            sp_far,
        ),
    ] + [
        remote(ga_own.at[rows], ga_far.at[rows], xs.at[4], xr.at[4 + i], sp_far)
        for i, rows in enumerate(halves(tok))
    ]
    q_rest = pl.ds(early * HD, width - early * HD)
    x_copies.append(remote(q_ref.at[:, q_rest], q_far.at[:, q_rest], xs.at[3], xr.at[6], sp_far))
    grad_far = [
        remote(
            raw.at[me_tp, rows, pl.ds(0, wide)],
            raw_far.at[me_tp, rows],
            xs.at[5],
            xr.at[7 + i],
            sp_far,
        )
        for i, rows in enumerate(halves(tok))
    ]

    w_core = remote(w_all.at[me_dp], w_all.at[me_dp], ws.at[0], wr.at[0], core_peer)
    w_top = [
        remote(w_all.at[me_dp, rows], w_all.at[me_dp, rows], ws.at[1], wr.at[1 + i], top_peer)
        for i, rows in enumerate(halves(width))
    ]
    w_relay = [
        remote(
            w_all.at[me_dp ^ top_bit, rows],
            w_all.at[me_dp ^ top_bit, rows],
            ws.at[2],
            wr.at[3 + i],
            core_peer,
        )
        for i, rows in enumerate(halves(width))
    ]

    near_line = (raw, us, ur, ds, dr)
    far_line = (raw_far, fus, fur, fds, fdr)

    def up_copy(line, step, i, block, where):
        ref = line[0].at[block, halves(tok)[i]]
        return remote(ref, ref, line[1].at[0], line[2].at[step, i], {"tp": where})

    def down_copy(line, step, i, block, where):
        ref = line[0].at[block, halves(tok)[i]]
        return remote(ref, ref, line[3].at[0], line[4].at[step, i], {"tp": where})

    def start_z(line, i):
        @pl.when(has_up)
        def _():
            up_copy(line, 0, i, me_tp, me_tp + 1).start()

        @pl.when(has_down)
        def _():
            down_copy(line, 0, i, me_tp, me_tp - 1).start()

    def sent_z(line):
        for sent in range(1, n_tp):
            ref = line[0].at[pl.ds(0, sent)]

            @pl.when(me_tp + 1 == sent)
            def _():
                remote(ref, ref, line[1].at[0], line[2].at[0, 0], {"tp": me_tp + 1}).wait_send()

            @pl.when(n_tp - me_tp == sent)
            def _():
                remote(ref, ref, line[3].at[0], line[4].at[0, 0], {"tp": me_tp - 1}).wait_send()

    def relay(line, step, i):
        @pl.when(has_up & (me_tp >= step + 1))
        def _():
            up_copy(line, step, i, me_tp - 1 - step, me_tp - 1).wait_recv()
            up_copy(line, step + 1, i, me_tp - 1 - step, me_tp + 1).start()

        @pl.when(has_down & (me_tp + 1 + step < n_tp))
        def _():
            down_copy(line, step, i, me_tp + 1 + step, me_tp + 1).wait_recv()
            down_copy(line, step + 1, i, me_tp + 1 + step, me_tp - 1).start()

    def settle(line, step, i):
        @pl.when(jnp.logical_not(has_up) & (me_tp >= step + 1))
        def _():
            up_copy(line, step, i, me_tp - 1 - step, me_tp - 1).wait_recv()

        @pl.when(jnp.logical_not(has_down) & (me_tp + 1 + step < n_tp))
        def _():
            down_copy(line, step, i, me_tp + 1 + step, me_tp + 1).wait_recv()

    def each_block(step, act):
        def side(i, carry):
            block = me_tp + (2 * i - 1) * (step + 1)

            @pl.when((block >= 0) & (block < n_tp))
            def _():
                act(block)

            return carry

        lax.fori_loop(0, 2, side, 0)

    loads[0].wait()
    for i in range(2):
        start_z(near_line, i)
    loads[1].wait()
    x_copies[1].start()
    loads[2].wait()
    for c in w_top:
        c.start()
    w_core.start()
    loads[3].wait()
    x_copies[2].start()
    loads[4].wait()
    x_copies[3].start()
    for c in grad_far:
        c.start()
    loads[6].wait()
    win_own[:count, :2] = windows_ref[...]
    x_copies[0].start()
    x_copies[6].start()
    for i in (5, 7, 8, 9, 10):
        loads[i].wait()

    def scale(block, rows=slice(None)):
        gate = gate_ref[:, pl.ds(pl.multiple_of(block * w, HD), w)].astype(f32)
        nat[block, rows] = (raw[block, rows].astype(f32) * gate).astype(bf16)

    def add_block(block):
        acc[...] += mm(nat[block], w_all[block], NT)

    def p_copy(block):
        slot = lax.div(block, 2)
        return remote(outgoing.at[slot], incoming.at[slot], ps.at[0], pr.at[slot], core_peer)

    def part(block):
        parts[block] = mm(att_t[...], nat[block], NN)

        @pl.when(lax.rem(block + me_dp, 2) == 1)
        def _():
            outgoing[lax.div(block, 2)] = parts[block, :, wide:].astype(bf16)
            p_copy(block).start()

    def both_copy(block):
        slot = lax.div(block, 2)
        return remote(
            both_outgoing.at[slot], both_incoming.at[slot], bps.at[0], bpr.at[slot], core_peer
        )

    def part_far(block):
        gate = gate_ref[:, pl.ds(pl.multiple_of(block * w, HD), wide)].astype(f32)
        cols = (raw_far[block].astype(f32) * gate).astype(bf16)
        both = parts[block, :, :wide] + mm(att_far[...], cols, NN)

        @pl.when(lax.rem(block + me_dp, 2) == 1)
        def _():
            both_outgoing[lax.div(block, 2)] = both.astype(bf16)
            both_copy(block).start()

        @pl.when(lax.rem(block + me_dp, 2) == 0)
        def _():
            parts[block, :, :wide] = both

    def bias_of(vis, t, far):
        owner = far_sp if far else me_sp
        place = map_ref[t, owner]

        def span(slab):
            apart = jnp.abs(owner - slab)
            spans = []
            for j in range(count):
                distance = jnp.abs(place - map_ref[j, slab])
                seen = (vis[t : t + 1, 0:1] >= apart) & (vis[t : t + 1, 1:2] >= distance)
                value = jnp.where(seen, 0.0, -1e30).astype(f32)
                spans.append(jnp.broadcast_to(value, (tile, 1)))
            return spans

        place_of = lax.broadcasted_iota(jnp.int32, (text, 1), 0)
        words = jnp.where(place_of < live_ref[0], 0.0, -1e30).astype(f32)
        return jnp.concatenate(span(me_sp) + [words] + span(far_sp), axis=0)

    def soft(q, h_cols, bias):
        scores = factor * mm(keys[:, h_cols], q, NT) + bias
        top = jnp.max(scores, axis=0, keepdims=True)
        weights = jnp.exp(scores - top)
        total = jnp.sum(weights, axis=0, keepdims=True)
        return weights * (1.0 / total)

    def cols_of(h):
        return pl.ds(pl.multiple_of(h * HD, HD), HD)

    def delta_of(ga, att):
        return jnp.sum(ga.astype(f32).T * att.astype(f32), axis=0, keepdims=True)

    def rows_of(t):
        return slice(t * tile, (t + 1) * tile)

    def chunk_rows(h):
        return pl.ds(pl.multiple_of(h * step_rows, step_rows), step_rows)

    def y_copy(h):
        rows = chunk_rows(h)
        return remote(last_out.at[rows], last_in.at[rows], ys.at[0], yr.at[h], top_peer)

    def g_copy(h):
        rows = chunk_rows(h)
        return remote(x_out.at[rows], x_in.at[rows], gs_sem.at[0], gr_sem.at[h], sp_far)

    def both_top(h):
        rows = chunk_rows(h)
        return remote(both_out.at[rows], both_in.at[rows], bys.at[0], byr.at[h], top_peer)

    scale(me_tp)
    for i in range(2):
        relay(near_line, 0, i)
    for i in range(2):
        settle(near_line, 0, i)
    each_block(0, scale)
    x_copies[1].wait_recv()

    def forward(h, carry):
        c = cols_of(h)
        for t in range(count):
            rows = rows_of(t)
            weights_s[h, :, rows] = soft(q_ref[rows, c], c, bias_of(win_own, t, False))
        return carry

    lax.fori_loop(0, heads, forward, 0)
    w_top[0].wait_recv()
    w_relay[0].start()
    for step in range(1, last):
        for i in range(2):
            relay(near_line, step, i)
    w_top[1].wait_recv()
    w_relay[1].start()
    for step in range(1, last):
        for i in range(2):
            settle(near_line, step, i)
    x_copies[2].wait_recv()

    def attend(h, carry):
        c = cols_of(h)
        att_t[c, :] = mm(vals[:, c], weights_s[h].astype(bf16), TN).astype(bf16)
        return carry

    lax.fori_loop(0, heads, attend, 0)
    part(me_tp)
    each_block(0, part)
    for step in range(1, last):
        each_block(step, scale)
        each_block(step, part)
    w_core.wait_recv()
    for c in w_relay:
        c.wait_recv()
    acc[...] = mm(nat[me_tp], w_all[me_tp], NT)
    for step in range(last):
        each_block(step, add_block)

    away = me_dp ^ top_bit

    def send_top():
        p_copy(away).wait_recv()

        def chunk(h, carry):
            rows = chunk_rows(h)
            mine = parts[away, rows, wide:]
            pair = mine + incoming[lax.div(away, 2), rows, :].astype(f32)
            last_out[rows, :] = pair.astype(bf16)
            y_copy(h).start()
            return carry

        lax.fori_loop(0, chunks, chunk, 0)

    def send_both_top():
        both_copy(away).wait_recv()

        def chunk(h, carry):
            rows = chunk_rows(h)
            mine = parts[away, rows, :wide]
            pair = mine + both_incoming[lax.div(away, 2), rows, :].astype(f32)
            both_out[rows, :] = pair.astype(bf16)
            both_top(h).start()
            return carry

        lax.fori_loop(0, chunks, chunk, 0)

    late = jnp.abs(away - me_tp) == n_tp - 1

    @pl.when(jnp.logical_not(late))
    def _():
        send_top()

    for i in range(2):
        rows = slice(i * half, (i + 1) * half)
        grad_far[i].wait_recv()
        start_z(far_line, i)
        settle(near_line, last, i)

        def add_half(block):
            scale(block, rows)
            acc[rows] += mm(nat[block, rows], w_all[block], NT)

        each_block(last, add_half)
        ga_own[rows] = acc[rows].astype(bf16)
        x_copies[4 + i].start()
    each_block(last, part)

    def backward(h, carry):
        c = cols_of(h)
        for t in range(count):
            rows = rows_of(t)
            q = q_ref[rows, c]
            ga = ga_own[rows, c]
            weights = weights_s[h, :, rows]
            delta = delta_of(ga, att_t[c, rows])
            gp = mm(vals[:, c], ga, NT)
            gs = (weights * (gp - delta)).astype(bf16)
            gq_ref[rows, c] = (factor * mm(keys[:, c], gs, TN)).T.astype(bf16)
            gk = mm(gs[:near], q, NN)
            gv = mm(weights[:near].astype(bf16), ga, NN)
            if t == 0:
                gk_sum[:, c] = gk
                gv_sum[:, c] = gv
            else:
                gk_sum[:, c] += gk
                gv_sum[:, c] += gv

        return carry

    def pass_on(h):
        y_copy(h).wait_recv()
        rows = chunk_rows(h)
        mine = parts[me_dp, rows, wide:] + incoming[lax.div(me_dp, 2), rows, :].astype(f32)
        total = mine + last_in[rows, :].astype(f32)
        gw_ref[rows, wide:] = total
        x_out[rows, :] = total.astype(bf16)
        g_copy(h).start()

    x_copies[0].wait_recv()
    x_copies[3].wait_recv()

    def far_soft(h, carry):
        c = cols_of(h)
        for t in range(count):
            rows = rows_of(t)
            weights = soft(q_far[rows, c], c, bias_of(win_far, t, True))
            weights_far[h, :, rows] = weights[:near]
            att_far[c, rows] = mm(vals[:, c], weights.astype(bf16), TN).astype(bf16)
        return carry

    lax.fori_loop(0, early, far_soft, 0)

    @pl.when(late)
    def _():
        send_top()

    for i in range(2):
        relay(far_line, 0, i)
    x_copies[6].wait_recv()
    lax.fori_loop(early, heads, far_soft, 0)
    part_far(me_tp)
    for step in range(last):
        for i in range(2):
            if step:
                relay(far_line, step, i)
            settle(far_line, step, i)
        each_block(step, part_far)

    def pass_next(h, carry):
        pass_on(h)
        return carry

    first = lax.rem(me_dp, 2) == 0

    @pl.when(first)
    def _():
        p_copy(me_dp).wait_recv()
        lax.fori_loop(0, early, pass_next, 0)

    @pl.when(jnp.logical_not(late))
    def _():
        send_both_top()

    lax.fori_loop(0, heads - 2, backward, 0)
    for i in range(2):
        settle(far_line, last, i)
    each_block(last, part_far)

    @pl.when(first)
    def _():
        lax.fori_loop(early, chunks, pass_next, 0)

    lax.fori_loop(heads - 2, heads, backward, 0)
    x_copies[4].wait_recv()
    x_copies[5].wait_recv()

    @pl.when(jnp.logical_not(first))
    def _():
        p_copy(me_dp).wait_recv()
        lax.fori_loop(0, chunks, pass_next, 0)

    @pl.when(late)
    def _():
        send_both_top()


    def far(h, carry):
        c = cols_of(h)
        gk_all = gk_sum[:, c]
        gv_all = gv_sum[:, c]
        for t in range(count):
            rows = rows_of(t)
            q = q_far[rows, c]
            ga = ga_far[rows, c]
            weights = weights_far[h, :, rows]
            delta = delta_of(ga, att_far[c, rows])
            gp = mm(vals[:near, c], ga, NT)
            gs = (weights * (gp - delta)).astype(bf16)
            gk_all += mm(gs, q, NN)
            gv_all += mm(weights.astype(bf16), ga, NN)
        gk_ref[:, c] = (factor * gk_all[:tok]).astype(bf16)
        gtk_ref[:, c] = (factor * gk_all[tok:]).astype(bf16)
        gv_ref[:, c] = gv_all[:tok].astype(bf16)
        gtv_ref[:, c] = gv_all[tok:].astype(bf16)
        return carry

    lax.fori_loop(0, heads, far, 0)
    both_copy(me_dp).wait_recv()

    def finish_both(h, carry):
        rows = chunk_rows(h)
        both_top(h).wait_recv()
        mine = parts[me_dp, rows, :wide] + both_incoming[lax.div(me_dp, 2), rows, :].astype(f32)
        gw_ref[rows, :wide] = mine + both_in[rows, :].astype(f32)
        return carry

    lax.fori_loop(0, chunks, finish_both, 0)
    both_keys, pair = pl.ds(0, 2 * tok), pl.ds(0, n_dp // 2)
    for c in [
        x_copies[0],
        remote(keys.at[both_keys], keys.at[both_keys], xs.at[1], xr.at[1], sp_far),
        remote(q_ref, q_far, xs.at[3], xr.at[3], sp_far),
        remote(ga_own, ga_far, xs.at[4], xr.at[4], sp_far),
        remote(raw_far.at[me_tp], raw_far.at[me_tp], xs.at[5], xr.at[7], sp_far),
        w_core,
        remote(w_all.at[me_dp], w_all.at[me_dp], ws.at[1], wr.at[1], top_peer),
        remote(w_all.at[me_dp], w_all.at[me_dp], ws.at[2], wr.at[3], core_peer),
        remote(outgoing.at[pair], incoming.at[pair], ps.at[0], pr.at[0], core_peer),
        remote(both_outgoing.at[pair], both_incoming.at[pair], bps.at[0], bpr.at[0], core_peer),
        remote(last_out, last_in, ys.at[0], yr.at[0], top_peer),
        remote(both_out, both_in, bys.at[0], byr.at[0], top_peer),
    ]:
        c.wait_send()
    for line in (near_line, far_line):
        sent_z(line)

    def finish(h, carry):
        rows = chunk_rows(h)
        g_copy(h).wait_recv()
        gw_ref[rows, wide:] += x_in[rows, :].astype(f32)
        return carry

    lax.fori_loop(0, chunks, finish, 0)
    remote(x_out, x_in, gs_sem.at[0], gr_sem.at[0], sp_far).wait_send()


def mega_call(n_tp, n_dp, q, k, v, tk, tv, s, w, gate, windows, tile_map, text_count):
    tok, width = q.shape
    text = tk.shape[0]
    heads = width // HD
    cols = w.shape[1]
    total = 2 * tok + text
    near = tok + text
    count = tile_map.shape[0]
    pairs = n_dp // 2
    wide = int(cols * SHARE) // HD * HD
    bf16, f32 = jnp.bfloat16, jnp.float32
    dma = pltpu.SemaphoreType.DMA
    shapes = [
        ((tok, width), bf16),
        ((tok, width), bf16),
        ((tok, width), bf16),
        ((text, width), bf16),
        ((text, width), bf16),
        ((width, cols), f32),
    ]
    small = [
        pltpu.VMEM((tok, width), bf16),
        pltpu.VMEM(gate.shape, bf16),
        pltpu.VMEM(windows.shape, jnp.int32),
        pltpu.SMEM(tile_map.shape, jnp.int32),
        pltpu.SMEM(text_count.shape, jnp.int32),
    ]
    scratch = [
        ((total, width), bf16),
        ((total, width), bf16),
        ((tok, width), bf16),
        ((tok, width), bf16),
        ((tok, width), bf16),
        ((count + -count % 8, HD), jnp.int32),
        ((count + -count % 8, HD), jnp.int32),
        ((n_tp, tok, s.shape[1]), bf16),
        ((n_tp, tok, s.shape[1]), bf16),
        ((n_tp, tok, wide), bf16),
        ((n_dp, width, cols), bf16),
        ((tok, width), f32),
        ((width, tok), bf16),
        ((width, tok), bf16),
        ((heads, total, tok), f32),
        ((heads, near, tok), f32),
        ((near, width), f32),
        ((near, width), f32),
        ((n_dp, width, cols), f32),
        ((pairs, width, cols - wide), bf16),
        ((pairs, width, cols - wide), bf16),
        ((width, cols - wide), bf16),
        ((width, cols - wide), bf16),
        ((width, cols - wide), bf16),
        ((width, cols - wide), bf16),
        ((pairs, width, wide), bf16),
        ((pairs, width, wide), bf16),
        ((width, wide), bf16),
        ((width, wide), bf16),
    ]
    sems = [(11,), (6,), (9,), (3,), (5,)] + [(1,), (n_tp - 1, 2)] * 4 + [(1,), (pairs,)] * 2
    sems += [(1,), (heads,)] * 3
    held = sum(jnp.dtype(b).itemsize * a[0] * a[1] for a, b in shapes)
    return pl.pallas_call(
        functools.partial(mega_kernel, count, n_tp, n_dp),
        out_shape=[pltpu.VMEM(a, b) for a, b in shapes],
        in_specs=[pl.BlockSpec(memory_space=pltpu.HBM)] * 11,
        out_specs=[pl.BlockSpec(memory_space=pltpu.VMEM)] * 6,
        scratch_shapes=small + [pltpu.VMEM(a, b) for a, b in scratch] + [dma(n) for n in sems],
        compiler_params=pltpu.CompilerParams(
            collective_id=0, has_side_effects=True, vmem_limit_bytes=VMEM - held - (1 << 18)
        ),
        name="attention_backward",
    )(q, k, v, tk, tv, s, w, gate, windows, tile_map, text_count)


def per_device(
    query,
    key,
    value,
    text_key,
    text_value,
    grad_out,
    gate,
    out_weight,
    windows,
    tile_map,
    text_count,
):
    q, k, v = query[0], key[0], value[0]
    tk, tv = text_key[0], text_value[0]
    tok, width = q.shape
    n_sp = lax.axis_size("sp")
    n_dp = lax.axis_size("dp")
    n_tp = lax.axis_size("tp")
    me_sp = lax.axis_index("sp")
    me_tp = lax.axis_index("tp")
    me_dp = lax.axis_index("dp")
    index = jnp.stack([me_tp, me_dp]).astype(jnp.int32)

    offsets = sorted({1 % n_sp, (n_sp - 1) % n_sp} - {0})

    def from_offset(block, offset):
        route = [((i + offset) % n_sp, i) for i in range(n_sp)]
        route = [(a, b) for a, b in route if abs(a - b) <= 1]
        return lax.ppermute(block, "sp", route)

    def to_offset(block, offset):
        route = [(i, (i + offset) % n_sp) for i in range(n_sp)]
        route = [(a, b) for a, b in route if abs(a - b) <= 1]
        return lax.ppermute(block, "sp", route)

    own_gate = lax.dynamic_slice_in_dim(gate[0], me_tp * width, width, 0)
    scaled = (grad_out[0].astype(jnp.float32) * own_gate.astype(jnp.float32)[None, :]).astype(
        jnp.bfloat16
    )
    own_map = lax.dynamic_index_in_dim(tile_map, me_sp, 0, keepdims=False)
    count = own_map.shape[0]
    tile = tok // count
    live = jnp.arange(tk.shape[0], dtype=jnp.int32) < text_count[0]

    def tiles_seen(o):
        other = lax.rem(me_sp + o, n_sp)
        apart = jnp.abs(other - me_sp)
        other_map = lax.dynamic_index_in_dim(tile_map, other, 0, keepdims=False)
        near_time = (apart <= windows[:, 0]) & (apart <= 1)
        near_space = jnp.abs(own_map[:, None] - other_map[None, :]) <= windows[:, 1][:, None]
        return near_time[:, None] & near_space

    if offsets == [n_sp - 1] and n_tp == n_dp and len(bits_of(n_dp)) == 2:
        outs = mega_call(
            n_tp,
            n_dp,
            q,
            k,
            v,
            tk,
            tv,
            grad_out[0],
            out_weight,
            gate,
            windows,
            tile_map.T,
            text_count,
        )
        outs = copy_call(outs)
        return tuple(o[None] for o in outs[:5]) + (outs[5],)

    near_k = [from_offset(k, o) for o in offsets]
    near_v = [from_offset(v, o) for o in offsets]

    s_rel = ring_gather(scaled, "tp")
    w_rel = xor_gather(out_weight, "dp")

    seen = [jnp.repeat(tiles_seen(o), tile, axis=1) for o in [0] + offsets]
    seen.append(jnp.broadcast_to(live[None, :], (count, tk.shape[0])))
    bias = jnp.where(jnp.concatenate(seen, axis=1), 0.0, -1e30).astype(jnp.float32)[:, :, None]

    nat, ga = grad_attn_call(index, s_rel, w_rel)

    heads = width // HD
    groups = GROUPS if heads % GROUPS == 0 else 1
    each = heads // groups
    ks = [k] + near_k + [tk]
    vs = [v] + near_v + [tv]
    nk = len(ks)
    ats, gqs, gks, gvs, gtk, gtv = [], [], [], [], [], []
    for g in range(groups):
        res = attention_call(g * each, each, count, q, ga, bias, ks, vs)
        at, gq = res[:2]
        gk, gv = list(res[2 : 2 + nk]), list(res[2 + nk :])
        ats.append(at)
        gqs.append(gq)
        own_k, own_v = gk[0], gv[0]
        for i, o in enumerate(offsets):
            own_k = own_k + to_offset(gk[1 + i], o).astype(jnp.float32)
            own_v = own_v + to_offset(gv[1 + i], o).astype(jnp.float32)
        gks.append(own_k)
        gvs.append(own_v)
        gtk.append(total_over(gk[-1], "sp"))
        gtv.append(total_over(gv[-1], "sp"))

    parts = dict(enumerate(weight_call(index, nat, ats, n_dp)))
    for bit in bits_of(n_dp):
        got = {
            d: lax.ppermute(parts[d | bit].astype(jnp.bfloat16), "dp", xor_route("dp", bit))
            for d in parts
            if not d & bit
        }
        parts = {d: parts[d].astype(jnp.float32) + got[d].astype(jnp.float32) for d in got}
    weight_grad = total_over(parts[0], "sp")

    def joined(pieces):
        return jnp.concatenate(pieces, axis=1).astype(jnp.bfloat16)[None]

    return (joined(gqs), joined(gks), joined(gvs), joined(gtk), joined(gtv), weight_grad)


def solution(mesh):
    placed = (
        P("dp", "sp", "tp"),
        P("dp", "sp", "tp"),
        P("dp", "sp", "tp"),
        P("dp", None, "tp"),
        P("dp", None, "tp"),
        P("dp", "sp", "tp"),
        P("dp", None),
        P("tp", "dp"),
        P("sp", None),
        P(),
        P("dp"),
    )
    return jax.shard_map(
        per_device,
        mesh=mesh,
        in_specs=placed,
        out_specs=(
            P("dp", "sp", "tp"),
            P("dp", "sp", "tp"),
            P("dp", "sp", "tp"),
            P("dp", None, "tp"),
            P("dp", None, "tp"),
            P("tp", "dp"),
        ),
        check_vma=False,
    )
```

```python
import functools

import jax
import jax.numpy as jnp
from jax import lax
from jax.experimental import pallas as pl
from jax.experimental.pallas import tpu as pltpu
from jax.sharding import PartitionSpec as P

HD = 128
GROUPS = 2
SHARE = 0.5


NT = (((1,), (1,)), ((), ()))
NN = (((1,), (0,)), ((), ()))
TN = (((0,), (0,)), ((), ()))


def mm(a, b, dims):
    return lax.dot_general(a, b, dims, preferred_element_type=jnp.float32)


def ring_gather(block, axis):
    n = lax.axis_size(axis)
    rel = [block] + [None] * (n - 1)
    up = [(i, (i + 1) % n) for i in range(n)]
    down = [((i + 1) % n, i) for i in range(n)]
    ahead = behind = block
    for step in range(1, (n - 1) // 2 + 1):
        ahead = lax.ppermute(ahead, axis, down)
        behind = lax.ppermute(behind, axis, up)
        rel[step] = ahead
        rel[n - step] = behind
    if n % 2 == 0:
        half = block.shape[0] // 2
        first = lax.ppermute(ahead[:half], axis, down)
        second = lax.ppermute(behind[half:], axis, up)
        rel[n // 2] = jnp.concatenate([first, second], axis=0)
    return rel


def xor_route(axis, bit):
    n = lax.axis_size(axis)
    return [(i, i ^ bit) for i in range(n)]


def bits_of(n):
    return [1 << b for b in range(n.bit_length() - 1)]


def xor_gather(block, axis):
    n = lax.axis_size(axis)
    rel = {0: block}
    for bit in reversed(bits_of(n)):
        got = {d | bit: lax.ppermute(b, axis, xor_route(axis, bit)) for d, b in rel.items()}
        rel.update(got)
    return [rel[d] for d in range(n)]


def grad_attn_kernel(n_tp, n_dp, idx_ref, *refs):
    s_refs = refs[:n_tp]
    w_refs = refs[n_tp : n_tp + n_dp]
    nat_ref, ga_ref, acc_ref = refs[n_tp + n_dp :]
    me_tp = idx_ref[0]
    me_dp = idx_ref[1]
    w = s_refs[0].shape[1]
    for j in range(n_tp):
        nat_ref[lax.rem(me_tp + j, n_tp)] = s_refs[j][...]
    r = w_refs[0].shape[1] // w
    acc = None
    for d in range(n_dp):
        for piece in range(r):
            s = nat_ref[(me_dp ^ d) * r + piece]
            term = mm(s, w_refs[d][:, piece * w : (piece + 1) * w], NT)
            if d == 0 and piece == 0:
                acc_ref[...] = term
            else:
                acc_ref[...] += term
    ga_ref[...] = acc_ref[...].astype(jnp.bfloat16)


def grad_attn_call(index, s_rel, w_rel):
    tok, w = s_rel[0].shape
    rows = w_rel[0].shape[0]
    n_tp, n_dp = len(s_rel), len(w_rel)
    vm = pl.BlockSpec(memory_space=pltpu.VMEM)
    return pl.pallas_call(
        functools.partial(grad_attn_kernel, n_tp, n_dp),
        out_shape=(
            jax.ShapeDtypeStruct((n_tp, tok, w), jnp.bfloat16),
            jax.ShapeDtypeStruct((tok, rows), jnp.bfloat16),
        ),
        in_specs=[pl.BlockSpec(memory_space=pltpu.SMEM)] + [vm] * (n_tp + n_dp),
        out_specs=(vm, vm),
        scratch_shapes=[pltpu.VMEM((tok, rows), jnp.float32)],
        cost_estimate=pl.CostEstimate(
            flops=2 * tok * rows * n_tp * w, bytes_accessed=12 << 20, transcendentals=0
        ),
        name="grad_attn",
    )(index, *s_rel, *w_rel)


def attention_kernel(count, nk, q_ref, ga_ref, bias_ref, *refs):
    k_refs = refs[:nk]
    v_refs = refs[nk : 2 * nk]
    at_ref, gq_ref = refs[2 * nk : 2 * nk + 2]
    gk_refs = refs[2 * nk + 2 : 3 * nk + 2]
    gv_refs = refs[3 * nk + 2 : 4 * nk + 2]
    factor = HD ** (-0.5)
    tok = q_ref.shape[0]
    tile = tok // count
    keys = jnp.concatenate([r[...] for r in k_refs], axis=0)
    vals = jnp.concatenate([r[...] for r in v_refs], axis=0)
    gk_sum = gv_sum = None
    for t in range(count):
        rows = slice(t * tile, (t + 1) * tile)
        q = q_ref[rows, :]
        ga = ga_ref[rows, :]
        scores = factor * mm(keys, q, NT) + bias_ref[t]
        top = jnp.max(scores, axis=0, keepdims=True)
        weights = jnp.exp(scores - top)
        total = jnp.sum(weights, axis=0, keepdims=True)
        weights = weights * (1.0 / total)
        probs = weights.astype(jnp.bfloat16)
        att = mm(vals, probs, TN).astype(jnp.bfloat16)
        at_ref[:, rows] = att
        ga_t = ga.astype(jnp.float32).T
        delta = jnp.sum(ga_t * att.astype(jnp.float32), axis=0, keepdims=True)
        gp = mm(vals, ga, NT)
        gs = (weights * (gp - delta)).astype(jnp.bfloat16)
        gq = factor * mm(keys, gs, TN)
        gq_ref[rows, :] = gq.T.astype(jnp.bfloat16)
        gk = factor * mm(gs, q, NN)
        gv = mm(probs, ga, NN)
        gk_sum = gk if t == 0 else gk_sum + gk
        gv_sum = gv if t == 0 else gv_sum + gv
    at = 0
    for i in range(nk):
        n = gk_refs[i].shape[0]
        gk_refs[i][...] = gk_sum[at : at + n].astype(gk_refs[i].dtype)
        gv_refs[i][...] = gv_sum[at : at + n].astype(gv_refs[i].dtype)
        at += n


def attention_call(first, heads, count, q, ga, bias, ks, vs):
    tok = q.shape[0]
    nk = len(ks)

    def head(n):
        return pl.BlockSpec((n, HD), lambda h: (0, first + h))

    def out(n):
        return pl.BlockSpec((n, HD), lambda h: (0, h))

    sizes = [k.shape[0] for k in ks]
    kinds = [jnp.float32 if i == 0 else jnp.bfloat16 for i in range(nk)]
    kinds[-1] = jnp.float32
    total = sum(sizes)
    width = heads * HD
    grads = [jax.ShapeDtypeStruct((n, width), kind) for n, kind in zip(sizes, kinds)]
    return pl.pallas_call(
        functools.partial(attention_kernel, count, nk),
        grid=(heads,),
        out_shape=[
            jax.ShapeDtypeStruct((width, tok), jnp.bfloat16),
            jax.ShapeDtypeStruct((tok, width), jnp.bfloat16),
        ]
        + grads
        + grads,
        in_specs=[head(tok), head(tok), pl.BlockSpec(memory_space=pltpu.VMEM)]
        + [head(n) for n in sizes]
        + [head(n) for n in sizes],
        out_specs=[pl.BlockSpec((HD, tok), lambda h: (h, 0)), out(tok)]
        + [out(n) for n in sizes]
        + [out(n) for n in sizes],
        cost_estimate=pl.CostEstimate(
            flops=heads * 20 * tok * total * HD,
            bytes_accessed=heads * 4 << 20,
            transcendentals=heads * tok * total,
        ),
        name="attention",
    )(q, ga, bias, *ks, *vs)


def weight_kernel(n_dp, groups, idx_ref, nat_ref, *refs):
    at_refs = refs[:groups]
    outs = refs[groups:]
    me_dp = idx_ref[1]
    w = nat_ref.shape[2]
    r = outs[0].shape[1] // w
    for d in range(n_dp):
        for piece in range(r):
            s = nat_ref[(me_dp ^ d) * r + piece]
            row = 0
            for at in at_refs:
                n = at.shape[0]
                outs[d][row : row + n, piece * w : (piece + 1) * w] = mm(at[...], s, NN).astype(
                    outs[d].dtype
                )
                row += n


def weight_call(index, nat, ats, n_dp):
    n_tp, tok, w = nat.shape
    rows = sum(a.shape[0] for a in ats)
    cols = n_tp * w // n_dp
    vm = pl.BlockSpec(memory_space=pltpu.VMEM)
    return pl.pallas_call(
        functools.partial(weight_kernel, n_dp, len(ats)),
        out_shape=[
            jax.ShapeDtypeStruct((rows, cols), jnp.bfloat16 if d & 1 else jnp.float32)
            for d in range(n_dp)
        ],
        in_specs=[pl.BlockSpec(memory_space=pltpu.SMEM)] + [vm] * (1 + len(ats)),
        out_specs=[vm] * n_dp,
        cost_estimate=pl.CostEstimate(
            flops=2 * tok * rows * n_tp * w, bytes_accessed=16 << 20, transcendentals=0
        ),
        name="weight",
    )(index, nat, *ats)


def total_over(block, axis):
    for bit in bits_of(lax.axis_size(axis)):
        got = lax.ppermute(block.astype(jnp.bfloat16), axis, xor_route(axis, bit))
        block = block + got.astype(jnp.float32)
    return block


VMEM = 67043328


def copy_kernel(n, *refs):
    srcs, dsts, sem = refs[:n], refs[n : 2 * n], refs[2 * n]
    copies = [pltpu.make_async_copy(srcs[i], dsts[i], sem.at[i]) for i in reversed(range(n))]
    for c in copies:
        c.start()
    for c in copies:
        c.wait()


def copy_call(arrays):
    n = len(arrays)
    return pl.pallas_call(
        functools.partial(copy_kernel, n),
        out_shape=[jax.ShapeDtypeStruct(a.shape, a.dtype) for a in arrays],
        in_specs=[pl.BlockSpec(memory_space=pltpu.VMEM)] * n,
        out_specs=[pl.BlockSpec(memory_space=pltpu.HBM)] * n,
        scratch_shapes=[pltpu.SemaphoreType.DMA((n,))],
        compiler_params=pltpu.CompilerParams(vmem_limit_bytes=4 << 20),
        name="results",
    )(*arrays)


MESH = pl.DeviceIdType.MESH


def mega_kernel(
    count,
    n_tp,
    n_dp,
    q_hbm,
    k_hbm,
    v_hbm,
    tk_hbm,
    tv_hbm,
    s_hbm,
    w_hbm,
    gate_hbm,
    windows_hbm,
    map_hbm,
    live_hbm,
    gq_ref,
    gk_ref,
    gv_ref,
    gtk_ref,
    gtv_ref,
    gw_ref,
    q_ref,
    gate_ref,
    windows_ref,
    map_ref,
    live_ref,
    keys,
    vals,
    q_far,
    ga_own,
    ga_far,
    win_own,
    win_far,
    raw,
    nat,
    raw_far,
    w_all,
    acc,
    att_t,
    att_far,
    weights_s,
    weights_far,
    gk_sum,
    gv_sum,
    parts,
    outgoing,
    incoming,
    last_out,
    last_in,
    x_out,
    x_in,
    both_outgoing,
    both_incoming,
    both_out,
    both_in,
    ls,
    xs,
    xr,
    ws,
    wr,
    us,
    ds,
    zr,
    fus,
    fds,
    fzr,
    ps,
    pr,
    bps,
    bpr,
    ys,
    yr,
    bys,
    byr,
    gs_sem,
    gr_sem,
):
    factor = HD ** (-0.5)
    bf16, f32 = jnp.bfloat16, jnp.float32
    tok, width = q_ref.shape
    text = tk_hbm.shape[0]
    heads = width // HD
    chunks = heads
    step_rows = width // chunks
    early = heads // 2
    tile = tok // count
    near = tok + text
    w = raw.shape[2]
    half = tok // 2
    wide = raw_far.shape[2]
    me_sp = lax.axis_index("sp")
    me_dp = lax.axis_index("dp")
    me_tp = lax.axis_index("tp")
    far_sp = 1 - me_sp
    core_bit, top_bit = bits_of(n_dp)
    core_peer, top_peer = {"dp": me_dp ^ core_bit}, {"dp": me_dp ^ top_bit}
    sp_far = {"sp": far_sp}
    has_up = me_tp + 1 < n_tp
    has_down = me_tp >= 1
    last = n_tp - 2

    barrier = pltpu.get_barrier_semaphore()
    for peer in (sp_far, core_peer, top_peer):
        pl.semaphore_signal(barrier, inc=1, device_id=peer, device_id_type=MESH)

    @pl.when(has_up)
    def _():
        pl.semaphore_signal(barrier, inc=1, device_id={"tp": me_tp + 1}, device_id_type=MESH)

    @pl.when(has_down)
    def _():
        pl.semaphore_signal(barrier, inc=1, device_id={"tp": me_tp - 1}, device_id_type=MESH)

    loads = [
        pltpu.make_async_copy(a, b, ls.at[i])
        for i, (a, b) in enumerate(
            [
                (s_hbm, raw.at[me_tp]),
                (k_hbm, keys.at[pl.ds(0, tok)]),
                (w_hbm, w_all.at[me_dp]),
                (v_hbm, vals.at[pl.ds(0, tok)]),
                (q_hbm, q_ref),
                (gate_hbm, gate_ref),
                (windows_hbm, windows_ref),
                (tk_hbm, keys.at[pl.ds(tok, text)]),
                (tv_hbm, vals.at[pl.ds(tok, text)]),
                (map_hbm, map_ref),
                (live_hbm, live_ref),
            ]
        )
    ]
    for c in loads:
        c.start()
    pl.semaphore_wait(barrier, 3 + jnp.where(has_up, 1, 0) + jnp.where(has_down, 1, 0))

    def remote(src, dst, send, recv, where):
        return pltpu.make_async_remote_copy(
            src_ref=src,
            dst_ref=dst,
            send_sem=send,
            recv_sem=recv,
            device_id=where,
            device_id_type=MESH,
        )

    def halves(n):
        return [pl.ds(0, n // 2), pl.ds(n // 2, n // 2)]

    x_copies = [
        remote(win_own, win_far, xs.at[0], xr.at[0], sp_far),
        remote(keys.at[pl.ds(0, tok)], keys.at[pl.ds(near, tok)], xs.at[1], xr.at[1], sp_far),
        remote(vals.at[pl.ds(0, tok)], vals.at[pl.ds(near, tok)], xs.at[1], xr.at[2], sp_far),
        remote(
            q_ref.at[:, pl.ds(0, early * HD)],
            q_far.at[:, pl.ds(0, early * HD)],
            xs.at[3],
            xr.at[3],
            sp_far,
        ),
    ] + [
        remote(ga_own.at[rows], ga_far.at[rows], xs.at[4], xr.at[4 + i], sp_far)
        for i, rows in enumerate(halves(tok))
    ]
    q_rest = pl.ds(early * HD, width - early * HD)
    x_copies.append(remote(q_ref.at[:, q_rest], q_far.at[:, q_rest], xs.at[3], xr.at[6], sp_far))
    grad_far = [
        remote(
            raw.at[me_tp, rows, pl.ds(0, wide)],
            raw_far.at[me_tp, rows],
            xs.at[5],
            xr.at[7 + i],
            sp_far,
        )
        for i, rows in enumerate(halves(tok))
    ]

    w_core = remote(w_all.at[me_dp], w_all.at[me_dp], ws.at[0], wr.at[0], core_peer)
    w_top = [
        remote(w_all.at[me_dp, rows], w_all.at[me_dp, rows], ws.at[1], wr.at[1 + i], top_peer)
        for i, rows in enumerate(halves(width))
    ]
    w_relay = [
        remote(
            w_all.at[me_dp ^ top_bit, rows],
            w_all.at[me_dp ^ top_bit, rows],
            ws.at[2],
            wr.at[3 + i],
            core_peer,
        )
        for i, rows in enumerate(halves(width))
    ]

    near_line = (raw, us, ds, zr)
    far_line = (raw_far, fus, fds, fzr)

    def up_copy(line, i, block, where):
        ref = line[0].at[block, halves(tok)[i]]
        return remote(ref, ref, line[1].at[0], line[3].at[block, i], {"tp": where})

    def down_copy(line, i, block, where):
        ref = line[0].at[block, halves(tok)[i]]
        return remote(ref, ref, line[2].at[0], line[3].at[block, i], {"tp": where})

    def start_z(line, i):
        @pl.when(has_up)
        def _():
            up_copy(line, i, me_tp, me_tp + 1).start()

        @pl.when(has_down)
        def _():
            down_copy(line, i, me_tp, me_tp - 1).start()

    def sent_z(line):
        for sent in range(1, n_tp):
            ref = line[0].at[pl.ds(0, sent)]

            @pl.when(me_tp + 1 == sent)
            def _():
                remote(ref, ref, line[1].at[0], line[3].at[0, 0], {"tp": me_tp + 1}).wait_send()

            @pl.when(n_tp - me_tp == sent)
            def _():
                remote(ref, ref, line[2].at[0], line[3].at[0, 0], {"tp": me_tp - 1}).wait_send()

    def relay(line, step, i):
        @pl.when(has_up & (me_tp >= step + 1))
        def _():
            up_copy(line, i, me_tp - 1 - step, me_tp - 1).wait_recv()
            up_copy(line, i, me_tp - 1 - step, me_tp + 1).start()

        @pl.when(has_down & (me_tp + 1 + step < n_tp))
        def _():
            down_copy(line, i, me_tp + 1 + step, me_tp + 1).wait_recv()
            down_copy(line, i, me_tp + 1 + step, me_tp - 1).start()

    def settle(line, step, i):
        @pl.when(jnp.logical_not(has_up) & (me_tp >= step + 1))
        def _():
            up_copy(line, i, me_tp - 1 - step, me_tp - 1).wait_recv()

        @pl.when(jnp.logical_not(has_down) & (me_tp + 1 + step < n_tp))
        def _():
            down_copy(line, i, me_tp + 1 + step, me_tp + 1).wait_recv()

    def each_block(step, act):
        def side(i, carry):
            block = me_tp + (2 * i - 1) * (step + 1)

            @pl.when((block >= 0) & (block < n_tp))
            def _():
                act(block)

            return carry

        lax.fori_loop(0, 2, side, 0)

    loads[1].wait()
    x_copies[1].start()
    loads[0].wait()
    for i in range(2):
        start_z(near_line, i)
    loads[2].wait()
    for c in w_top:
        c.start()
    w_core.start()
    loads[3].wait()
    x_copies[2].start()
    loads[4].wait()
    x_copies[3].start()
    for c in grad_far:
        c.start()
    loads[6].wait()
    win_own[:count, :2] = windows_ref[...]
    x_copies[0].start()
    x_copies[6].start()
    for i in (5, 7, 8, 9, 10):
        loads[i].wait()

    def scale(block, rows=slice(None)):
        gate = gate_ref[:, pl.ds(pl.multiple_of(block * w, HD), w)].astype(f32)
        nat[block, rows] = (raw[block, rows].astype(f32) * gate).astype(bf16)

    def add_block(block):
        acc[...] += mm(nat[block], w_all[block], NT)

    def p_copy(block):
        slot = lax.div(block, 2)
        return remote(outgoing.at[slot], incoming.at[slot], ps.at[0], pr.at[slot], core_peer)

    def part(block):
        parts[block] = mm(att_t[...], nat[block], NN)

        @pl.when(lax.rem(block + me_dp, 2) == 1)
        def _():
            outgoing[lax.div(block, 2)] = parts[block, :, wide:].astype(bf16)
            p_copy(block).start()

    def both_copy(block):
        slot = lax.div(block, 2)
        return remote(
            both_outgoing.at[slot], both_incoming.at[slot], bps.at[0], bpr.at[slot], core_peer
        )

    def part_far(block):
        gate = gate_ref[:, pl.ds(pl.multiple_of(block * w, HD), wide)].astype(f32)
        cols = (raw_far[block].astype(f32) * gate).astype(bf16)
        both = parts[block, :, :wide] + mm(att_far[...], cols, NN)

        @pl.when(lax.rem(block + me_dp, 2) == 1)
        def _():
            both_outgoing[lax.div(block, 2)] = both.astype(bf16)
            both_copy(block).start()

        @pl.when(lax.rem(block + me_dp, 2) == 0)
        def _():
            parts[block, :, :wide] = both

    def bias_of(vis, t, far):
        owner = far_sp if far else me_sp
        place = map_ref[t, owner]

        def span(slab):
            apart = jnp.abs(owner - slab)
            spans = []
            for j in range(count):
                distance = jnp.abs(place - map_ref[j, slab])
                seen = (vis[t : t + 1, 0:1] >= apart) & (vis[t : t + 1, 1:2] >= distance)
                value = jnp.where(seen, 0.0, -1e30).astype(f32)
                spans.append(jnp.broadcast_to(value, (tile, 1)))
            return spans

        place_of = lax.broadcasted_iota(jnp.int32, (text, 1), 0)
        words = jnp.where(place_of < live_ref[0], 0.0, -1e30).astype(f32)
        return jnp.concatenate(span(me_sp) + [words] + span(far_sp), axis=0)

    def soft(q, h_cols, bias):
        scores = factor * mm(keys[:, h_cols], q, NT) + bias
        top = jnp.max(scores, axis=0, keepdims=True)
        weights = jnp.exp(scores - top)
        total = jnp.sum(weights, axis=0, keepdims=True)
        return weights * (1.0 / total)

    def cols_of(h):
        return pl.ds(pl.multiple_of(h * HD, HD), HD)

    def delta_of(ga, att):
        return jnp.sum(ga.astype(f32).T * att.astype(f32), axis=0, keepdims=True)

    def rows_of(t):
        return slice(t * tile, (t + 1) * tile)

    def chunk_rows(h):
        return pl.ds(pl.multiple_of(h * step_rows, step_rows), step_rows)

    def y_copy(h):
        rows = chunk_rows(h)
        return remote(last_out.at[rows], last_in.at[rows], ys.at[0], yr.at[h], top_peer)

    def g_copy(h):
        rows = chunk_rows(h)
        return remote(x_out.at[rows], x_in.at[rows], gs_sem.at[0], gr_sem.at[h], sp_far)

    def both_top(h):
        rows = chunk_rows(h)
        return remote(both_out.at[rows], both_in.at[rows], bys.at[0], byr.at[h], top_peer)

    scale(me_tp)
    for i in range(2):
        relay(near_line, 0, i)
    for i in range(2):
        settle(near_line, 0, i)
    each_block(0, scale)
    x_copies[1].wait_recv()

    def forward(h, carry):
        c = cols_of(h)
        for t in range(count):
            rows = rows_of(t)
            weights_s[h, :, rows] = soft(q_ref[rows, c], c, bias_of(win_own, t, False))
        return carry

    lax.fori_loop(0, heads, forward, 0)
    w_top[0].wait_recv()
    w_relay[0].start()
    for step in range(1, last):
        for i in range(2):
            relay(near_line, step, i)
    w_top[1].wait_recv()
    w_relay[1].start()
    for step in range(1, last):
        for i in range(2):
            settle(near_line, step, i)
    x_copies[2].wait_recv()

    def attend(h, carry):
        c = cols_of(h)
        att_t[c, :] = mm(vals[:, c], weights_s[h].astype(bf16), TN).astype(bf16)
        return carry

    lax.fori_loop(0, heads, attend, 0)
    part(me_tp)
    each_block(0, part)
    for step in range(1, last):
        each_block(step, scale)
        each_block(step, part)
    w_core.wait_recv()
    for c in w_relay:
        c.wait_recv()
    acc[...] = mm(nat[me_tp], w_all[me_tp], NT)
    for step in range(last):
        each_block(step, add_block)

    away = me_dp ^ top_bit

    def send_top():
        p_copy(away).wait_recv()

        def chunk(h, carry):
            rows = chunk_rows(h)
            mine = parts[away, rows, wide:]
            pair = mine + incoming[lax.div(away, 2), rows, :].astype(f32)
            last_out[rows, :] = pair.astype(bf16)
            y_copy(h).start()
            return carry

        lax.fori_loop(0, chunks, chunk, 0)

    def send_both_top():
        both_copy(away).wait_recv()

        def chunk(h, carry):
            rows = chunk_rows(h)
            mine = parts[away, rows, :wide]
            pair = mine + both_incoming[lax.div(away, 2), rows, :].astype(f32)
            both_out[rows, :] = pair.astype(bf16)
            both_top(h).start()
            return carry

        lax.fori_loop(0, chunks, chunk, 0)

    late = jnp.abs(away - me_tp) == n_tp - 1

    @pl.when(jnp.logical_not(late))
    def _():
        send_top()

    for i in range(2):
        rows = slice(i * half, (i + 1) * half)
        grad_far[i].wait_recv()
        start_z(far_line, i)
        settle(near_line, last, i)

        def add_half(block):
            scale(block, rows)
            acc[rows] += mm(nat[block, rows], w_all[block], NT)

        each_block(last, add_half)
        ga_own[rows] = acc[rows].astype(bf16)
        x_copies[4 + i].start()
    each_block(last, part)

    def backward(h, carry):
        c = cols_of(h)
        for t in range(count):
            rows = rows_of(t)
            q = q_ref[rows, c]
            ga = ga_own[rows, c]
            weights = weights_s[h, :, rows]
            delta = delta_of(ga, att_t[c, rows])
            gp = mm(vals[:, c], ga, NT)
            gs = (weights * (gp - delta)).astype(bf16)
            gq_ref[rows, c] = (factor * mm(keys[:, c], gs, TN)).T.astype(bf16)
            gk = mm(gs[:near], q, NN)
            gv = mm(weights[:near].astype(bf16), ga, NN)
            if t == 0:
                gk_sum[:, c] = gk
                gv_sum[:, c] = gv
            else:
                gk_sum[:, c] += gk
                gv_sum[:, c] += gv

        return carry

    def pass_on(h):
        y_copy(h).wait_recv()
        rows = chunk_rows(h)
        mine = parts[me_dp, rows, wide:] + incoming[lax.div(me_dp, 2), rows, :].astype(f32)
        total = mine + last_in[rows, :].astype(f32)
        gw_ref[rows, wide:] = total
        x_out[rows, :] = total.astype(bf16)
        g_copy(h).start()

    x_copies[0].wait_recv()
    x_copies[3].wait_recv()

    def far_soft(h, carry):
        c = cols_of(h)
        for t in range(count):
            rows = rows_of(t)
            weights = soft(q_far[rows, c], c, bias_of(win_far, t, True))
            weights_far[h, :, rows] = weights[:near]
            att_far[c, rows] = mm(vals[:, c], weights.astype(bf16), TN).astype(bf16)
        return carry

    lax.fori_loop(0, early, far_soft, 0)

    @pl.when(late)
    def _():
        send_top()

    for i in range(2):
        relay(far_line, 0, i)
    x_copies[6].wait_recv()
    lax.fori_loop(early, heads, far_soft, 0)
    part_far(me_tp)
    for step in range(last):
        for i in range(2):
            if step:
                relay(far_line, step, i)
            settle(far_line, step, i)
        each_block(step, part_far)

    def pass_next(h, carry):
        pass_on(h)
        return carry

    first = lax.rem(me_dp, 2) == 0

    @pl.when(first)
    def _():
        p_copy(me_dp).wait_recv()
        lax.fori_loop(0, early, pass_next, 0)

    @pl.when(jnp.logical_not(late))
    def _():
        send_both_top()

    lax.fori_loop(0, heads - 2, backward, 0)
    for i in range(2):
        settle(far_line, last, i)
    each_block(last, part_far)

    @pl.when(first)
    def _():
        lax.fori_loop(early, chunks, pass_next, 0)

    lax.fori_loop(heads - 2, heads, backward, 0)
    x_copies[4].wait_recv()
    x_copies[5].wait_recv()

    @pl.when(jnp.logical_not(first))
    def _():
        p_copy(me_dp).wait_recv()
        lax.fori_loop(0, chunks, pass_next, 0)

    @pl.when(late)
    def _():
        send_both_top()


    def far(h, carry):
        c = cols_of(h)
        gk_all = gk_sum[:, c]
        gv_all = gv_sum[:, c]
        for t in range(count):
            rows = rows_of(t)
            q = q_far[rows, c]
            ga = ga_far[rows, c]
            weights = weights_far[h, :, rows]
            delta = delta_of(ga, att_far[c, rows])
            gp = mm(vals[:near, c], ga, NT)
            gs = (weights * (gp - delta)).astype(bf16)
            gk_all += mm(gs, q, NN)
            gv_all += mm(weights.astype(bf16), ga, NN)
        gk_ref[:, c] = (factor * gk_all[:tok]).astype(bf16)
        gtk_ref[:, c] = (factor * gk_all[tok:]).astype(bf16)
        gv_ref[:, c] = gv_all[:tok].astype(bf16)
        gtv_ref[:, c] = gv_all[tok:].astype(bf16)
        return carry

    lax.fori_loop(0, heads, far, 0)
    both_copy(me_dp).wait_recv()

    def finish_both(h, carry):
        rows = chunk_rows(h)
        both_top(h).wait_recv()
        mine = parts[me_dp, rows, :wide] + both_incoming[lax.div(me_dp, 2), rows, :].astype(f32)
        gw_ref[rows, :wide] = mine + both_in[rows, :].astype(f32)
        return carry

    lax.fori_loop(0, chunks, finish_both, 0)
    both_keys, pair = pl.ds(0, 2 * tok), pl.ds(0, n_dp // 2)
    for c in [
        x_copies[0],
        remote(keys.at[both_keys], keys.at[both_keys], xs.at[1], xr.at[1], sp_far),
        remote(q_ref, q_far, xs.at[3], xr.at[3], sp_far),
        remote(ga_own, ga_far, xs.at[4], xr.at[4], sp_far),
        remote(raw_far.at[me_tp], raw_far.at[me_tp], xs.at[5], xr.at[7], sp_far),
        w_core,
        remote(w_all.at[me_dp], w_all.at[me_dp], ws.at[1], wr.at[1], top_peer),
        remote(w_all.at[me_dp], w_all.at[me_dp], ws.at[2], wr.at[3], core_peer),
        remote(outgoing.at[pair], incoming.at[pair], ps.at[0], pr.at[0], core_peer),
        remote(both_outgoing.at[pair], both_incoming.at[pair], bps.at[0], bpr.at[0], core_peer),
        remote(last_out, last_in, ys.at[0], yr.at[0], top_peer),
        remote(both_out, both_in, bys.at[0], byr.at[0], top_peer),
    ]:
        c.wait_send()
    for line in (near_line, far_line):
        sent_z(line)

    def finish(h, carry):
        rows = chunk_rows(h)
        g_copy(h).wait_recv()
        gw_ref[rows, wide:] += x_in[rows, :].astype(f32)
        return carry

    lax.fori_loop(0, chunks, finish, 0)
    remote(x_out, x_in, gs_sem.at[0], gr_sem.at[0], sp_far).wait_send()


def mega_call(n_tp, n_dp, q, k, v, tk, tv, s, w, gate, windows, tile_map, text_count):
    tok, width = q.shape
    text = tk.shape[0]
    heads = width // HD
    cols = w.shape[1]
    total = 2 * tok + text
    near = tok + text
    count = tile_map.shape[0]
    pairs = n_dp // 2
    wide = int(cols * SHARE) // HD * HD
    bf16, f32 = jnp.bfloat16, jnp.float32
    dma = pltpu.SemaphoreType.DMA
    shapes = [
        ((tok, width), bf16),
        ((tok, width), bf16),
        ((tok, width), bf16),
        ((text, width), bf16),
        ((text, width), bf16),
        ((width, cols), f32),
    ]
    small = [
        pltpu.VMEM((tok, width), bf16),
        pltpu.VMEM(gate.shape, bf16),
        pltpu.VMEM(windows.shape, jnp.int32),
        pltpu.SMEM(tile_map.shape, jnp.int32),
        pltpu.SMEM(text_count.shape, jnp.int32),
    ]
    scratch = [
        ((total, width), bf16),
        ((total, width), bf16),
        ((tok, width), bf16),
        ((tok, width), bf16),
        ((tok, width), bf16),
        ((count + -count % 8, HD), jnp.int32),
        ((count + -count % 8, HD), jnp.int32),
        ((n_tp, tok, s.shape[1]), bf16),
        ((n_tp, tok, s.shape[1]), bf16),
        ((n_tp, tok, wide), bf16),
        ((n_dp, width, cols), bf16),
        ((tok, width), f32),
        ((width, tok), bf16),
        ((width, tok), bf16),
        ((heads, total, tok), f32),
        ((heads, near, tok), f32),
        ((near, width), f32),
        ((near, width), f32),
        ((n_dp, width, cols), f32),
        ((pairs, width, cols - wide), bf16),
        ((pairs, width, cols - wide), bf16),
        ((width, cols - wide), bf16),
        ((width, cols - wide), bf16),
        ((width, cols - wide), bf16),
        ((width, cols - wide), bf16),
        ((pairs, width, wide), bf16),
        ((pairs, width, wide), bf16),
        ((width, wide), bf16),
        ((width, wide), bf16),
    ]
    sems = [(11,), (6,), (9,), (3,), (5,)] + [(1,), (1,), (n_tp, 2)] * 2 + [(1,), (pairs,)] * 2
    sems += [(1,), (heads,)] * 3
    held = sum(jnp.dtype(b).itemsize * a[0] * a[1] for a, b in shapes)
    return pl.pallas_call(
        functools.partial(mega_kernel, count, n_tp, n_dp),
        out_shape=[pltpu.VMEM(a, b) for a, b in shapes],
        in_specs=[pl.BlockSpec(memory_space=pltpu.HBM)] * 11,
        out_specs=[pl.BlockSpec(memory_space=pltpu.VMEM)] * 6,
        scratch_shapes=small + [pltpu.VMEM(a, b) for a, b in scratch] + [dma(n) for n in sems],
        compiler_params=pltpu.CompilerParams(
            collective_id=0, has_side_effects=True, vmem_limit_bytes=VMEM - held - (1 << 18)
        ),
        name="attention_backward",
    )(q, k, v, tk, tv, s, w, gate, windows, tile_map, text_count)


def per_device(
    query,
    key,
    value,
    text_key,
    text_value,
    grad_out,
    gate,
    out_weight,
    windows,
    tile_map,
    text_count,
):
    q, k, v = query[0], key[0], value[0]
    tk, tv = text_key[0], text_value[0]
    tok, width = q.shape
    n_sp = lax.axis_size("sp")
    n_dp = lax.axis_size("dp")
    n_tp = lax.axis_size("tp")
    me_sp = lax.axis_index("sp")
    me_tp = lax.axis_index("tp")
    me_dp = lax.axis_index("dp")
    index = jnp.stack([me_tp, me_dp]).astype(jnp.int32)

    offsets = sorted({1 % n_sp, (n_sp - 1) % n_sp} - {0})

    def from_offset(block, offset):
        route = [((i + offset) % n_sp, i) for i in range(n_sp)]
        route = [(a, b) for a, b in route if abs(a - b) <= 1]
        return lax.ppermute(block, "sp", route)

    def to_offset(block, offset):
        route = [(i, (i + offset) % n_sp) for i in range(n_sp)]
        route = [(a, b) for a, b in route if abs(a - b) <= 1]
        return lax.ppermute(block, "sp", route)

    own_gate = lax.dynamic_slice_in_dim(gate[0], me_tp * width, width, 0)
    scaled = (grad_out[0].astype(jnp.float32) * own_gate.astype(jnp.float32)[None, :]).astype(
        jnp.bfloat16
    )
    own_map = lax.dynamic_index_in_dim(tile_map, me_sp, 0, keepdims=False)
    count = own_map.shape[0]
    tile = tok // count
    live = jnp.arange(tk.shape[0], dtype=jnp.int32) < text_count[0]

    def tiles_seen(o):
        other = lax.rem(me_sp + o, n_sp)
        apart = jnp.abs(other - me_sp)
        other_map = lax.dynamic_index_in_dim(tile_map, other, 0, keepdims=False)
        near_time = (apart <= windows[:, 0]) & (apart <= 1)
        near_space = jnp.abs(own_map[:, None] - other_map[None, :]) <= windows[:, 1][:, None]
        return near_time[:, None] & near_space

    if offsets == [n_sp - 1] and n_tp == n_dp and len(bits_of(n_dp)) == 2:
        outs = mega_call(
            n_tp,
            n_dp,
            q,
            k,
            v,
            tk,
            tv,
            grad_out[0],
            out_weight,
            gate,
            windows,
            tile_map.T,
            text_count,
        )
        outs = copy_call(outs)
        return tuple(o[None] for o in outs[:5]) + (outs[5],)

    near_k = [from_offset(k, o) for o in offsets]
    near_v = [from_offset(v, o) for o in offsets]

    s_rel = ring_gather(scaled, "tp")
    w_rel = xor_gather(out_weight, "dp")

    seen = [jnp.repeat(tiles_seen(o), tile, axis=1) for o in [0] + offsets]
    seen.append(jnp.broadcast_to(live[None, :], (count, tk.shape[0])))
    bias = jnp.where(jnp.concatenate(seen, axis=1), 0.0, -1e30).astype(jnp.float32)[:, :, None]

    nat, ga = grad_attn_call(index, s_rel, w_rel)

    heads = width // HD
    groups = GROUPS if heads % GROUPS == 0 else 1
    each = heads // groups
    ks = [k] + near_k + [tk]
    vs = [v] + near_v + [tv]
    nk = len(ks)
    ats, gqs, gks, gvs, gtk, gtv = [], [], [], [], [], []
    for g in range(groups):
        res = attention_call(g * each, each, count, q, ga, bias, ks, vs)
        at, gq = res[:2]
        gk, gv = list(res[2 : 2 + nk]), list(res[2 + nk :])
        ats.append(at)
        gqs.append(gq)
        own_k, own_v = gk[0], gv[0]
        for i, o in enumerate(offsets):
            own_k = own_k + to_offset(gk[1 + i], o).astype(jnp.float32)
            own_v = own_v + to_offset(gv[1 + i], o).astype(jnp.float32)
        gks.append(own_k)
        gvs.append(own_v)
        gtk.append(total_over(gk[-1], "sp"))
        gtv.append(total_over(gv[-1], "sp"))

    parts = dict(enumerate(weight_call(index, nat, ats, n_dp)))
    for bit in bits_of(n_dp):
        got = {
            d: lax.ppermute(parts[d | bit].astype(jnp.bfloat16), "dp", xor_route("dp", bit))
            for d in parts
            if not d & bit
        }
        parts = {d: parts[d].astype(jnp.float32) + got[d].astype(jnp.float32) for d in got}
    weight_grad = total_over(parts[0], "sp")

    def joined(pieces):
        return jnp.concatenate(pieces, axis=1).astype(jnp.bfloat16)[None]

    return (joined(gqs), joined(gks), joined(gvs), joined(gtk), joined(gtv), weight_grad)


def solution(mesh):
    placed = (
        P("dp", "sp", "tp"),
        P("dp", "sp", "tp"),
        P("dp", "sp", "tp"),
        P("dp", None, "tp"),
        P("dp", None, "tp"),
        P("dp", "sp", "tp"),
        P("dp", None),
        P("tp", "dp"),
        P("sp", None),
        P(),
        P("dp"),
    )
    return jax.shard_map(
        per_device,
        mesh=mesh,
        in_specs=placed,
        out_specs=(
            P("dp", "sp", "tp"),
            P("dp", "sp", "tp"),
            P("dp", "sp", "tp"),
            P("dp", None, "tp"),
            P("dp", None, "tp"),
            P("tp", "dp"),
        ),
        check_vma=False,
    )
```

```python
import functools

import jax
import jax.numpy as jnp
from jax import lax
from jax.experimental import pallas as pl
from jax.experimental.pallas import tpu as pltpu
from jax.sharding import PartitionSpec as P

HD = 128
GROUPS = 2
SHARE = 0.5


NT = (((1,), (1,)), ((), ()))
NN = (((1,), (0,)), ((), ()))
TN = (((0,), (0,)), ((), ()))


def mm(a, b, dims):
    return lax.dot_general(a, b, dims, preferred_element_type=jnp.float32)


def ring_gather(block, axis):
    n = lax.axis_size(axis)
    rel = [block] + [None] * (n - 1)
    up = [(i, (i + 1) % n) for i in range(n)]
    down = [((i + 1) % n, i) for i in range(n)]
    ahead = behind = block
    for step in range(1, (n - 1) // 2 + 1):
        ahead = lax.ppermute(ahead, axis, down)
        behind = lax.ppermute(behind, axis, up)
        rel[step] = ahead
        rel[n - step] = behind
    if n % 2 == 0:
        half = block.shape[0] // 2
        first = lax.ppermute(ahead[:half], axis, down)
        second = lax.ppermute(behind[half:], axis, up)
        rel[n // 2] = jnp.concatenate([first, second], axis=0)
    return rel


def xor_route(axis, bit):
    n = lax.axis_size(axis)
    return [(i, i ^ bit) for i in range(n)]


def bits_of(n):
    return [1 << b for b in range(n.bit_length() - 1)]


def xor_gather(block, axis):
    n = lax.axis_size(axis)
    rel = {0: block}
    for bit in reversed(bits_of(n)):
        got = {d | bit: lax.ppermute(b, axis, xor_route(axis, bit)) for d, b in rel.items()}
        rel.update(got)
    return [rel[d] for d in range(n)]


def grad_attn_kernel(n_tp, n_dp, idx_ref, *refs):
    s_refs = refs[:n_tp]
    w_refs = refs[n_tp : n_tp + n_dp]
    nat_ref, ga_ref, acc_ref = refs[n_tp + n_dp :]
    me_tp = idx_ref[0]
    me_dp = idx_ref[1]
    w = s_refs[0].shape[1]
    for j in range(n_tp):
        nat_ref[lax.rem(me_tp + j, n_tp)] = s_refs[j][...]
    r = w_refs[0].shape[1] // w
    acc = None
    for d in range(n_dp):
        for piece in range(r):
            s = nat_ref[(me_dp ^ d) * r + piece]
            term = mm(s, w_refs[d][:, piece * w : (piece + 1) * w], NT)
            if d == 0 and piece == 0:
                acc_ref[...] = term
            else:
                acc_ref[...] += term
    ga_ref[...] = acc_ref[...].astype(jnp.bfloat16)


def grad_attn_call(index, s_rel, w_rel):
    tok, w = s_rel[0].shape
    rows = w_rel[0].shape[0]
    n_tp, n_dp = len(s_rel), len(w_rel)
    vm = pl.BlockSpec(memory_space=pltpu.VMEM)
    return pl.pallas_call(
        functools.partial(grad_attn_kernel, n_tp, n_dp),
        out_shape=(
            jax.ShapeDtypeStruct((n_tp, tok, w), jnp.bfloat16),
            jax.ShapeDtypeStruct((tok, rows), jnp.bfloat16),
        ),
        in_specs=[pl.BlockSpec(memory_space=pltpu.SMEM)] + [vm] * (n_tp + n_dp),
        out_specs=(vm, vm),
        scratch_shapes=[pltpu.VMEM((tok, rows), jnp.float32)],
        cost_estimate=pl.CostEstimate(
            flops=2 * tok * rows * n_tp * w, bytes_accessed=12 << 20, transcendentals=0
        ),
        name="grad_attn",
    )(index, *s_rel, *w_rel)


def attention_kernel(count, nk, q_ref, ga_ref, bias_ref, *refs):
    k_refs = refs[:nk]
    v_refs = refs[nk : 2 * nk]
    at_ref, gq_ref = refs[2 * nk : 2 * nk + 2]
    gk_refs = refs[2 * nk + 2 : 3 * nk + 2]
    gv_refs = refs[3 * nk + 2 : 4 * nk + 2]
    factor = HD ** (-0.5)
    tok = q_ref.shape[0]
    tile = tok // count
    keys = jnp.concatenate([r[...] for r in k_refs], axis=0)
    vals = jnp.concatenate([r[...] for r in v_refs], axis=0)
    gk_sum = gv_sum = None
    for t in range(count):
        rows = slice(t * tile, (t + 1) * tile)
        q = q_ref[rows, :]
        ga = ga_ref[rows, :]
        scores = factor * mm(keys, q, NT) + bias_ref[t]
        top = jnp.max(scores, axis=0, keepdims=True)
        weights = jnp.exp(scores - top)
        total = jnp.sum(weights, axis=0, keepdims=True)
        weights = weights * (1.0 / total)
        probs = weights.astype(jnp.bfloat16)
        att = mm(vals, probs, TN).astype(jnp.bfloat16)
        at_ref[:, rows] = att
        ga_t = ga.astype(jnp.float32).T
        delta = jnp.sum(ga_t * att.astype(jnp.float32), axis=0, keepdims=True)
        gp = mm(vals, ga, NT)
        gs = (weights * (gp - delta)).astype(jnp.bfloat16)
        gq = factor * mm(keys, gs, TN)
        gq_ref[rows, :] = gq.T.astype(jnp.bfloat16)
        gk = factor * mm(gs, q, NN)
        gv = mm(probs, ga, NN)
        gk_sum = gk if t == 0 else gk_sum + gk
        gv_sum = gv if t == 0 else gv_sum + gv
    at = 0
    for i in range(nk):
        n = gk_refs[i].shape[0]
        gk_refs[i][...] = gk_sum[at : at + n].astype(gk_refs[i].dtype)
        gv_refs[i][...] = gv_sum[at : at + n].astype(gv_refs[i].dtype)
        at += n


def attention_call(first, heads, count, q, ga, bias, ks, vs):
    tok = q.shape[0]
    nk = len(ks)

    def head(n):
        return pl.BlockSpec((n, HD), lambda h: (0, first + h))

    def out(n):
        return pl.BlockSpec((n, HD), lambda h: (0, h))

    sizes = [k.shape[0] for k in ks]
    kinds = [jnp.float32 if i == 0 else jnp.bfloat16 for i in range(nk)]
    kinds[-1] = jnp.float32
    total = sum(sizes)
    width = heads * HD
    grads = [jax.ShapeDtypeStruct((n, width), kind) for n, kind in zip(sizes, kinds)]
    return pl.pallas_call(
        functools.partial(attention_kernel, count, nk),
        grid=(heads,),
        out_shape=[
            jax.ShapeDtypeStruct((width, tok), jnp.bfloat16),
            jax.ShapeDtypeStruct((tok, width), jnp.bfloat16),
        ]
        + grads
        + grads,
        in_specs=[head(tok), head(tok), pl.BlockSpec(memory_space=pltpu.VMEM)]
        + [head(n) for n in sizes]
        + [head(n) for n in sizes],
        out_specs=[pl.BlockSpec((HD, tok), lambda h: (h, 0)), out(tok)]
        + [out(n) for n in sizes]
        + [out(n) for n in sizes],
        cost_estimate=pl.CostEstimate(
            flops=heads * 20 * tok * total * HD,
            bytes_accessed=heads * 4 << 20,
            transcendentals=heads * tok * total,
        ),
        name="attention",
    )(q, ga, bias, *ks, *vs)


def weight_kernel(n_dp, groups, idx_ref, nat_ref, *refs):
    at_refs = refs[:groups]
    outs = refs[groups:]
    me_dp = idx_ref[1]
    w = nat_ref.shape[2]
    r = outs[0].shape[1] // w
    for d in range(n_dp):
        for piece in range(r):
            s = nat_ref[(me_dp ^ d) * r + piece]
            row = 0
            for at in at_refs:
                n = at.shape[0]
                outs[d][row : row + n, piece * w : (piece + 1) * w] = mm(at[...], s, NN).astype(
                    outs[d].dtype
                )
                row += n


def weight_call(index, nat, ats, n_dp):
    n_tp, tok, w = nat.shape
    rows = sum(a.shape[0] for a in ats)
    cols = n_tp * w // n_dp
    vm = pl.BlockSpec(memory_space=pltpu.VMEM)
    return pl.pallas_call(
        functools.partial(weight_kernel, n_dp, len(ats)),
        out_shape=[
            jax.ShapeDtypeStruct((rows, cols), jnp.bfloat16 if d & 1 else jnp.float32)
            for d in range(n_dp)
        ],
        in_specs=[pl.BlockSpec(memory_space=pltpu.SMEM)] + [vm] * (1 + len(ats)),
        out_specs=[vm] * n_dp,
        cost_estimate=pl.CostEstimate(
            flops=2 * tok * rows * n_tp * w, bytes_accessed=16 << 20, transcendentals=0
        ),
        name="weight",
    )(index, nat, *ats)


def total_over(block, axis):
    for bit in bits_of(lax.axis_size(axis)):
        got = lax.ppermute(block.astype(jnp.bfloat16), axis, xor_route(axis, bit))
        block = block + got.astype(jnp.float32)
    return block


VMEM = 67043328


def copy_kernel(n, *refs):
    srcs, dsts, sem = refs[:n], refs[n : 2 * n], refs[2 * n]
    copies = [pltpu.make_async_copy(srcs[i], dsts[i], sem.at[i]) for i in reversed(range(n))]
    for c in copies:
        c.start()
    for c in copies:
        c.wait()


def copy_call(arrays):
    n = len(arrays)
    return pl.pallas_call(
        functools.partial(copy_kernel, n),
        out_shape=[jax.ShapeDtypeStruct(a.shape, a.dtype) for a in arrays],
        in_specs=[pl.BlockSpec(memory_space=pltpu.VMEM)] * n,
        out_specs=[pl.BlockSpec(memory_space=pltpu.HBM)] * n,
        scratch_shapes=[pltpu.SemaphoreType.DMA((n,))],
        compiler_params=pltpu.CompilerParams(vmem_limit_bytes=4 << 20),
        name="results",
    )(*arrays)


MESH = pl.DeviceIdType.MESH


def mega_kernel(
    count,
    n_tp,
    n_dp,
    q_hbm,
    k_hbm,
    v_hbm,
    tk_hbm,
    tv_hbm,
    s_hbm,
    w_hbm,
    gate_hbm,
    windows_hbm,
    map_hbm,
    live_hbm,
    gq_ref,
    gk_ref,
    gv_ref,
    gtk_ref,
    gtv_ref,
    gw_ref,
    q_ref,
    gate_ref,
    windows_ref,
    map_ref,
    live_ref,
    keys,
    vals,
    q_far,
    ga_own,
    ga_far,
    win_own,
    win_far,
    raw,
    nat,
    raw_far,
    w_all,
    acc,
    att_t,
    att_far,
    weights_s,
    weights_far,
    gk_sum,
    gv_sum,
    parts,
    outgoing,
    incoming,
    last_out,
    last_in,
    x_out,
    x_in,
    both_outgoing,
    both_incoming,
    both_out,
    both_in,
    ls,
    xs,
    xr,
    ws,
    wr,
    us,
    ds,
    zr,
    fus,
    fds,
    fzr,
    ps,
    pr,
    bps,
    bpr,
    ys,
    yr,
    bys,
    byr,
    gs_sem,
    gr_sem,
):
    factor = HD ** (-0.5)
    bf16, f32 = jnp.bfloat16, jnp.float32
    tok, width = q_ref.shape
    text = tk_hbm.shape[0]
    heads = width // HD
    chunks = heads
    step_rows = width // chunks
    early = heads // 2
    tile = tok // count
    near = tok + text
    w = raw.shape[2]
    half = tok // 2
    wide = raw_far.shape[2]
    me_sp = lax.axis_index("sp")
    me_dp = lax.axis_index("dp")
    me_tp = lax.axis_index("tp")
    far_sp = 1 - me_sp
    core_bit, top_bit = bits_of(n_dp)
    core_peer, top_peer = {"dp": me_dp ^ core_bit}, {"dp": me_dp ^ top_bit}
    sp_far = {"sp": far_sp}
    has_up = me_tp + 1 < n_tp
    has_down = me_tp >= 1
    last = n_tp - 2

    barrier = pltpu.get_barrier_semaphore()
    for peer in (sp_far, core_peer, top_peer):
        pl.semaphore_signal(barrier, inc=1, device_id=peer, device_id_type=MESH)

    @pl.when(has_up)
    def _():
        pl.semaphore_signal(barrier, inc=1, device_id={"tp": me_tp + 1}, device_id_type=MESH)

    @pl.when(has_down)
    def _():
        pl.semaphore_signal(barrier, inc=1, device_id={"tp": me_tp - 1}, device_id_type=MESH)

    loads = [
        pltpu.make_async_copy(a, b, ls.at[i])
        for i, (a, b) in enumerate(
            [
                (s_hbm, raw.at[me_tp]),
                (k_hbm, keys.at[pl.ds(0, tok)]),
                (w_hbm, w_all.at[me_dp]),
                (v_hbm, vals.at[pl.ds(0, tok)]),
                (q_hbm, q_ref),
                (gate_hbm, gate_ref),
                (windows_hbm, windows_ref),
                (tk_hbm, keys.at[pl.ds(tok, text)]),
                (tv_hbm, vals.at[pl.ds(tok, text)]),
                (map_hbm, map_ref),
                (live_hbm, live_ref),
            ]
        )
    ]
    for c in loads:
        c.start()
    pl.semaphore_wait(barrier, 3 + jnp.where(has_up, 1, 0) + jnp.where(has_down, 1, 0))

    def remote(src, dst, send, recv, where):
        return pltpu.make_async_remote_copy(
            src_ref=src,
            dst_ref=dst,
            send_sem=send,
            recv_sem=recv,
            device_id=where,
            device_id_type=MESH,
        )

    def halves(n):
        return [pl.ds(0, n // 2), pl.ds(n // 2, n // 2)]

    x_copies = [
        remote(win_own, win_far, xs.at[0], xr.at[0], sp_far),
        remote(keys.at[pl.ds(0, tok)], keys.at[pl.ds(near, tok)], xs.at[1], xr.at[1], sp_far),
        remote(vals.at[pl.ds(0, tok)], vals.at[pl.ds(near, tok)], xs.at[1], xr.at[2], sp_far),
        remote(
            q_ref.at[:, pl.ds(0, early * HD)],
            q_far.at[:, pl.ds(0, early * HD)],
            xs.at[3],
            xr.at[3],
            sp_far,
        ),
    ] + [
        remote(ga_own.at[rows], ga_far.at[rows], xs.at[4], xr.at[4], sp_far)
        for i, rows in enumerate(halves(tok))
    ]
    q_rest = pl.ds(early * HD, width - early * HD)
    x_copies.append(remote(q_ref.at[:, q_rest], q_far.at[:, q_rest], xs.at[3], xr.at[6], sp_far))
    grad_far = [
        remote(
            raw.at[me_tp, rows, pl.ds(0, wide)],
            raw_far.at[me_tp, rows],
            xs.at[5],
            xr.at[5 + 2 * i],
            sp_far,
        )
        for i, rows in enumerate(halves(tok))
    ]

    w_core = remote(w_all.at[me_dp], w_all.at[me_dp], ws.at[0], wr.at[0], core_peer)
    w_top = [
        remote(w_all.at[me_dp, rows], w_all.at[me_dp, rows], ws.at[1], wr.at[1 + i], top_peer)
        for i, rows in enumerate(halves(width))
    ]
    w_relay = [
        remote(
            w_all.at[me_dp ^ top_bit, rows],
            w_all.at[me_dp ^ top_bit, rows],
            ws.at[2],
            wr.at[3],
            core_peer,
        )
        for i, rows in enumerate(halves(width))
    ]

    near_line = (raw, us, ds, zr)
    far_line = (raw_far, fus, fds, fzr)

    def up_copy(line, i, block, where):
        ref = line[0].at[block, halves(tok)[i]]
        return remote(ref, ref, line[1].at[0], line[3].at[block, i], {"tp": where})

    def down_copy(line, i, block, where):
        ref = line[0].at[block, halves(tok)[i]]
        return remote(ref, ref, line[2].at[0], line[3].at[block, i], {"tp": where})

    def start_z(line, i):
        @pl.when(has_up)
        def _():
            up_copy(line, i, me_tp, me_tp + 1).start()

        @pl.when(has_down)
        def _():
            down_copy(line, i, me_tp, me_tp - 1).start()

    def sent_z(line):
        for sent in range(1, n_tp):
            ref = line[0].at[pl.ds(0, sent)]

            @pl.when(me_tp + 1 == sent)
            def _():
                remote(ref, ref, line[1].at[0], line[3].at[0, 0], {"tp": me_tp + 1}).wait_send()

            @pl.when(n_tp - me_tp == sent)
            def _():
                remote(ref, ref, line[2].at[0], line[3].at[0, 0], {"tp": me_tp - 1}).wait_send()

    def relay(line, step, i):
        @pl.when(has_up & (me_tp >= step + 1))
        def _():
            up_copy(line, i, me_tp - 1 - step, me_tp - 1).wait_recv()
            up_copy(line, i, me_tp - 1 - step, me_tp + 1).start()

        @pl.when(has_down & (me_tp + 1 + step < n_tp))
        def _():
            down_copy(line, i, me_tp + 1 + step, me_tp + 1).wait_recv()
            down_copy(line, i, me_tp + 1 + step, me_tp - 1).start()

    def settle(line, step, i):
        @pl.when(jnp.logical_not(has_up) & (me_tp >= step + 1))
        def _():
            up_copy(line, i, me_tp - 1 - step, me_tp - 1).wait_recv()

        @pl.when(jnp.logical_not(has_down) & (me_tp + 1 + step < n_tp))
        def _():
            down_copy(line, i, me_tp + 1 + step, me_tp + 1).wait_recv()

    def each_block(step, act):
        def side(i, carry):
            block = me_tp + (2 * i - 1) * (step + 1)

            @pl.when((block >= 0) & (block < n_tp))
            def _():
                act(block)

            return carry

        lax.fori_loop(0, 2, side, 0)

    loads[1].wait()
    x_copies[1].start()
    loads[0].wait()
    for i in range(2):
        start_z(near_line, i)
    loads[2].wait()
    for c in w_top:
        c.start()
    w_core.start()
    loads[3].wait()
    x_copies[2].start()
    loads[4].wait()
    x_copies[3].start()
    for c in grad_far:
        c.start()
    loads[6].wait()
    win_own[:count, :2] = windows_ref[...]
    x_copies[0].start()
    x_copies[6].start()
    for i in (5, 7, 8, 9, 10):
        loads[i].wait()

    def scale(block, rows=slice(None)):
        gate = gate_ref[:, pl.ds(pl.multiple_of(block * w, HD), w)].astype(f32)
        nat[block, rows] = (raw[block, rows].astype(f32) * gate).astype(bf16)

    def add_block(block):
        acc[...] += mm(nat[block], w_all[block], NT)

    def p_copy(block):
        slot = lax.div(block, 2)
        return remote(outgoing.at[slot], incoming.at[slot], ps.at[0], pr.at[slot], core_peer)

    def part(block):
        parts[block] = mm(att_t[...], nat[block], NN)

        @pl.when(lax.rem(block + me_dp, 2) == 1)
        def _():
            outgoing[lax.div(block, 2)] = parts[block, :, wide:].astype(bf16)
            p_copy(block).start()

    def both_copy(block):
        slot = lax.div(block, 2)
        return remote(
            both_outgoing.at[slot], both_incoming.at[slot], bps.at[0], bpr.at[slot], core_peer
        )

    def part_far(block):
        gate = gate_ref[:, pl.ds(pl.multiple_of(block * w, HD), wide)].astype(f32)
        cols = (raw_far[block].astype(f32) * gate).astype(bf16)
        both = parts[block, :, :wide] + mm(att_far[...], cols, NN)

        @pl.when(lax.rem(block + me_dp, 2) == 1)
        def _():
            both_outgoing[lax.div(block, 2)] = both.astype(bf16)
            both_copy(block).start()

        @pl.when(lax.rem(block + me_dp, 2) == 0)
        def _():
            parts[block, :, :wide] = both

    def bias_of(vis, t, far):
        owner = far_sp if far else me_sp
        place = map_ref[t, owner]

        def span(slab):
            apart = jnp.abs(owner - slab)
            spans = []
            for j in range(count):
                distance = jnp.abs(place - map_ref[j, slab])
                seen = (vis[t : t + 1, 0:1] >= apart) & (vis[t : t + 1, 1:2] >= distance)
                value = jnp.where(seen, 0.0, -1e30).astype(f32)
                spans.append(jnp.broadcast_to(value, (tile, 1)))
            return spans

        place_of = lax.broadcasted_iota(jnp.int32, (text, 1), 0)
        words = jnp.where(place_of < live_ref[0], 0.0, -1e30).astype(f32)
        return jnp.concatenate(span(me_sp) + [words] + span(far_sp), axis=0)

    def soft(q, h_cols, bias):
        scores = factor * mm(keys[:, h_cols], q, NT) + bias
        top = jnp.max(scores, axis=0, keepdims=True)
        weights = jnp.exp(scores - top)
        total = jnp.sum(weights, axis=0, keepdims=True)
        return weights * (1.0 / total)

    def cols_of(h):
        return pl.ds(pl.multiple_of(h * HD, HD), HD)

    def delta_of(ga, att):
        return jnp.sum(ga.astype(f32).T * att.astype(f32), axis=0, keepdims=True)

    def rows_of(t):
        return slice(t * tile, (t + 1) * tile)

    def chunk_rows(h):
        return pl.ds(pl.multiple_of(h * step_rows, step_rows), step_rows)

    def y_copy(h):
        rows = chunk_rows(h)
        return remote(last_out.at[rows], last_in.at[rows], ys.at[0], yr.at[h], top_peer)

    def g_copy(h):
        rows = chunk_rows(h)
        return remote(x_out.at[rows], x_in.at[rows], gs_sem.at[0], gr_sem.at[h], sp_far)

    def both_top(h):
        rows = chunk_rows(h)
        return remote(both_out.at[rows], both_in.at[rows], bys.at[0], byr.at[0], top_peer)

    scale(me_tp)
    for i in range(2):
        relay(near_line, 0, i)
    for i in range(2):
        settle(near_line, 0, i)
    each_block(0, scale)
    x_copies[1].wait_recv()

    def forward(h, carry):
        c = cols_of(h)
        for t in range(count):
            rows = rows_of(t)
            weights_s[h, :, rows] = soft(q_ref[rows, c], c, bias_of(win_own, t, False))
        return carry

    lax.fori_loop(0, heads, forward, 0)
    w_top[0].wait_recv()
    w_relay[0].start()
    for step in range(1, last):
        for i in range(2):
            relay(near_line, step, i)
    w_top[1].wait_recv()
    w_relay[1].start()
    for step in range(1, last):
        for i in range(2):
            settle(near_line, step, i)
    x_copies[2].wait_recv()

    def attend(h, carry):
        c = cols_of(h)
        att_t[c, :] = mm(vals[:, c], weights_s[h].astype(bf16), TN).astype(bf16)
        return carry

    lax.fori_loop(0, heads, attend, 0)
    part(me_tp)
    each_block(0, part)
    for step in range(1, last):
        each_block(step, scale)
        each_block(step, part)
    w_core.wait_recv()
    relayed = w_all.at[me_dp ^ core_bit ^ top_bit]
    remote(relayed, relayed, ws.at[2], wr.at[3], core_peer).wait_recv()
    acc[...] = mm(nat[me_tp], w_all[me_tp], NT)
    for step in range(last):
        each_block(step, add_block)

    away = me_dp ^ top_bit

    def send_top():
        p_copy(away).wait_recv()

        def chunk(h, carry):
            rows = chunk_rows(h)
            mine = parts[away, rows, wide:]
            pair = mine + incoming[lax.div(away, 2), rows, :].astype(f32)
            last_out[rows, :] = pair.astype(bf16)
            y_copy(h).start()
            return carry

        lax.fori_loop(0, chunks, chunk, 0)

    def send_both_top():
        both_copy(away).wait_recv()

        def chunk(h, carry):
            rows = chunk_rows(h)
            mine = parts[away, rows, :wide]
            pair = mine + both_incoming[lax.div(away, 2), rows, :].astype(f32)
            both_out[rows, :] = pair.astype(bf16)
            both_top(h).start()
            return carry

        lax.fori_loop(0, chunks, chunk, 0)

    late = jnp.abs(away - me_tp) == n_tp - 1

    @pl.when(jnp.logical_not(late))
    def _():
        send_top()

    for i in range(2):
        rows = slice(i * half, (i + 1) * half)
        grad_far[i].wait_recv()
        start_z(far_line, i)
        settle(near_line, last, i)

        def add_half(block):
            scale(block, rows)
            acc[rows] += mm(nat[block, rows], w_all[block], NT)

        each_block(last, add_half)
        ga_own[rows] = acc[rows].astype(bf16)
        x_copies[4 + i].start()
    each_block(last, part)

    def backward(h, carry):
        c = cols_of(h)
        for t in range(count):
            rows = rows_of(t)
            q = q_ref[rows, c]
            ga = ga_own[rows, c]
            weights = weights_s[h, :, rows]
            delta = delta_of(ga, att_t[c, rows])
            gp = mm(vals[:, c], ga, NT)
            gs = (weights * (gp - delta)).astype(bf16)
            gq_ref[rows, c] = (factor * mm(keys[:, c], gs, TN)).T.astype(bf16)
            gk = mm(gs[:near], q, NN)
            gv = mm(weights[:near].astype(bf16), ga, NN)
            if t == 0:
                gk_sum[:, c] = gk
                gv_sum[:, c] = gv
            else:
                gk_sum[:, c] += gk
                gv_sum[:, c] += gv

        return carry

    def pass_on(h):
        y_copy(h).wait_recv()
        rows = chunk_rows(h)
        mine = parts[me_dp, rows, wide:] + incoming[lax.div(me_dp, 2), rows, :].astype(f32)
        total = mine + last_in[rows, :].astype(f32)
        gw_ref[rows, wide:] = total
        x_out[rows, :] = total.astype(bf16)
        g_copy(h).start()

    x_copies[0].wait_recv()
    x_copies[3].wait_recv()

    def far_soft(h, carry):
        c = cols_of(h)
        for t in range(count):
            rows = rows_of(t)
            weights = soft(q_far[rows, c], c, bias_of(win_far, t, True))
            weights_far[h, :, rows] = weights[:near]
            att_far[c, rows] = mm(vals[:, c], weights.astype(bf16), TN).astype(bf16)
        return carry

    lax.fori_loop(0, early, far_soft, 0)

    @pl.when(late)
    def _():
        send_top()

    for i in range(2):
        relay(far_line, 0, i)
    x_copies[6].wait_recv()
    lax.fori_loop(early, heads, far_soft, 0)
    part_far(me_tp)
    for step in range(last):
        for i in range(2):
            if step:
                relay(far_line, step, i)
            settle(far_line, step, i)
        each_block(step, part_far)

    def pass_next(h, carry):
        pass_on(h)
        return carry

    first = lax.rem(me_dp, 2) == 0

    @pl.when(first)
    def _():
        p_copy(me_dp).wait_recv()
        lax.fori_loop(0, early, pass_next, 0)

    @pl.when(jnp.logical_not(late))
    def _():
        send_both_top()

    lax.fori_loop(0, heads - 2, backward, 0)
    for i in range(2):
        settle(far_line, last, i)
    each_block(last, part_far)

    @pl.when(first)
    def _():
        lax.fori_loop(early, chunks, pass_next, 0)

    lax.fori_loop(heads - 2, heads, backward, 0)
    remote(ga_own, ga_far, xs.at[4], xr.at[4], sp_far).wait_recv()

    @pl.when(jnp.logical_not(first))
    def _():
        p_copy(me_dp).wait_recv()
        lax.fori_loop(0, chunks, pass_next, 0)

    @pl.when(late)
    def _():
        send_both_top()


    def far(h, carry):
        c = cols_of(h)
        gk_all = gk_sum[:, c]
        gv_all = gv_sum[:, c]
        for t in range(count):
            rows = rows_of(t)
            q = q_far[rows, c]
            ga = ga_far[rows, c]
            weights = weights_far[h, :, rows]
            delta = delta_of(ga, att_far[c, rows])
            gp = mm(vals[:near, c], ga, NT)
            gs = (weights * (gp - delta)).astype(bf16)
            gk_all += mm(gs, q, NN)
            gv_all += mm(weights.astype(bf16), ga, NN)
        gk_ref[:, c] = (factor * gk_all[:tok]).astype(bf16)
        gtk_ref[:, c] = (factor * gk_all[tok:]).astype(bf16)
        gv_ref[:, c] = gv_all[:tok].astype(bf16)
        gtv_ref[:, c] = gv_all[tok:].astype(bf16)
        return carry

    lax.fori_loop(0, heads, far, 0)
    both_copy(me_dp).wait_recv()
    remote(both_out, both_in, bys.at[0], byr.at[0], top_peer).wait_recv()

    def finish_both(h, carry):
        rows = chunk_rows(h)
        mine = parts[me_dp, rows, :wide] + both_incoming[lax.div(me_dp, 2), rows, :].astype(f32)
        gw_ref[rows, :wide] = mine + both_in[rows, :].astype(f32)
        return carry

    lax.fori_loop(0, chunks, finish_both, 0)
    both_keys, pair = pl.ds(0, 2 * tok), pl.ds(0, n_dp // 2)
    for c in [
        x_copies[0],
        remote(keys.at[both_keys], keys.at[both_keys], xs.at[1], xr.at[1], sp_far),
        remote(q_ref, q_far, xs.at[3], xr.at[3], sp_far),
        remote(ga_own, ga_far, xs.at[4], xr.at[4], sp_far),
        remote(raw_far.at[me_tp], raw_far.at[me_tp], xs.at[5], xr.at[7], sp_far),
        w_core,
        remote(w_all.at[me_dp], w_all.at[me_dp], ws.at[1], wr.at[1], top_peer),
        remote(w_all.at[me_dp], w_all.at[me_dp], ws.at[2], wr.at[3], core_peer),
        remote(outgoing.at[pair], incoming.at[pair], ps.at[0], pr.at[0], core_peer),
        remote(both_outgoing.at[pair], both_incoming.at[pair], bps.at[0], bpr.at[0], core_peer),
        remote(last_out, last_in, ys.at[0], yr.at[0], top_peer),
        remote(both_out, both_in, bys.at[0], byr.at[0], top_peer),
    ]:
        c.wait_send()
    for line in (near_line, far_line):
        sent_z(line)

    def finish(h, carry):
        rows = chunk_rows(h)
        g_copy(h).wait_recv()
        gw_ref[rows, wide:] += x_in[rows, :].astype(f32)
        return carry

    lax.fori_loop(0, chunks, finish, 0)
    remote(x_out, x_in, gs_sem.at[0], gr_sem.at[0], sp_far).wait_send()


def mega_call(n_tp, n_dp, q, k, v, tk, tv, s, w, gate, windows, tile_map, text_count):
    tok, width = q.shape
    text = tk.shape[0]
    heads = width // HD
    cols = w.shape[1]
    total = 2 * tok + text
    near = tok + text
    count = tile_map.shape[0]
    pairs = n_dp // 2
    wide = int(cols * SHARE) // HD * HD
    bf16, f32 = jnp.bfloat16, jnp.float32
    dma = pltpu.SemaphoreType.DMA
    shapes = [
        ((tok, width), bf16),
        ((tok, width), bf16),
        ((tok, width), bf16),
        ((text, width), bf16),
        ((text, width), bf16),
        ((width, cols), f32),
    ]
    small = [
        pltpu.VMEM((tok, width), bf16),
        pltpu.VMEM(gate.shape, bf16),
        pltpu.VMEM(windows.shape, jnp.int32),
        pltpu.SMEM(tile_map.shape, jnp.int32),
        pltpu.SMEM(text_count.shape, jnp.int32),
    ]
    scratch = [
        ((total, width), bf16),
        ((total, width), bf16),
        ((tok, width), bf16),
        ((tok, width), bf16),
        ((tok, width), bf16),
        ((count + -count % 8, HD), jnp.int32),
        ((count + -count % 8, HD), jnp.int32),
        ((n_tp, tok, s.shape[1]), bf16),
        ((n_tp, tok, s.shape[1]), bf16),
        ((n_tp, tok, wide), bf16),
        ((n_dp, width, cols), bf16),
        ((tok, width), f32),
        ((width, tok), bf16),
        ((width, tok), bf16),
        ((heads, total, tok), f32),
        ((heads, near, tok), f32),
        ((near, width), f32),
        ((near, width), f32),
        ((n_dp, width, cols), f32),
        ((pairs, width, cols - wide), bf16),
        ((pairs, width, cols - wide), bf16),
        ((width, cols - wide), bf16),
        ((width, cols - wide), bf16),
        ((width, cols - wide), bf16),
        ((width, cols - wide), bf16),
        ((pairs, width, wide), bf16),
        ((pairs, width, wide), bf16),
        ((width, wide), bf16),
        ((width, wide), bf16),
    ]
    sems = [(11,), (6,), (8,), (3,), (4,)] + [(1,), (1,), (n_tp, 2)] * 2 + [(1,), (pairs,)] * 2
    sems += [(1,), (heads,), (1,), (1,), (1,), (heads,)]
    held = sum(jnp.dtype(b).itemsize * a[0] * a[1] for a, b in shapes)
    return pl.pallas_call(
        functools.partial(mega_kernel, count, n_tp, n_dp),
        out_shape=[pltpu.VMEM(a, b) for a, b in shapes],
        in_specs=[pl.BlockSpec(memory_space=pltpu.HBM)] * 11,
        out_specs=[pl.BlockSpec(memory_space=pltpu.VMEM)] * 6,
        scratch_shapes=small + [pltpu.VMEM(a, b) for a, b in scratch] + [dma(n) for n in sems],
        compiler_params=pltpu.CompilerParams(
            collective_id=0, has_side_effects=True, vmem_limit_bytes=VMEM - held - (1 << 18)
        ),
        name="attention_backward",
    )(q, k, v, tk, tv, s, w, gate, windows, tile_map, text_count)


def per_device(
    query,
    key,
    value,
    text_key,
    text_value,
    grad_out,
    gate,
    out_weight,
    windows,
    tile_map,
    text_count,
):
    q, k, v = query[0], key[0], value[0]
    tk, tv = text_key[0], text_value[0]
    tok, width = q.shape
    n_sp = lax.axis_size("sp")
    n_dp = lax.axis_size("dp")
    n_tp = lax.axis_size("tp")
    me_sp = lax.axis_index("sp")
    me_tp = lax.axis_index("tp")
    me_dp = lax.axis_index("dp")
    index = jnp.stack([me_tp, me_dp]).astype(jnp.int32)

    offsets = sorted({1 % n_sp, (n_sp - 1) % n_sp} - {0})

    def from_offset(block, offset):
        route = [((i + offset) % n_sp, i) for i in range(n_sp)]
        route = [(a, b) for a, b in route if abs(a - b) <= 1]
        return lax.ppermute(block, "sp", route)

    def to_offset(block, offset):
        route = [(i, (i + offset) % n_sp) for i in range(n_sp)]
        route = [(a, b) for a, b in route if abs(a - b) <= 1]
        return lax.ppermute(block, "sp", route)

    own_gate = lax.dynamic_slice_in_dim(gate[0], me_tp * width, width, 0)
    scaled = (grad_out[0].astype(jnp.float32) * own_gate.astype(jnp.float32)[None, :]).astype(
        jnp.bfloat16
    )
    own_map = lax.dynamic_index_in_dim(tile_map, me_sp, 0, keepdims=False)
    count = own_map.shape[0]
    tile = tok // count
    live = jnp.arange(tk.shape[0], dtype=jnp.int32) < text_count[0]

    def tiles_seen(o):
        other = lax.rem(me_sp + o, n_sp)
        apart = jnp.abs(other - me_sp)
        other_map = lax.dynamic_index_in_dim(tile_map, other, 0, keepdims=False)
        near_time = (apart <= windows[:, 0]) & (apart <= 1)
        near_space = jnp.abs(own_map[:, None] - other_map[None, :]) <= windows[:, 1][:, None]
        return near_time[:, None] & near_space

    if offsets == [n_sp - 1] and n_tp == n_dp and len(bits_of(n_dp)) == 2:
        outs = mega_call(
            n_tp,
            n_dp,
            q,
            k,
            v,
            tk,
            tv,
            grad_out[0],
            out_weight,
            gate,
            windows,
            tile_map.T,
            text_count,
        )
        outs = copy_call(outs)
        return tuple(o[None] for o in outs[:5]) + (outs[5],)

    near_k = [from_offset(k, o) for o in offsets]
    near_v = [from_offset(v, o) for o in offsets]

    s_rel = ring_gather(scaled, "tp")
    w_rel = xor_gather(out_weight, "dp")

    seen = [jnp.repeat(tiles_seen(o), tile, axis=1) for o in [0] + offsets]
    seen.append(jnp.broadcast_to(live[None, :], (count, tk.shape[0])))
    bias = jnp.where(jnp.concatenate(seen, axis=1), 0.0, -1e30).astype(jnp.float32)[:, :, None]

    nat, ga = grad_attn_call(index, s_rel, w_rel)

    heads = width // HD
    groups = GROUPS if heads % GROUPS == 0 else 1
    each = heads // groups
    ks = [k] + near_k + [tk]
    vs = [v] + near_v + [tv]
    nk = len(ks)
    ats, gqs, gks, gvs, gtk, gtv = [], [], [], [], [], []
    for g in range(groups):
        res = attention_call(g * each, each, count, q, ga, bias, ks, vs)
        at, gq = res[:2]
        gk, gv = list(res[2 : 2 + nk]), list(res[2 + nk :])
        ats.append(at)
        gqs.append(gq)
        own_k, own_v = gk[0], gv[0]
        for i, o in enumerate(offsets):
            own_k = own_k + to_offset(gk[1 + i], o).astype(jnp.float32)
            own_v = own_v + to_offset(gv[1 + i], o).astype(jnp.float32)
        gks.append(own_k)
        gvs.append(own_v)
        gtk.append(total_over(gk[-1], "sp"))
        gtv.append(total_over(gv[-1], "sp"))

    parts = dict(enumerate(weight_call(index, nat, ats, n_dp)))
    for bit in bits_of(n_dp):
        got = {
            d: lax.ppermute(parts[d | bit].astype(jnp.bfloat16), "dp", xor_route("dp", bit))
            for d in parts
            if not d & bit
        }
        parts = {d: parts[d].astype(jnp.float32) + got[d].astype(jnp.float32) for d in got}
    weight_grad = total_over(parts[0], "sp")

    def joined(pieces):
        return jnp.concatenate(pieces, axis=1).astype(jnp.bfloat16)[None]

    return (joined(gqs), joined(gks), joined(gvs), joined(gtk), joined(gtv), weight_grad)


def solution(mesh):
    placed = (
        P("dp", "sp", "tp"),
        P("dp", "sp", "tp"),
        P("dp", "sp", "tp"),
        P("dp", None, "tp"),
        P("dp", None, "tp"),
        P("dp", "sp", "tp"),
        P("dp", None),
        P("tp", "dp"),
        P("sp", None),
        P(),
        P("dp"),
    )
    return jax.shard_map(
        per_device,
        mesh=mesh,
        in_specs=placed,
        out_specs=(
            P("dp", "sp", "tp"),
            P("dp", "sp", "tp"),
            P("dp", "sp", "tp"),
            P("dp", None, "tp"),
            P("dp", None, "tp"),
            P("tp", "dp"),
        ),
        check_vma=False,
    )
```
